8 devices in a mesh: dp: 2 (over z, y), tp: 4 (over x, core).
Axes of the slice: x: 2, y: 2, z: 1, core: 2. Of those that a mesh axis runs over, the one named last changes fastest.
Arguments:
- hidden: bfloat16 [32, 1024], P('dp'), parts along dimension 0
- lengths: int32 [32], P('dp'), parts along dimension 0
- choice: int32 [2, 32, 8], P(None, 'dp'), parts along dimension 1
- keys_one: bfloat16 [32, 64, 8, 64], P('dp', 'tp'), parts along dimension 0
- vals_one: bfloat16 [32, 64, 8, 64], P('dp', 'tp'), parts along dimension 0
- keys_two: bfloat16 [32, 64, 8, 64], P('dp', 'tp'), parts along dimension 0
- vals_two: bfloat16 [32, 64, 8, 64], P('dp', 'tp'), parts along dimension 0
- g_attn: bfloat16 [2, 1024], replicated
- w_q: bfloat16 [2, 1024, 1024], P(None, None, 'tp')
- w_k: bfloat16 [2, 1024, 512], P(None, None, 'tp')
- w_v: bfloat16 [2, 1024, 512], P(None, None, 'tp')
- w_o: bfloat16 [2, 1024, 1024], P(None, 'tp')
- g_mlp: bfloat16 [2, 1024], replicated
- w_router: bfloat16 [2, 1024, 32], replicated
- w_gate: bfloat16 [2, 32, 1024, 512], P(None, None, None, 'tp')
- w_up: bfloat16 [2, 32, 1024, 512], P(None, None, None, 'tp')
- w_down: bfloat16 [2, 32, 512, 1024], P(None, None, 'tp')
Outputs:
- output 1: bfloat16 [32, 1024], P('dp'), parts along dimension 0
- output 2: bfloat16 [32, 64, 8, 64], P('dp', None, 'tp'), parts along dimension 0
- output 3: bfloat16 [32, 64, 8, 64], P('dp', None, 'tp'), parts along dimension 0
- output 4: bfloat16 [32, 64, 8, 64], P('dp', None, 'tp'), parts along dimension 0
- output 5: bfloat16 [32, 64, 8, 64], P('dp', None, 'tp'), parts along dimension 0
There are 2 independent parts. The reference program is written for one: setup_inputs(seed, part) draws one part's arguments, and reference() takes and returns one part's arrays. A program takes and returns all parts, laid end to end along the dimension named above; an argument that names none is the same for every part.
All inputs are finite; a program needn't handle non-finite values.
Results may differ from the reference program's by a relative error of at most 0.02.
Values are sent between devices in bfloat16 or wider.
A program may use at most 1 GiB of HBM per device.

```python
import jax
import jax.numpy as jnp
from jax import lax

BATCH = 16
SEQ = 64
D = 1024
HEADS = 16
KV_HEADS = 8
HEAD = 64
FF = 512
EXPERTS = 32
TOP = 8
LAYERS = 2
EPS = 1e-5
THETA = 1000000.0


def weight_draw(key, shape, fan_in, gain_mult):
    return (jax.random.normal(key, shape, jnp.float32) * (gain_mult * fan_in ** -0.5)).astype(jnp.bfloat16)


def value_walk(key, cache_shape):
    step_key, noise_key = jax.random.split(key)
    walk_steps = jax.random.normal(step_key, cache_shape, jnp.float32) * SEQ ** -0.5
    noise_part = 0.5 * jax.random.normal(noise_key, cache_shape, jnp.float32)
    return (jnp.cumsum(walk_steps, axis=1) + noise_part).astype(jnp.bfloat16)


def setup_inputs(seed: int = 0, part: int = 0) -> dict:
    base_key = jax.random.key(seed)
    shared = jax.random.split(base_key, 11)
    local_keys = jax.random.split(jax.random.fold_in(base_key, part), 9)
    cache_shape = (BATCH, SEQ, KV_HEADS, HEAD)
    hidden = jax.random.normal(local_keys[0], (BATCH, D), jnp.float32).astype(jnp.bfloat16)
    drawn_lens = jax.random.randint(local_keys[1], (BATCH,), 0, SEQ)
    full_row = jax.random.randint(local_keys[2], (), 0, BATCH)
    lengths = jnp.where(jnp.arange(BATCH) == full_row, SEQ - 1, drawn_lens).astype(jnp.int32)
    rank_score = jax.random.randint(local_keys[3], (LAYERS, BATCH, EXPERTS), 0, 2 ** 20) * EXPERTS + jnp.arange(EXPERTS)
    choice = lax.top_k(rank_score, TOP)[1].astype(jnp.int32)
    return {
        'hidden': hidden,
        'lengths': lengths,
        'choice': choice,
        'keys_one': jax.random.normal(local_keys[4], cache_shape, jnp.float32).astype(jnp.bfloat16),
        'vals_one': value_walk(local_keys[5], cache_shape),
        'keys_two': jax.random.normal(local_keys[6], cache_shape, jnp.float32).astype(jnp.bfloat16),
        'vals_two': value_walk(local_keys[7], cache_shape),
        'g_attn': (1.0 + 0.3 * jax.random.normal(shared[0], (LAYERS, D), jnp.float32)).astype(jnp.bfloat16),
        'w_q': weight_draw(shared[1], (LAYERS, D, HEADS * HEAD), D, 1.0),
        'w_k': weight_draw(shared[2], (LAYERS, D, KV_HEADS * HEAD), D, 1.0),
        'w_v': weight_draw(shared[3], (LAYERS, D, KV_HEADS * HEAD), D, 1.0),
        'w_o': weight_draw(shared[4], (LAYERS, HEADS * HEAD, D), HEADS * HEAD, 1.0),
        'g_mlp': (1.0 + 0.3 * jax.random.normal(shared[5], (LAYERS, D), jnp.float32)).astype(jnp.bfloat16),
        'w_router': weight_draw(shared[6], (LAYERS, D, EXPERTS), D, 2.0),
        'w_gate': weight_draw(shared[7], (LAYERS, EXPERTS, D, FF), D, 1.0),
        'w_up': weight_draw(shared[8], (LAYERS, EXPERTS, D, FF), D, 1.0),
        'w_down': weight_draw(shared[9], (LAYERS, EXPERTS, FF, D), FF, 2.0),
    }


def rms_norm(tensor, gain_vec):
    tensor_f = tensor.astype(jnp.float32)
    scale = lax.rsqrt(jnp.mean(tensor_f * tensor_f, axis=-1, keepdims=True) + EPS)
    return (tensor_f * scale * gain_vec.astype(jnp.float32)).astype(jnp.bfloat16)


def apply_rope(tensor, lengths):
    head_dim = tensor.shape[-1]
    half_dim = head_dim // 2
    inv_freq = THETA ** (-2.0 * jnp.arange(half_dim, dtype=jnp.float32) / head_dim)
    angle = lengths.astype(jnp.float32)[:, None] * inv_freq[None, :]
    cos_part = jnp.cos(angle)[:, None, :]
    sin_part = jnp.sin(angle)[:, None, :]
    lower_half = tensor[..., :half_dim]
    upper_half = tensor[..., half_dim:]
    return jnp.concatenate([lower_half * cos_part - upper_half * sin_part, upper_half * cos_part + lower_half * sin_part], axis=-1)


def decode_layer(hidden, lengths, choice, key_cache, val_cache, g_attn, w_q, w_k, w_v, w_o, g_mlp, w_router, w_gate, w_up, w_down):
    batch_rows = hidden.shape[0]
    seq_len = key_cache.shape[1]
    normed = rms_norm(hidden, g_attn)
    query_rot = apply_rope(jnp.dot(normed, w_q, preferred_element_type=jnp.float32).reshape(batch_rows, HEADS, HEAD), lengths).astype(jnp.bfloat16)
    key_new = apply_rope(jnp.dot(normed, w_k, preferred_element_type=jnp.float32).reshape(batch_rows, KV_HEADS, HEAD), lengths).astype(jnp.bfloat16)
    val_new = jnp.dot(normed, w_v, preferred_element_type=jnp.float32).astype(jnp.bfloat16).reshape(batch_rows, KV_HEADS, HEAD)
    positions = jnp.arange(seq_len)
    is_new = (positions[None, :] == lengths[:, None])[:, :, None, None]
    key_cache = jnp.where(is_new, key_new[:, None], key_cache)
    val_cache = jnp.where(is_new, val_new[:, None], val_cache)
    query_grp = query_rot.reshape(batch_rows, KV_HEADS, HEADS // KV_HEADS, HEAD)
    scores = jnp.einsum('bgrd,bsgd->bgrs', query_grp.astype(jnp.float32), key_cache.astype(jnp.float32)) * HEAD ** -0.5
    is_valid = (positions[None, :] <= lengths[:, None])[:, None, None, :]
    attn_prob = jax.nn.softmax(jnp.where(is_valid, scores, -1e30), axis=-1).astype(jnp.bfloat16)
    attn_vec = jnp.einsum('bgrs,bsgd->bgrd', attn_prob.astype(jnp.float32), val_cache.astype(jnp.float32)).astype(jnp.bfloat16).reshape(batch_rows, HEADS * HEAD)
    x_mid = (hidden.astype(jnp.float32) + jnp.dot(attn_vec, w_o, preferred_element_type=jnp.float32)).astype(jnp.bfloat16)
    normed_mid = rms_norm(x_mid, g_mlp)
    logits = jnp.dot(normed_mid, w_router, preferred_element_type=jnp.float32)
    onehot = (choice[:, :, None] == jnp.arange(EXPERTS)[None, None, :]).astype(jnp.float32)
    gate_prob = jax.nn.softmax(jnp.sum(onehot * logits[:, None, :], axis=-1), axis=-1)
    gate_mat = jnp.sum(gate_prob[:, :, None] * onehot, axis=1)
    gate_act = jnp.einsum('bd,edf->bef', normed_mid.astype(jnp.float32), w_gate.astype(jnp.float32))
    up_act = jnp.einsum('bd,edf->bef', normed_mid.astype(jnp.float32), w_up.astype(jnp.float32))
    expert_in = (jax.nn.silu(gate_act) * up_act * gate_mat[:, :, None]).astype(jnp.bfloat16)
    moe_out = jnp.einsum('bef,efd->bd', expert_in.astype(jnp.float32), w_down.astype(jnp.float32))
    return (x_mid.astype(jnp.float32) + moe_out).astype(jnp.bfloat16), key_cache, val_cache


def reference(hidden, lengths, choice, keys_one, vals_one, keys_two, vals_two, g_attn, w_q, w_k, w_v, w_o, g_mlp, w_router, w_gate, w_up, w_down):
    caches = [(keys_one, vals_one), (keys_two, vals_two)]
    results = []
    for layer_idx in range(LAYERS):
        hidden, key_cache, val_cache = decode_layer(hidden, lengths, choice[layer_idx], caches[layer_idx][0], caches[layer_idx][1], g_attn[layer_idx], w_q[layer_idx], w_k[layer_idx], w_v[layer_idx], w_o[layer_idx], g_mlp[layer_idx], w_router[layer_idx], w_gate[layer_idx], w_up[layer_idx], w_down[layer_idx])
        results.append(key_cache)
        results.append(val_cache)
    return (hidden, results[0], results[1], results[2], results[3])
```

```python
import functools

import numpy as np

import jax
import jax.numpy as jnp
from jax import lax
from jax.experimental import pallas as pl
from jax.experimental.pallas import tpu as pltpu
from jax.sharding import PartitionSpec as P

EPS = 1e-5
THETA = 1000000.0
MESH = pl.DeviceIdType.MESH
B = 16
D = 1024
SEQ = 64
BLK = 16
NTP = 4
EXP = 32
FL = 128
GCH = 4
DCH = 8
NCH = 512
F32 = jnp.float32
BF16 = jnp.bfloat16


def _norm(h_f, gain_row):
    scale = lax.rsqrt(jnp.mean(h_f * h_f, axis=-1, keepdims=True) + EPS)
    return (h_f * scale * gain_row).astype(BF16)


def _rope(x, cosv, sinv, low):
    rot = jnp.where(low, -pltpu.roll(x, 96, 1), pltpu.roll(x, 32, 1))
    return x * cosv + rot * sinv


def _kernel(hid_h, len_h, cho_h, k1_h, v1_h, k2_h, v2_h, ga_h, wq_h, wk_h, wv_h, wo_h, gm_h, wr_h, wg_h, wu_h, wd_h, inv_h,
            hout_h, ok1_h, ov1_h, ok2_h, ov2_h,
            hid, lens, cho, raw, ga, wq, wk, wv, wo, gm, wr, wg, wu, wd, inv,
            spread, snd, kall, xown, xrecv, gexp, act, hfin,
            sem_s, sem_raw, sem_g, sem_u, sem_d, send_c, recv_c, send_x, recv_x, sem_o):
    me = lax.axis_index("tp")
    chip, core = me // 2, me % 2
    partner = chip * 2 + (1 - core)
    cross_a = (1 - chip) * 2 + core
    cross_b = (1 - chip) * 2 + (1 - core)
    peers = (cross_a, cross_b, partner)

    barrier = pltpu.get_barrier_semaphore()
    for p in peers:
        pl.semaphore_signal(barrier, inc=1, device_id={"tp": p}, device_id_type=MESH)

    raw_src = (k1_h, v1_h, k2_h, v2_h)

    def raw_copy(c):
        return pltpu.make_async_copy(raw_src[c], raw.at[c], sem_raw.at[c])

    smalls = ((hid_h, hid), (len_h, lens), (cho_h, cho), (ga_h, ga), (gm_h, gm), (inv_h, inv),
              (wq_h, wq), (wk_h, wk), (wv_h, wv), (wo_h, wo), (wr_h, wr))

    def small_copy(i):
        return pltpu.make_async_copy(smalls[i][0], smalls[i][1], sem_s.at[i])

    def g_copy(l, i):
        sl = pl.ds(i * GCH, GCH)
        return pltpu.make_async_copy(wg_h.at[l, sl], wg.at[l, sl], sem_g.at[l, i])

    def u_copy(l, i):
        sl = pl.ds(i * GCH, GCH)
        return pltpu.make_async_copy(wu_h.at[l, sl], wu.at[l, sl], sem_u.at[l, i])

    def d_copy(l, i):
        sl = pl.ds(i * DCH, DCH)
        return pltpu.make_async_copy(wd_h.at[l, sl], wd.at[l, sl], sem_d.at[l, i])

    raw_copy(0).start()
    raw_copy(1).start()
    for i in range(len(smalls)):
        small_copy(i).start()
    raw_copy(2).start()
    raw_copy(3).start()

    def start_layer(l):
        def gu(i, _):
            g_copy(l, i).start()
            u_copy(l, i).start()
            return 0
        lax.fori_loop(0, EXP // GCH, gu, 0)

        def dn(i, _):
            d_copy(l, i).start()
            return 0
        lax.fori_loop(0, EXP // DCH, dn, 0)

    def cache_copy(c, n):
        return pltpu.make_async_remote_copy(
            src_ref=snd.at[c, peers[n]], dst_ref=kall.at[c, me],
            send_sem=send_c.at[c, n], recv_sem=recv_c.at[c, me],
            device_id={"tp": peers[n]}, device_id_type=MESH)

    def cache_recv(c, n):
        return pltpu.make_async_remote_copy(
            src_ref=snd.at[c, peers[n]], dst_ref=kall.at[c, peers[n]],
            send_sem=send_c.at[c, n], recv_sem=recv_c.at[c, peers[n]],
            device_id={"tp": peers[n]}, device_id_type=MESH)

    def repack(c):
        raw_copy(c).wait()
        spread[...] = raw[c].reshape(B * BLK * 8, 64).astype(F32)
        for p in range(NTP):
            lo = spread[pl.ds(2 * p, B * BLK, stride=8), :]
            hi = spread[pl.ds(2 * p + 1, B * BLK, stride=8), :]
            snd[c, p] = jnp.concatenate([lo, hi], axis=1).astype(BF16).reshape(B, BLK, 128)
        kall[c, me] = snd[c, me]

    repack(0)
    pl.semaphore_wait(barrier, 3)
    for n in range(3):
        cache_copy(0, n).start()
    repack(1)
    for n in range(3):
        cache_copy(1, n).start()
    start_layer(0)
    start_layer(1)
    repack(2)
    repack(3)
    for c in (2, 3):
        cache_copy(c, 2).start()

    for i in range(len(smalls)):
        small_copy(i).wait()

    eye = lax.broadcasted_iota(jnp.int32, (B, B), 0) == lax.broadcasted_iota(jnp.int32, (B, B), 1)
    len_row = jnp.broadcast_to(lens[...].astype(F32), (B, B))
    len_col = jnp.sum(jnp.where(eye, len_row, 0.0), axis=1, keepdims=True)
    len_b = jnp.broadcast_to(len_col, (B, 128))
    angle = len_b * inv[...]
    cosv, sinv = jnp.cos(angle), jnp.sin(angle)
    lane = lax.broadcasted_iota(jnp.int32, (B, 128), 1)
    low = (lane % 64) < 32
    left = lane < 64
    col = lax.broadcasted_iota(jnp.int32, (64, 1024), 1)
    row = lax.broadcasted_iota(jnp.int32, (64, 1024), 0)
    len64 = jnp.concatenate([len_col] * 4, axis=0)
    pos = ((col // 256) * BLK + col % BLK).astype(F32)
    valid = (((col // BLK) % B) == (row % B)) & (pos <= len64)

    h_f = hid[...].astype(F32)

    def insert(c, new):
        new3 = jnp.broadcast_to(new[:, None, :], (B, BLK, 128))
        len3 = jnp.broadcast_to(len_b[:, None, :], (B, BLK, 128))
        pos3 = lax.broadcasted_iota(jnp.int32, (B, BLK, 128), 1).astype(F32)
        for s in range(NTP):
            cur = kall[c, s].astype(F32)
            kall[c, s] = jnp.where(pos3 + float(s * BLK) == len3, new3, cur).astype(BF16)

    def out_copy(c, s, ref):
        return pltpu.make_async_copy(kall.at[c, s], ref.at[:, pl.ds(s * BLK, BLK), :], sem_o.at[c, s])

    def x_copy(step, piece, n):
        sl = pl.ds(piece * NCH, NCH)
        return pltpu.make_async_remote_copy(
            src_ref=xown.at[step, :, sl], dst_ref=xrecv.at[step, me, :, sl],
            send_sem=send_x.at[step, piece, n], recv_sem=recv_x.at[step, me, piece],
            device_id={"tp": peers[n]}, device_id_type=MESH)

    def x_recv(step, piece, n):
        sl = pl.ds(piece * NCH, NCH)
        return pltpu.make_async_remote_copy(
            src_ref=xown.at[step, :, sl], dst_ref=xrecv.at[step, peers[n], :, sl],
            send_sem=send_x.at[step, piece, n], recv_sem=recv_x.at[step, peers[n], piece],
            device_id={"tp": peers[n]}, device_id_type=MESH)

    def x_send(step, piece, val):
        sl = pl.ds(piece * NCH, NCH)
        xown[step, :, sl] = val
        for n in range(3):
            x_copy(step, piece, n).start()
        xrecv[step, me, :, sl] = val

    def x_sum(step):
        for piece in range(D // NCH):
            for n in range(3):
                x_recv(step, piece, n).wait_recv()
        tot = xrecv[step, 0].astype(F32)
        for s in range(1, NTP):
            tot = tot + xrecv[step, s].astype(F32)
        return tot

    outs = (ok1_h, ov1_h, ok2_h, ov2_h)

    for l in range(2):
        a = _norm(h_f, ga[pl.ds(l, 1), :].astype(F32))
        qf = jnp.dot(a, wq[l], preferred_element_type=F32)
        kf = jnp.dot(a, wk[l], preferred_element_type=F32)
        vf = jnp.dot(a, wv[l], preferred_element_type=F32)
        q0 = _rope(qf[:, :128], cosv, sinv, low)
        q1 = _rope(qf[:, 128:], cosv, sinv, low)
        knew = _rope(kf, cosv, sinv, low).astype(BF16).astype(F32)
        vnew = vf.astype(BF16).astype(F32)
        zero = jnp.zeros_like(q0)
        qrows = jnp.concatenate([
            jnp.where(left, q0, zero), jnp.where(left, pltpu.roll(q0, 64, 1), zero),
            jnp.where(left, zero, pltpu.roll(q1, 64, 1)), jnp.where(left, zero, q1)], axis=0).astype(BF16)
        kc, vc = 2 * l, 2 * l + 1
        for n in range(3):
            cache_recv(kc, n).wait_recv()
        insert(kc, knew)
        for s in range(NTP):
            out_copy(kc, s, outs[kc]).start()
        k2d = kall[kc].reshape(NTP * B * BLK, 128)
        sc = lax.dot_general(qrows, k2d, (((1,), (1,)), ((), ())), preferred_element_type=F32) * 0.125
        sc = jnp.where(valid, sc, -1e30)
        ex = jnp.exp(sc - jnp.max(sc, axis=1, keepdims=True))
        prob = (ex / jnp.sum(ex, axis=1, keepdims=True)).astype(BF16)
        for n in range(3):
            cache_recv(vc, n).wait_recv()
        insert(vc, vnew)
        for s in range(NTP):
            out_copy(vc, s, outs[vc]).start()
        if l == 0:
            cache_copy(2, 0).start()
        v2d = kall[vc].reshape(NTP * B * BLK, 128)
        ov = jnp.dot(prob, v2d, preferred_element_type=F32)
        o0 = jnp.where(left, ov[0:16], pltpu.roll(ov[16:32], 64, 1))
        o1 = jnp.where(left, pltpu.roll(ov[32:48], 64, 1), ov[48:64])
        attn = jnp.concatenate([o0, o1], axis=1).astype(BF16)
        for piece in range(D // NCH):
            x_send(2 * l, piece, jnp.dot(attn, wo[l, :, pl.ds(piece * NCH, NCH)], preferred_element_type=F32).astype(BF16))
        h1 = (h_f + x_sum(2 * l)).astype(BF16).astype(F32)
        if l == 0:
            cache_copy(2, 1).start()
            cache_copy(3, 0).start()
        m = _norm(h1, gm[pl.ds(l, 1), :].astype(F32))

        lg = lax.dot_general(wr[l], m, (((1,), (1,)), ((), ())), preferred_element_type=F32)
        eid = lax.broadcasted_iota(jnp.int32, (EXP, B), 0)
        chosen = eid < 0
        for k in range(8):
            chosen = chosen | (cho[l, pl.ds(k, 1), :] == eid)
        lg = jnp.where(chosen, lg, -jnp.inf)
        ex = jnp.where(chosen, jnp.exp(lg - jnp.max(lg, axis=0, keepdims=True)), 0.0)
        gate_t = ex / jnp.sum(ex, axis=0, keepdims=True)
        gate = gate_t.T
        for e in range(EXP):
            gexp[e] = jnp.broadcast_to(gate[:, e:e + 1], (B, FL))

        def gate_up(i, _):
            g_copy(l, i).wait()
            u_copy(l, i).wait()
            for j in range(GCH):
                e = i * GCH + j
                w = jnp.concatenate([wg[l, e], wu[l, e]], axis=1)
                gu = jnp.dot(m, w, preferred_element_type=F32)
                g, u = gu[:, :FL], gu[:, FL:]
                act[e] = (g * jax.nn.sigmoid(g) * u * gexp[e]).astype(BF16)
            return 0
        lax.fori_loop(0, EXP // GCH, gate_up, 0)

        def dwait(i, _):
            d_copy(l, i).wait()
            return 0
        lax.fori_loop(0, EXP // DCH, dwait, 0)
        for piece in range(D // NCH):
            sl = pl.ds(piece * NCH, NCH)

            def down(i, acc):
                for j in range(4):
                    e = i * 8 + 2 * j
                    lhs = jnp.concatenate([act[e], act[e + 1]], axis=1)
                    rhs = jnp.concatenate([wd[l, e, :, sl], wd[l, e + 1, :, sl]], axis=0)
                    acc = acc + jnp.dot(lhs, rhs, preferred_element_type=F32)
                return acc
            acc = lax.fori_loop(0, EXP // 8, down, jnp.zeros((B, NCH), F32))
            x_send(2 * l + 1, piece, acc.astype(BF16))
        if l == 0:
            cache_copy(3, 1).start()
        h_f = (h1 + x_sum(2 * l + 1)).astype(BF16).astype(F32)

    hfin[...] = h_f.astype(BF16)
    done = pltpu.make_async_copy(hfin, hout_h, sem_s.at[0])
    done.start()
    for c in range(4):
        for s in range(NTP):
            out_copy(c, s, outs[c]).wait()
        for n in range(3):
            cache_copy(c, n).wait_send()
    for step in range(4):
        for piece in range(D // NCH):
            for n in range(3):
                x_copy(step, piece, n).wait_send()
    done.wait()


def solution(mesh):
    seq_spec = P('dp', 'tp', None, None)
    head_spec = P('dp', None, 'tp', None)
    col_spec = P(None, None, 'tp')
    ff_spec = P(None, None, None, 'tp')
    inv_freq = (THETA ** (-2.0 * np.arange(32, dtype=np.float64) / 64)).astype(np.float32)
    inv_row = np.tile(inv_freq, 4)[None, :]

    def local_step(hidden, lengths, choice, keys_one, vals_one, keys_two, vals_two, g_attn, w_q, w_k, w_v, w_o, g_mlp, w_router, w_gate, w_up, w_down):
        dense = jax.ShapeDtypeStruct((B, SEQ, 128), BF16)
        any_spec = pl.BlockSpec(memory_space=pl.ANY)
        V = pltpu.VMEM
        DMA = pltpu.SemaphoreType.DMA
        outs = pl.pallas_call(
            _kernel,
            out_shape=(jax.ShapeDtypeStruct((B, D), BF16), dense, dense, dense, dense),
            in_specs=[any_spec] * 18,
            out_specs=(any_spec,) * 5,
            scratch_shapes=[
                V((B, D), BF16), V((1, B), jnp.int32), V((2, 8, B), jnp.int32), V((4, B, BLK, 8, 64), BF16),
                V((2, D), BF16), V((2, D, 256), BF16), V((2, D, 128), BF16), V((2, D, 128), BF16), V((2, 256, D), BF16),
                V((2, D), BF16), V((2, EXP, D), BF16), V((2, EXP, D, FL), BF16), V((2, EXP, D, FL), BF16), V((2, EXP, FL, D), BF16),
                V((1, 128), F32),
                V((B * BLK * 8, 64), F32), V((4, NTP, B, BLK, 128), BF16), V((4, NTP, B, BLK, 128), BF16),
                V((4, B, D), BF16), V((4, NTP, B, D), BF16), V((EXP, B, FL), F32), V((EXP, B, FL), BF16), V((B, D), BF16),
                DMA((12,)), DMA((4,)), DMA((2, EXP // GCH)), DMA((2, EXP // GCH)), DMA((2, EXP // DCH)),
                DMA((4, 3)), DMA((4, NTP)), DMA((4, D // NCH, 3)), DMA((4, NTP, D // NCH)), DMA((4, NTP)),
            ],
            compiler_params=pltpu.CompilerParams(collective_id=0, has_side_effects=True, vmem_limit_bytes=66_900_000),
        )(hidden, lengths.reshape(1, B), jnp.transpose(choice, (0, 2, 1)), keys_one, vals_one, keys_two, vals_two,
          g_attn, w_q, w_k, w_v, w_o, g_mlp, jnp.transpose(w_router, (0, 2, 1)), w_gate, w_up, w_down, jnp.asarray(inv_row))
        return (outs[0],) + tuple(o.reshape(B, SEQ, 2, 64) for o in outs[1:])

    return jax.shard_map(local_step, mesh=mesh, in_specs=(P('dp', None), P('dp'), P(None, 'dp', None), seq_spec, seq_spec, seq_spec, seq_spec, P(), col_spec, col_spec, col_spec, P(None, 'tp', None), P(), P(), ff_spec, ff_spec, P(None, None, 'tp', None)), out_specs=(P('dp', None), head_spec, head_spec, head_spec, head_spec), check_vma=False)
```

```python
import functools

import numpy as np

import jax
import jax.numpy as jnp
from jax import lax
from jax.experimental import pallas as pl
from jax.experimental.pallas import tpu as pltpu
from jax.sharding import PartitionSpec as P

EPS = 1e-5
THETA = 1000000.0
MESH = pl.DeviceIdType.MESH
B = 16
D = 1024
SEQ = 64
BLK = 16
NTP = 4
EXP = 32
FL = 128
GCH = 4
DCH = 8
NCH = 512
F32 = jnp.float32
BF16 = jnp.bfloat16


def _norm(h_f, gain_row):
    scale = lax.rsqrt(jnp.mean(h_f * h_f, axis=-1, keepdims=True) + EPS)
    return (h_f * scale * gain_row).astype(BF16)


def _rope(x, cosv, sinv, low):
    rot = jnp.where(low, -pltpu.roll(x, 96, 1), pltpu.roll(x, 32, 1))
    return x * cosv + rot * sinv


def _kernel(hid_h, len_h, cho_h, k1_h, v1_h, k2_h, v2_h, ga_h, wq_h, wk_h, wv_h, wo_h, gm_h, wr_h, wg_h, wu_h, wd_h, inv_h,
            hout, ok1, ov1, ok2, ov2,
            hid, lens, cho, raw, ga, wq, wk, wv, wo, gm, wr, wg, wu, wd, inv,
            spread, snd, kall, xown, xrecv, gexp, act,
            sem_s, sem_raw, sem_g, sem_u, sem_d, send_c, recv_c, send_x, recv_x):
    me = lax.axis_index("tp")
    chip, core = me // 2, me % 2
    partner = chip * 2 + (1 - core)
    cross_a = (1 - chip) * 2 + core
    cross_b = (1 - chip) * 2 + (1 - core)
    peers = (cross_a, cross_b, partner)

    barrier = pltpu.get_barrier_semaphore()
    for p in peers:
        pl.semaphore_signal(barrier, inc=1, device_id={"tp": p}, device_id_type=MESH)

    raw_src = (k1_h, v1_h, k2_h, v2_h)

    def raw_copy(c):
        return pltpu.make_async_copy(raw_src[c], raw.at[c], sem_raw.at[c])

    smalls = ((hid_h, hid), (len_h, lens), (cho_h, cho), (ga_h, ga), (gm_h, gm), (inv_h, inv),
              (wq_h, wq), (wk_h, wk), (wv_h, wv), (wo_h, wo), (wr_h, wr))

    def small_copy(i):
        return pltpu.make_async_copy(smalls[i][0], smalls[i][1], sem_s.at[i])

    def g_copy(l, i):
        sl = pl.ds(i * GCH, GCH)
        return pltpu.make_async_copy(wg_h.at[l, sl], wg.at[l, sl], sem_g.at[l, i])

    def u_copy(l, i):
        sl = pl.ds(i * GCH, GCH)
        return pltpu.make_async_copy(wu_h.at[l, sl], wu.at[l, sl], sem_u.at[l, i])

    def d_copy(l, i):
        sl = pl.ds(i * DCH, DCH)
        return pltpu.make_async_copy(wd_h.at[l, sl], wd.at[l, sl], sem_d.at[l, i])

    raw_copy(0).start()
    raw_copy(1).start()
    for i in range(len(smalls)):
        small_copy(i).start()
    raw_copy(2).start()
    raw_copy(3).start()

    def start_layer(l):
        def gu(i, _):
            g_copy(l, i).start()
            u_copy(l, i).start()
            return 0
        lax.fori_loop(0, EXP // GCH, gu, 0)

        def dn(i, _):
            d_copy(l, i).start()
            return 0
        lax.fori_loop(0, EXP // DCH, dn, 0)

    def cache_copy(c, n):
        return pltpu.make_async_remote_copy(
            src_ref=snd.at[c, peers[n]], dst_ref=kall.at[c, me],
            send_sem=send_c.at[c, n], recv_sem=recv_c.at[c, me],
            device_id={"tp": peers[n]}, device_id_type=MESH)

    def cache_recv(c, n):
        return pltpu.make_async_remote_copy(
            src_ref=snd.at[c, peers[n]], dst_ref=kall.at[c, peers[n]],
            send_sem=send_c.at[c, n], recv_sem=recv_c.at[c, peers[n]],
            device_id={"tp": peers[n]}, device_id_type=MESH)

    def repack(c):
        raw_copy(c).wait()
        spread[...] = raw[c].reshape(B * BLK * 8, 64).astype(F32)
        for p in range(NTP):
            lo = spread[pl.ds(2 * p, B * BLK, stride=8), :]
            hi = spread[pl.ds(2 * p + 1, B * BLK, stride=8), :]
            snd[c, p] = jnp.concatenate([lo, hi], axis=1).astype(BF16).reshape(B, BLK, 128)
        kall[c, me] = snd[c, me]

    repack(0)
    pl.semaphore_wait(barrier, 3)
    for n in range(3):
        cache_copy(0, n).start()
    repack(1)
    for n in range(3):
        cache_copy(1, n).start()
    start_layer(0)
    start_layer(1)
    repack(2)
    repack(3)
    for c in (2, 3):
        cache_copy(c, 2).start()

    for i in range(len(smalls)):
        small_copy(i).wait()

    eye = lax.broadcasted_iota(jnp.int32, (B, B), 0) == lax.broadcasted_iota(jnp.int32, (B, B), 1)
    len_row = jnp.broadcast_to(lens[...].astype(F32), (B, B))
    len_col = jnp.sum(jnp.where(eye, len_row, 0.0), axis=1, keepdims=True)
    len_b = jnp.broadcast_to(len_col, (B, 128))
    angle = len_b * inv[...]
    cosv, sinv = jnp.cos(angle), jnp.sin(angle)
    lane = lax.broadcasted_iota(jnp.int32, (B, 128), 1)
    low = (lane % 64) < 32
    left = lane < 64
    col = lax.broadcasted_iota(jnp.int32, (64, 1024), 1)
    row = lax.broadcasted_iota(jnp.int32, (64, 1024), 0)
    len64 = jnp.concatenate([len_col] * 4, axis=0)
    pos = ((col // 256) * BLK + col % BLK).astype(F32)
    valid = (((col // BLK) % B) == (row % B)) & (pos <= len64)

    h_f = hid[...].astype(F32)

    def insert(c, new):
        new3 = jnp.broadcast_to(new[:, None, :], (B, BLK, 128))
        len3 = jnp.broadcast_to(len_b[:, None, :], (B, BLK, 128))
        pos3 = lax.broadcasted_iota(jnp.int32, (B, BLK, 128), 1).astype(F32)
        for s in range(NTP):
            cur = kall[c, s].astype(F32)
            kall[c, s] = jnp.where(pos3 + float(s * BLK) == len3, new3, cur).astype(BF16)

    def emit(c):
        for s in range(NTP):
            x = kall[c, s].reshape(B * BLK, 128).astype(F32)
            spread[pl.ds(0, B * BLK, stride=2), :] = x[:, :64]
            spread[pl.ds(1, B * BLK, stride=2), :] = x[:, 64:]
            outs[c][:, pl.ds(s * 2 * BLK, 2 * BLK), :] = spread[pl.ds(0, 2 * B * BLK), :].astype(BF16).reshape(B, 2 * BLK, 64)

    def x_copy(step, piece, n):
        sl = pl.ds(piece * NCH, NCH)
        return pltpu.make_async_remote_copy(
            src_ref=xown.at[step, :, sl], dst_ref=xrecv.at[step, me, :, sl],
            send_sem=send_x.at[step, piece, n], recv_sem=recv_x.at[step, me, piece],
            device_id={"tp": peers[n]}, device_id_type=MESH)

    def x_recv(step, piece, n):
        sl = pl.ds(piece * NCH, NCH)
        return pltpu.make_async_remote_copy(
            src_ref=xown.at[step, :, sl], dst_ref=xrecv.at[step, peers[n], :, sl],
            send_sem=send_x.at[step, piece, n], recv_sem=recv_x.at[step, peers[n], piece],
            device_id={"tp": peers[n]}, device_id_type=MESH)

    def x_send(step, piece, val):
        sl = pl.ds(piece * NCH, NCH)
        xown[step, :, sl] = val
        for n in range(3):
            x_copy(step, piece, n).start()
        xrecv[step, me, :, sl] = val

    def x_sum(step):
        for piece in range(D // NCH):
            for n in range(3):
                x_recv(step, piece, n).wait_recv()
        tot = xrecv[step, 0].astype(F32)
        for s in range(1, NTP):
            tot = tot + xrecv[step, s].astype(F32)
        return tot

    outs = (ok1, ov1, ok2, ov2)

    for l in range(2):
        a = _norm(h_f, ga[pl.ds(l, 1), :].astype(F32))
        qf = jnp.dot(a, wq[l], preferred_element_type=F32)
        kf = jnp.dot(a, wk[l], preferred_element_type=F32)
        vf = jnp.dot(a, wv[l], preferred_element_type=F32)
        q0 = _rope(qf[:, :128], cosv, sinv, low)
        q1 = _rope(qf[:, 128:], cosv, sinv, low)
        knew = _rope(kf, cosv, sinv, low).astype(BF16).astype(F32)
        vnew = vf.astype(BF16).astype(F32)
        zero = jnp.zeros_like(q0)
        qrows = jnp.concatenate([
            jnp.where(left, q0, zero), jnp.where(left, pltpu.roll(q0, 64, 1), zero),
            jnp.where(left, zero, pltpu.roll(q1, 64, 1)), jnp.where(left, zero, q1)], axis=0).astype(BF16)
        kc, vc = 2 * l, 2 * l + 1
        for n in range(3):
            cache_recv(kc, n).wait_recv()
        insert(kc, knew)
        k2d = kall[kc].reshape(NTP * B * BLK, 128)
        sc = lax.dot_general(qrows, k2d, (((1,), (1,)), ((), ())), preferred_element_type=F32) * 0.125
        sc = jnp.where(valid, sc, -1e30)
        ex = jnp.exp(sc - jnp.max(sc, axis=1, keepdims=True))
        prob = (ex / jnp.sum(ex, axis=1, keepdims=True)).astype(BF16)
        for n in range(3):
            cache_recv(vc, n).wait_recv()
        insert(vc, vnew)
        if l == 0:
            cache_copy(2, 0).start()
        v2d = kall[vc].reshape(NTP * B * BLK, 128)
        ov = jnp.dot(prob, v2d, preferred_element_type=F32)
        o0 = jnp.where(left, ov[0:16], pltpu.roll(ov[16:32], 64, 1))
        o1 = jnp.where(left, pltpu.roll(ov[32:48], 64, 1), ov[48:64])
        attn = jnp.concatenate([o0, o1], axis=1).astype(BF16)
        for piece in range(D // NCH):
            x_send(2 * l, piece, jnp.dot(attn, wo[l, :, pl.ds(piece * NCH, NCH)], preferred_element_type=F32).astype(BF16))
        emit(kc)
        emit(vc)
        h1 = (h_f + x_sum(2 * l)).astype(BF16).astype(F32)
        if l == 0:
            cache_copy(2, 1).start()
            cache_copy(3, 0).start()
        m = _norm(h1, gm[pl.ds(l, 1), :].astype(F32))

        lg = lax.dot_general(wr[l], m, (((1,), (1,)), ((), ())), preferred_element_type=F32)
        eid = lax.broadcasted_iota(jnp.int32, (EXP, B), 0)
        chosen = eid < 0
        for k in range(8):
            chosen = chosen | (cho[l, pl.ds(k, 1), :] == eid)
        lg = jnp.where(chosen, lg, -jnp.inf)
        ex = jnp.where(chosen, jnp.exp(lg - jnp.max(lg, axis=0, keepdims=True)), 0.0)
        gate_t = ex / jnp.sum(ex, axis=0, keepdims=True)
        gate = gate_t.T
        for e in range(EXP):
            gexp[e] = jnp.broadcast_to(gate[:, e:e + 1], (B, FL))

        def gate_up(i, _):
            g_copy(l, i).wait()
            u_copy(l, i).wait()
            for j in range(GCH):
                e = i * GCH + j
                w = jnp.concatenate([wg[l, e], wu[l, e]], axis=1)
                gu = jnp.dot(m, w, preferred_element_type=F32)
                g, u = gu[:, :FL], gu[:, FL:]
                act[e] = (g * jax.nn.sigmoid(g) * u * gexp[e]).astype(BF16)
            return 0
        lax.fori_loop(0, EXP // GCH, gate_up, 0)

        def dwait(i, _):
            d_copy(l, i).wait()
            return 0
        lax.fori_loop(0, EXP // DCH, dwait, 0)
        for piece in range(D // NCH):
            sl = pl.ds(piece * NCH, NCH)

            def down(i, acc):
                for j in range(4):
                    e = i * 8 + 2 * j
                    lhs = jnp.concatenate([act[e], act[e + 1]], axis=1)
                    rhs = jnp.concatenate([wd[l, e, :, sl], wd[l, e + 1, :, sl]], axis=0)
                    acc = acc + jnp.dot(lhs, rhs, preferred_element_type=F32)
                return acc
            acc = lax.fori_loop(0, EXP // 8, down, jnp.zeros((B, NCH), F32))
            x_send(2 * l + 1, piece, acc.astype(BF16))
        if l == 0:
            cache_copy(3, 1).start()
        h_f = (h1 + x_sum(2 * l + 1)).astype(BF16).astype(F32)

    hout[...] = h_f.astype(BF16)
    for c in range(4):
        for n in range(3):
            cache_copy(c, n).wait_send()
    for step in range(4):
        for piece in range(D // NCH):
            for n in range(3):
                x_copy(step, piece, n).wait_send()


def _store(h, k1, v1, k2, v2, ho, ok1, ov1, ok2, ov2, sem):
    copies = [pltpu.make_async_copy(a, b, sem.at[i])
              for i, (a, b) in enumerate(((k1, ok1), (v1, ov1), (k2, ok2), (v2, ov2), (h, ho)))]
    for c in copies:
        c.start()
    for c in copies:
        c.wait()


def solution(mesh):
    seq_spec = P('dp', 'tp', None, None)
    head_spec = P('dp', None, 'tp', None)
    col_spec = P(None, None, 'tp')
    ff_spec = P(None, None, None, 'tp')
    inv_freq = (THETA ** (-2.0 * np.arange(32, dtype=np.float64) / 64)).astype(np.float32)
    inv_row = np.tile(inv_freq, 4)[None, :]

    def local_step(hidden, lengths, choice, keys_one, vals_one, keys_two, vals_two, g_attn, w_q, w_k, w_v, w_o, g_mlp, w_router, w_gate, w_up, w_down):
        shapes = (jax.ShapeDtypeStruct((B, D), BF16),) + (jax.ShapeDtypeStruct((B, 2 * SEQ, 64), BF16),) * 4
        any_spec = pl.BlockSpec(memory_space=pl.ANY)
        vmem_spec = pl.BlockSpec(memory_space=pltpu.VMEM)
        V = pltpu.VMEM
        DMA = pltpu.SemaphoreType.DMA
        outs = pl.pallas_call(
            _kernel,
            out_shape=tuple(V(s.shape, s.dtype) for s in shapes),
            in_specs=[any_spec] * 18,
            out_specs=(vmem_spec,) * 5,
            scratch_shapes=[
                V((B, D), BF16), V((1, B), jnp.int32), V((2, 8, B), jnp.int32), V((4, B, BLK, 8, 64), BF16),
                V((2, D), BF16), V((2, D, 256), BF16), V((2, D, 128), BF16), V((2, D, 128), BF16), V((2, 256, D), BF16),
                V((2, D), BF16), V((2, EXP, D), BF16), V((2, EXP, D, FL), BF16), V((2, EXP, D, FL), BF16), V((2, EXP, FL, D), BF16),
                V((1, 128), F32),
                V((B * BLK * 8, 64), F32), V((4, NTP, B, BLK, 128), BF16), V((4, NTP, B, BLK, 128), BF16),
                V((4, B, D), BF16), V((4, NTP, B, D), BF16), V((EXP, B, FL), F32), V((EXP, B, FL), BF16),
                DMA((12,)), DMA((4,)), DMA((2, EXP // GCH)), DMA((2, EXP // GCH)), DMA((2, EXP // DCH)),
                DMA((4, 3)), DMA((4, NTP)), DMA((4, D // NCH, 3)), DMA((4, NTP, D // NCH)),
            ],
            compiler_params=pltpu.CompilerParams(collective_id=0, has_side_effects=True, vmem_limit_bytes=64_000_000),
        )(hidden, lengths.reshape(1, B), jnp.transpose(choice, (0, 2, 1)), keys_one, vals_one, keys_two, vals_two,
          g_attn, w_q, w_k, w_v, w_o, g_mlp, jnp.transpose(w_router, (0, 2, 1)), w_gate, w_up, w_down, jnp.asarray(inv_row))
        outs = pl.pallas_call(
            _store,
            out_shape=shapes,
            in_specs=[vmem_spec] * 5,
            out_specs=(any_spec,) * 5,
            scratch_shapes=[DMA((5,))],
        )(*[pltpu.with_memory_space_constraint(o, pltpu.VMEM) for o in outs])
        return (outs[0],) + tuple(o.reshape(B, SEQ, 2, 64) for o in outs[1:])

    return jax.shard_map(local_step, mesh=mesh, in_specs=(P('dp', None), P('dp'), P(None, 'dp', None), seq_spec, seq_spec, seq_spec, seq_spec, P(), col_spec, col_spec, col_spec, P(None, 'tp', None), P(), P(), ff_spec, ff_spec, P(None, None, 'tp', None)), out_specs=(P('dp', None), head_spec, head_spec, head_spec, head_spec), check_vma=False)
```

```python
import functools

import numpy as np

import jax
import jax.numpy as jnp
from jax import lax
from jax.experimental import pallas as pl
from jax.experimental.pallas import tpu as pltpu
from jax.sharding import PartitionSpec as P

EPS = 1e-5
THETA = 1000000.0
MESH = pl.DeviceIdType.MESH
B = 16
D = 1024
SEQ = 64
BLK = 16
NTP = 4
EXP = 32
FL = 128
GCH = 4
DCH = 8
NCH = 512
F32 = jnp.float32
BF16 = jnp.bfloat16


def _norm(h_f, gain_row):
    scale = lax.rsqrt(jnp.mean(h_f * h_f, axis=-1, keepdims=True) + EPS)
    return (h_f * scale * gain_row).astype(BF16)


def _rope(x, cosv, sinv, low):
    rot = jnp.where(low, -pltpu.roll(x, 96, 1), pltpu.roll(x, 32, 1))
    return x * cosv + rot * sinv


def _kernel(hid_h, len_h, cho_h, k1_h, v1_h, k2_h, v2_h, ga_h, wq_h, wk_h, wv_h, wo_h, gm_h, wr_h, wg_h, wu_h, wd_h, inv_h,
            hout, ok1, ov1, ok2, ov2,
            hid, lens, cho, raw, ga, wq, wk, wv, wo, gm, wr, wg, wu, wd, inv,
            spread, snd, kall, xown, xrecv, gexp, act,
            sem_s, sem_raw, sem_g, sem_u, sem_d, send_c, recv_c, send_x, recv_x):
    me = lax.axis_index("tp")
    chip, core = me // 2, me % 2
    partner = chip * 2 + (1 - core)
    cross_a = (1 - chip) * 2 + core
    cross_b = (1 - chip) * 2 + (1 - core)
    peers = (cross_a, cross_b, partner)

    barrier = pltpu.get_barrier_semaphore()
    for p in peers:
        pl.semaphore_signal(barrier, inc=1, device_id={"tp": p}, device_id_type=MESH)

    raw_src = (k1_h, v1_h, k2_h, v2_h)

    def raw_copy(c):
        return pltpu.make_async_copy(raw_src[c], raw.at[c], sem_raw.at[c])

    smalls = ((hid_h, hid), (len_h, lens), (cho_h, cho), (ga_h, ga), (gm_h, gm), (inv_h, inv),
              (wq_h, wq), (wk_h, wk), (wv_h, wv), (wo_h, wo), (wr_h, wr))

    def small_copy(i):
        return pltpu.make_async_copy(smalls[i][0], smalls[i][1], sem_s.at[i])

    def g_copy(l, i):
        sl = pl.ds(i * GCH, GCH)
        return pltpu.make_async_copy(wg_h.at[l, sl], wg.at[l, sl], sem_g.at[l, i])

    def u_copy(l, i):
        sl = pl.ds(i * GCH, GCH)
        return pltpu.make_async_copy(wu_h.at[l, sl], wu.at[l, sl], sem_u.at[l, i])

    def d_copy(l, i):
        sl = pl.ds(i * DCH, DCH)
        return pltpu.make_async_copy(wd_h.at[l, sl], wd.at[l, sl], sem_d.at[l, i])

    raw_copy(0).start()
    raw_copy(1).start()
    for i in range(len(smalls)):
        small_copy(i).start()
    raw_copy(2).start()
    raw_copy(3).start()

    def start_layer(l):
        def gu(i, _):
            g_copy(l, i).start()
            u_copy(l, i).start()
            return 0
        lax.fori_loop(0, EXP // GCH, gu, 0)

        def dn(i, _):
            d_copy(l, i).start()
            return 0
        lax.fori_loop(0, EXP // DCH, dn, 0)

    def cache_copy(c, n):
        return pltpu.make_async_remote_copy(
            src_ref=snd.at[c, peers[n]], dst_ref=kall.at[c, me],
            send_sem=send_c.at[c, n], recv_sem=recv_c.at[c, me],
            device_id={"tp": peers[n]}, device_id_type=MESH)

    def cache_recv(c, n):
        return pltpu.make_async_remote_copy(
            src_ref=snd.at[c, peers[n]], dst_ref=kall.at[c, peers[n]],
            send_sem=send_c.at[c, n], recv_sem=recv_c.at[c, peers[n]],
            device_id={"tp": peers[n]}, device_id_type=MESH)

    def repack(c):
        raw_copy(c).wait()
        spread[...] = raw[c].reshape(B * BLK * 8, 64).astype(F32)
        for p in range(NTP):
            lo = spread[pl.ds(2 * p, B * BLK, stride=8), :]
            hi = spread[pl.ds(2 * p + 1, B * BLK, stride=8), :]
            snd[c, p] = jnp.concatenate([lo, hi], axis=1).astype(BF16).reshape(B, BLK, 128)
        kall[c, me] = snd[c, me]

    start_layer(0)
    start_layer(1)
    repack(0)
    pl.semaphore_wait(barrier, 3)
    for n in range(3):
        cache_copy(0, n).start()
    repack(1)
    for n in range(3):
        cache_copy(1, n).start()
    repack(2)
    repack(3)
    for c in (2, 3):
        cache_copy(c, 2).start()

    for i in range(len(smalls)):
        small_copy(i).wait()

    eye = lax.broadcasted_iota(jnp.int32, (B, B), 0) == lax.broadcasted_iota(jnp.int32, (B, B), 1)
    len_row = jnp.broadcast_to(lens[...].astype(F32), (B, B))
    len_col = jnp.sum(jnp.where(eye, len_row, 0.0), axis=1, keepdims=True)
    len_b = jnp.broadcast_to(len_col, (B, 128))
    angle = len_b * inv[...]
    cosv, sinv = jnp.cos(angle), jnp.sin(angle)
    lane = lax.broadcasted_iota(jnp.int32, (B, 128), 1)
    low = (lane % 64) < 32
    left = lane < 64
    col = lax.broadcasted_iota(jnp.int32, (64, 1024), 1)
    row = lax.broadcasted_iota(jnp.int32, (64, 1024), 0)
    len64 = jnp.concatenate([len_col] * 4, axis=0)
    pos = ((col // 256) * BLK + col % BLK).astype(F32)
    valid = (((col // BLK) % B) == (row % B)) & (pos <= len64)

    h_f = hid[...].astype(F32)

    def insert(c, new):
        new3 = jnp.broadcast_to(new[:, None, :], (B, BLK, 128))
        len3 = jnp.broadcast_to(len_b[:, None, :], (B, BLK, 128))
        pos3 = lax.broadcasted_iota(jnp.int32, (B, BLK, 128), 1).astype(F32)
        for s in range(NTP):
            cur = kall[c, s].astype(F32)
            kall[c, s] = jnp.where(pos3 + float(s * BLK) == len3, new3, cur).astype(BF16)

    def emit(c):
        for s in range(NTP):
            x = kall[c, s].reshape(B * BLK, 128).astype(F32)
            spread[pl.ds(0, B * BLK, stride=2), :] = x[:, :64]
            spread[pl.ds(1, B * BLK, stride=2), :] = x[:, 64:]
            outs[c][:, pl.ds(s * 2 * BLK, 2 * BLK), :] = spread[pl.ds(0, 2 * B * BLK), :].astype(BF16).reshape(B, 2 * BLK, 64)

    def x_copy(step, piece, n):
        sl = pl.ds(piece * NCH, NCH)
        return pltpu.make_async_remote_copy(
            src_ref=xown.at[step, :, sl], dst_ref=xrecv.at[step, me, :, sl],
            send_sem=send_x.at[step, piece, n], recv_sem=recv_x.at[step, me, piece],
            device_id={"tp": peers[n]}, device_id_type=MESH)

    def x_recv(step, piece, n):
        sl = pl.ds(piece * NCH, NCH)
        return pltpu.make_async_remote_copy(
            src_ref=xown.at[step, :, sl], dst_ref=xrecv.at[step, peers[n], :, sl],
            send_sem=send_x.at[step, piece, n], recv_sem=recv_x.at[step, peers[n], piece],
            device_id={"tp": peers[n]}, device_id_type=MESH)

    def x_send(step, piece, val):
        sl = pl.ds(piece * NCH, NCH)
        xown[step, :, sl] = val
        for n in range(3):
            x_copy(step, piece, n).start()
        xrecv[step, me, :, sl] = val

    def x_sum(step):
        for piece in range(D // NCH):
            for n in range(3):
                x_recv(step, piece, n).wait_recv()
        tot = xrecv[step, 0].astype(F32)
        for s in range(1, NTP):
            tot = tot + xrecv[step, s].astype(F32)
        return tot

    outs = (ok1, ov1, ok2, ov2)

    for l in range(2):
        a = _norm(h_f, ga[pl.ds(l, 1), :].astype(F32))
        qf = jnp.dot(a, wq[l], preferred_element_type=F32)
        kf = jnp.dot(a, wk[l], preferred_element_type=F32)
        vf = jnp.dot(a, wv[l], preferred_element_type=F32)
        q0 = _rope(qf[:, :128], cosv, sinv, low)
        q1 = _rope(qf[:, 128:], cosv, sinv, low)
        knew = _rope(kf, cosv, sinv, low).astype(BF16).astype(F32)
        vnew = vf.astype(BF16).astype(F32)
        zero = jnp.zeros_like(q0)
        qrows = jnp.concatenate([
            jnp.where(left, q0, zero), jnp.where(left, pltpu.roll(q0, 64, 1), zero),
            jnp.where(left, zero, pltpu.roll(q1, 64, 1)), jnp.where(left, zero, q1)], axis=0).astype(BF16)
        kc, vc = 2 * l, 2 * l + 1
        for n in range(3):
            cache_recv(kc, n).wait_recv()
        insert(kc, knew)
        k2d = kall[kc].reshape(NTP * B * BLK, 128)
        sc = lax.dot_general(qrows, k2d, (((1,), (1,)), ((), ())), preferred_element_type=F32) * 0.125
        sc = jnp.where(valid, sc, -1e30)
        ex = jnp.exp(sc - jnp.max(sc, axis=1, keepdims=True))
        prob = (ex / jnp.sum(ex, axis=1, keepdims=True)).astype(BF16)
        for n in range(3):
            cache_recv(vc, n).wait_recv()
        insert(vc, vnew)
        if l == 0:
            cache_copy(2, 0).start()
        v2d = kall[vc].reshape(NTP * B * BLK, 128)
        ov = jnp.dot(prob, v2d, preferred_element_type=F32)
        o0 = jnp.where(left, ov[0:16], pltpu.roll(ov[16:32], 64, 1))
        o1 = jnp.where(left, pltpu.roll(ov[32:48], 64, 1), ov[48:64])
        attn = jnp.concatenate([o0, o1], axis=1).astype(BF16)
        for piece in range(D // NCH):
            x_send(2 * l, piece, jnp.dot(attn, wo[l, :, pl.ds(piece * NCH, NCH)], preferred_element_type=F32).astype(BF16))
        emit(kc)
        emit(vc)
        h1 = (h_f + x_sum(2 * l)).astype(BF16).astype(F32)
        if l == 0:
            cache_copy(2, 1).start()
            cache_copy(3, 0).start()
        m = _norm(h1, gm[pl.ds(l, 1), :].astype(F32))

        lg = lax.dot_general(wr[l], m, (((1,), (1,)), ((), ())), preferred_element_type=F32)
        eid = lax.broadcasted_iota(jnp.int32, (EXP, B), 0)
        chosen = eid < 0
        for k in range(8):
            chosen = chosen | (cho[l, pl.ds(k, 1), :] == eid)
        lg = jnp.where(chosen, lg, -jnp.inf)
        ex = jnp.where(chosen, jnp.exp(lg - jnp.max(lg, axis=0, keepdims=True)), 0.0)
        gate_t = ex / jnp.sum(ex, axis=0, keepdims=True)
        gate = gate_t.T
        for e in range(EXP):
            gexp[e] = jnp.broadcast_to(gate[:, e:e + 1], (B, FL))

        def gate_up(i, _):
            g_copy(l, i).wait()
            u_copy(l, i).wait()
            for j in range(GCH):
                e = i * GCH + j
                w = jnp.concatenate([wg[l, e], wu[l, e]], axis=1)
                gu = jnp.dot(m, w, preferred_element_type=F32)
                g, u = gu[:, :FL], gu[:, FL:]
                act[e] = (g * jax.nn.sigmoid(g) * u * gexp[e]).astype(BF16)
            return 0
        lax.fori_loop(0, EXP // GCH, gate_up, 0)

        def dwait(i, _):
            d_copy(l, i).wait()
            return 0
        lax.fori_loop(0, EXP // DCH, dwait, 0)
        for piece in range(D // NCH):
            sl = pl.ds(piece * NCH, NCH)

            def down(i, acc):
                for j in range(4):
                    e = i * 8 + 2 * j
                    lhs = jnp.concatenate([act[e], act[e + 1]], axis=1)
                    rhs = jnp.concatenate([wd[l, e, :, sl], wd[l, e + 1, :, sl]], axis=0)
                    acc = acc + jnp.dot(lhs, rhs, preferred_element_type=F32)
                return acc
            acc = lax.fori_loop(0, EXP // 8, down, jnp.zeros((B, NCH), F32))
            x_send(2 * l + 1, piece, acc.astype(BF16))
        if l == 0:
            cache_copy(3, 1).start()
        h_f = (h1 + x_sum(2 * l + 1)).astype(BF16).astype(F32)

    hout[...] = h_f.astype(BF16)
    for c in range(4):
        for n in range(3):
            cache_copy(c, n).wait_send()
    for step in range(4):
        for piece in range(D // NCH):
            for n in range(3):
                x_copy(step, piece, n).wait_send()


def _store(h, k1, v1, k2, v2, ho, ok1, ov1, ok2, ov2, sem):
    copies = [pltpu.make_async_copy(a, b, sem.at[i])
              for i, (a, b) in enumerate(((k1, ok1), (v1, ov1), (k2, ok2), (v2, ov2), (h, ho)))]
    for c in copies:
        c.start()
    for c in copies:
        c.wait()


def solution(mesh):
    seq_spec = P('dp', 'tp', None, None)
    head_spec = P('dp', None, 'tp', None)
    col_spec = P(None, None, 'tp')
    ff_spec = P(None, None, None, 'tp')
    inv_freq = (THETA ** (-2.0 * np.arange(32, dtype=np.float64) / 64)).astype(np.float32)
    inv_row = np.tile(inv_freq, 4)[None, :]

    def local_step(hidden, lengths, choice, keys_one, vals_one, keys_two, vals_two, g_attn, w_q, w_k, w_v, w_o, g_mlp, w_router, w_gate, w_up, w_down):
        shapes = (jax.ShapeDtypeStruct((B, D), BF16),) + (jax.ShapeDtypeStruct((B, 2 * SEQ, 64), BF16),) * 4
        any_spec = pl.BlockSpec(memory_space=pl.ANY)
        vmem_spec = pl.BlockSpec(memory_space=pltpu.VMEM)
        V = pltpu.VMEM
        DMA = pltpu.SemaphoreType.DMA
        outs = pl.pallas_call(
            _kernel,
            out_shape=tuple(V(s.shape, s.dtype) for s in shapes),
            in_specs=[any_spec] * 18,
            out_specs=(vmem_spec,) * 5,
            scratch_shapes=[
                V((B, D), BF16), V((1, B), jnp.int32), V((2, 8, B), jnp.int32), V((4, B, BLK, 8, 64), BF16),
                V((2, D), BF16), V((2, D, 256), BF16), V((2, D, 128), BF16), V((2, D, 128), BF16), V((2, 256, D), BF16),
                V((2, D), BF16), V((2, EXP, D), BF16), V((2, EXP, D, FL), BF16), V((2, EXP, D, FL), BF16), V((2, EXP, FL, D), BF16),
                V((1, 128), F32),
                V((B * BLK * 8, 64), F32), V((4, NTP, B, BLK, 128), BF16), V((4, NTP, B, BLK, 128), BF16),
                V((4, B, D), BF16), V((4, NTP, B, D), BF16), V((EXP, B, FL), F32), V((EXP, B, FL), BF16),
                DMA((12,)), DMA((4,)), DMA((2, EXP // GCH)), DMA((2, EXP // GCH)), DMA((2, EXP // DCH)),
                DMA((4, 3)), DMA((4, NTP)), DMA((4, D // NCH, 3)), DMA((4, NTP, D // NCH)),
            ],
            compiler_params=pltpu.CompilerParams(collective_id=0, has_side_effects=True, vmem_limit_bytes=64_000_000),
        )(hidden, lengths.reshape(1, B), jnp.transpose(choice, (0, 2, 1)), keys_one, vals_one, keys_two, vals_two,
          g_attn, w_q, w_k, w_v, w_o, g_mlp, jnp.transpose(w_router, (0, 2, 1)), w_gate, w_up, w_down, jnp.asarray(inv_row))
        outs = pl.pallas_call(
            _store,
            out_shape=shapes,
            in_specs=[vmem_spec] * 5,
            out_specs=(any_spec,) * 5,
            scratch_shapes=[DMA((5,))],
        )(*[pltpu.with_memory_space_constraint(o, pltpu.VMEM) for o in outs])
        return (outs[0],) + tuple(o.reshape(B, SEQ, 2, 64) for o in outs[1:])

    return jax.shard_map(local_step, mesh=mesh, in_specs=(P('dp', None), P('dp'), P(None, 'dp', None), seq_spec, seq_spec, seq_spec, seq_spec, P(), col_spec, col_spec, col_spec, P(None, 'tp', None), P(), P(), ff_spec, ff_spec, P(None, None, 'tp', None)), out_specs=(P('dp', None), head_spec, head_spec, head_spec, head_spec), check_vma=False)
```

```python
import functools

import numpy as np

import jax
import jax.numpy as jnp
from jax import lax
from jax.experimental import pallas as pl
from jax.experimental.pallas import tpu as pltpu
from jax.sharding import PartitionSpec as P

EPS = 1e-5
THETA = 1000000.0
MESH = pl.DeviceIdType.MESH
B = 16
D = 1024
SEQ = 64
BLK = 16
NTP = 4
EXP = 32
FL = 128
GCH = 4
DCH = 8
PIECES = (((0, 1024),), ((0, 512), (512, 512)))
NP = 2
F32 = jnp.float32
BF16 = jnp.bfloat16


def _norm(h_f, gain_row):
    scale = lax.rsqrt(jnp.mean(h_f * h_f, axis=-1, keepdims=True) + EPS)
    return (h_f * scale * gain_row).astype(BF16)


def _rope(x, cosv, sinv, low):
    rot = jnp.where(low, -pltpu.roll(x, 96, 1), pltpu.roll(x, 32, 1))
    return x * cosv + rot * sinv


def _kernel(hid_h, len_h, cho_h, k1_h, v1_h, k2_h, v2_h, ga_h, wq_h, wk_h, wv_h, wo_h, gm_h, wr_h, wg_h, wu_h, wd_h, inv_h,
            hout, ok1, ov1, ok2, ov2,
            hid, lens, cho, raw, ga, wq, wk, wv, wo, gm, wr, wg, wu, wd, inv,
            spread, snd, kall, xown, xrecv, act,
            sem_s, sem_raw, sem_g, sem_u, sem_d, send_c, recv_c, send_x, recv_x):
    me = lax.axis_index("tp")
    chip, core = me // 2, me % 2
    partner = chip * 2 + (1 - core)
    cross_a = (1 - chip) * 2 + core
    cross_b = (1 - chip) * 2 + (1 - core)
    peers = (cross_a, cross_b, partner)

    barrier = pltpu.get_barrier_semaphore()
    for p in peers:
        pl.semaphore_signal(barrier, inc=1, device_id={"tp": p}, device_id_type=MESH)

    raw_src = (k1_h, v1_h, k2_h, v2_h)

    def raw_copy(c):
        return pltpu.make_async_copy(raw_src[c], raw.at[c], sem_raw.at[c])

    smalls = ((hid_h, hid), (len_h, lens), (cho_h, cho), (ga_h, ga), (gm_h, gm), (inv_h, inv),
              (wq_h, wq), (wk_h, wk), (wv_h, wv), (wo_h, wo), (wr_h, wr))

    def small_copy(i):
        return pltpu.make_async_copy(smalls[i][0], smalls[i][1], sem_s.at[i])

    def g_copy(l, i):
        sl = pl.ds(i * GCH, GCH)
        return pltpu.make_async_copy(wg_h.at[l, sl], wg.at[l, sl], sem_g.at[l, i])

    def u_copy(l, i):
        sl = pl.ds(i * GCH, GCH)
        return pltpu.make_async_copy(wu_h.at[l, sl], wu.at[l, sl], sem_u.at[l, i])

    def d_copy(l, i):
        sl = pl.ds(i * DCH, DCH)
        return pltpu.make_async_copy(wd_h.at[l, sl], wd.at[l, sl], sem_d.at[l, i])

    raw_copy(0).start()
    raw_copy(1).start()
    for i in range(len(smalls)):
        small_copy(i).start()
    raw_copy(2).start()
    raw_copy(3).start()

    def start_layer(l):
        def gu(i, _):
            g_copy(l, i).start()
            u_copy(l, i).start()
            return 0
        lax.fori_loop(0, EXP // GCH, gu, 0)

        def dn(i, _):
            d_copy(l, i).start()
            return 0
        lax.fori_loop(0, EXP // DCH, dn, 0)

    def cache_copy(c, n):
        return pltpu.make_async_remote_copy(
            src_ref=snd.at[c, peers[n]], dst_ref=kall.at[c, me],
            send_sem=send_c.at[c, n], recv_sem=recv_c.at[c, me],
            device_id={"tp": peers[n]}, device_id_type=MESH)

    def cache_recv(c, n):
        return pltpu.make_async_remote_copy(
            src_ref=snd.at[c, peers[n]], dst_ref=kall.at[c, peers[n]],
            send_sem=send_c.at[c, n], recv_sem=recv_c.at[c, peers[n]],
            device_id={"tp": peers[n]}, device_id_type=MESH)

    def repack(c):
        raw_copy(c).wait()
        spread[...] = raw[c].reshape(B * BLK * 8, 64).astype(F32)
        for p in range(NTP):
            lo = spread[pl.ds(2 * p, B * BLK, stride=8), :]
            hi = spread[pl.ds(2 * p + 1, B * BLK, stride=8), :]
            snd[c, p] = jnp.concatenate([lo, hi], axis=1).astype(BF16).reshape(B, BLK, 128)
        kall[c, me] = snd[c, me]

    start_layer(0)
    start_layer(1)
    repack(0)
    pl.semaphore_wait(barrier, 3)
    for n in range(3):
        cache_copy(0, n).start()
    repack(1)
    for n in range(3):
        cache_copy(1, n).start()
    repack(2)
    repack(3)
    for c in (2, 3):
        cache_copy(c, 2).start()

    for i in range(len(smalls)):
        small_copy(i).wait()

    eye = lax.broadcasted_iota(jnp.int32, (B, B), 0) == lax.broadcasted_iota(jnp.int32, (B, B), 1)
    len_row = jnp.broadcast_to(lens[...].astype(F32), (B, B))
    len_col = jnp.sum(jnp.where(eye, len_row, 0.0), axis=1, keepdims=True)
    len_b = jnp.broadcast_to(len_col, (B, 128))
    angle = len_b * inv[...]
    cosv, sinv = jnp.cos(angle), jnp.sin(angle)
    lane = lax.broadcasted_iota(jnp.int32, (B, 128), 1)
    low = (lane % 64) < 32
    left = lane < 64
    col = lax.broadcasted_iota(jnp.int32, (64, 1024), 1)
    row = lax.broadcasted_iota(jnp.int32, (64, 1024), 0)
    len64 = jnp.concatenate([len_col] * 4, axis=0)
    pos = ((col // 256) * BLK + col % BLK).astype(F32)
    valid = (((col // BLK) % B) == (row % B)) & (pos < len64)

    h_f = hid[...].astype(F32)

    def emit(c, new):
        new3 = jnp.broadcast_to(new[:, None, :], (B, BLK, 128))
        len3 = jnp.broadcast_to(len_b[:, None, :], (B, BLK, 128))
        pos3 = lax.broadcasted_iota(jnp.int32, (B, BLK, 128), 1).astype(F32)
        for s in range(NTP):
            x = jnp.where(pos3 + float(s * BLK) == len3, new3, kall[c, s].astype(F32)).reshape(B * BLK, 128)
            spread[pl.ds(0, B * BLK, stride=2), :] = x[:, :64]
            spread[pl.ds(1, B * BLK, stride=2), :] = x[:, 64:]
            outs[c][:, pl.ds(s * 2 * BLK, 2 * BLK), :] = spread[pl.ds(0, 2 * B * BLK), :].astype(BF16).reshape(B, 2 * BLK, 64)

    def x_desc(step, piece, n, slot):
        sl = pl.ds(*PIECES[step % 2][piece])
        return pltpu.make_async_remote_copy(
            src_ref=xown.at[step, :, sl], dst_ref=xrecv.at[step, slot, :, sl],
            send_sem=send_x.at[step, piece, n], recv_sem=recv_x.at[step, slot, piece],
            device_id={"tp": peers[n]}, device_id_type=MESH)

    def x_send(step, piece, val):
        sl = pl.ds(*PIECES[step % 2][piece])
        xown[step, :, sl] = val
        for n in range(3):
            x_desc(step, piece, n, me).start()
        xrecv[step, me, :, sl] = val

    def x_sum(step):
        for piece in range(len(PIECES[step % 2])):
            for n in range(3):
                x_desc(step, piece, n, peers[n]).wait_recv()
        tot = xrecv[step, 0].astype(F32)
        for s in range(1, NTP):
            tot = tot + xrecv[step, s].astype(F32)
        return tot

    outs = (ok1, ov1, ok2, ov2)

    for l in range(2):
        a = _norm(h_f, ga[pl.ds(l, 1), :].astype(F32))
        qf = jnp.dot(a, wq[l], preferred_element_type=F32)
        kf = jnp.dot(a, wk[l], preferred_element_type=F32)
        vf = jnp.dot(a, wv[l], preferred_element_type=F32)
        q0 = _rope(qf[:, :128], cosv, sinv, low)
        q1 = _rope(qf[:, 128:], cosv, sinv, low)
        knew = _rope(kf, cosv, sinv, low).astype(BF16).astype(F32)
        vnew = vf.astype(BF16).astype(F32)
        zero = jnp.zeros_like(q0)
        qrows = jnp.concatenate([
            jnp.where(left, q0, zero), jnp.where(left, pltpu.roll(q0, 64, 1), zero),
            jnp.where(left, zero, pltpu.roll(q1, 64, 1)), jnp.where(left, zero, q1)], axis=0).astype(BF16)
        kc, vc = 2 * l, 2 * l + 1
        for n in range(3):
            cache_recv(kc, n).wait_recv()
        k2d = kall[kc].reshape(NTP * B * BLK, 128)
        sc = lax.dot_general(qrows, k2d, (((1,), (1,)), ((), ())), preferred_element_type=F32) * 0.125
        sc = jnp.where(valid, sc, -1e30)
        ns = jnp.sum(qrows.astype(F32) * jnp.concatenate([knew] * 4, axis=0), axis=1, keepdims=True) * 0.125
        top = jnp.maximum(jnp.max(sc, axis=1, keepdims=True), ns)
        ex, nex = jnp.exp(sc - top), jnp.exp(ns - top)
        den = jnp.sum(ex, axis=1, keepdims=True) + nex
        prob = (ex / den).astype(BF16)
        nprob = (nex / den).astype(BF16).astype(F32)
        for n in range(3):
            cache_recv(vc, n).wait_recv()
        v2d = kall[vc].reshape(NTP * B * BLK, 128)
        ov = jnp.dot(prob, v2d, preferred_element_type=F32) + nprob * jnp.concatenate([vnew] * 4, axis=0)
        o0 = jnp.where(left, ov[0:16], pltpu.roll(ov[16:32], 64, 1))
        o1 = jnp.where(left, pltpu.roll(ov[32:48], 64, 1), ov[48:64])
        attn = jnp.concatenate([o0, o1], axis=1).astype(BF16)
        x_send(2 * l, 0, jnp.dot(attn, wo[l], preferred_element_type=F32).astype(BF16))
        if l == 0:
            cache_copy(2, 0).start()
            cache_copy(2, 1).start()
            cache_copy(3, 0).start()
        emit(kc, knew)
        emit(vc, vnew)
        h1 = (h_f + x_sum(2 * l)).astype(BF16).astype(F32)
        m = _norm(h1, gm[pl.ds(l, 1), :].astype(F32))

        lg = lax.dot_general(wr[l], m, (((1,), (1,)), ((), ())), preferred_element_type=F32)
        eid = lax.broadcasted_iota(jnp.int32, (EXP, B), 0)
        chosen = eid < 0
        for k in range(8):
            chosen = chosen | (cho[l, pl.ds(k, 1), :] == eid)
        lg = jnp.where(chosen, lg, -jnp.inf)
        ex = jnp.where(chosen, jnp.exp(lg - jnp.max(lg, axis=0, keepdims=True)), 0.0)
        gate_t = ex / jnp.sum(ex, axis=0, keepdims=True)
        gate = gate_t.T
        for i in range(EXP // GCH):
            g_copy(l, i).wait()
            u_copy(l, i).wait()
        for i in range(EXP // DCH):
            d_copy(l, i).wait()
        for e in range(EXP):
            w = jnp.concatenate([wg[l, e], wu[l, e]], axis=1)
            gu = jnp.dot(m, w, preferred_element_type=F32)
            g, u = gu[:, :FL], gu[:, FL:]
            act[:, pl.ds(e * FL, FL)] = (g * jax.nn.sigmoid(g) * u * jnp.broadcast_to(gate[:, e:e + 1], (B, FL))).astype(BF16)
        for piece, (first, width) in enumerate(PIECES[1]):
            acc = jnp.zeros((B, width), F32)
            for e in range(0, EXP, 2):
                rhs = wd[l, pl.ds(e, 2), :, pl.ds(first, width)].reshape(2 * FL, width)
                acc = acc + jnp.dot(act[:, pl.ds(e * FL, 2 * FL)], rhs, preferred_element_type=F32)
            x_send(2 * l + 1, piece, acc.astype(BF16))
        if l == 0:
            cache_copy(3, 1).start()
        h_f = (h1 + x_sum(2 * l + 1)).astype(BF16).astype(F32)

    hout[...] = h_f.astype(BF16)
    for c in range(4):
        for n in range(3):
            cache_copy(c, n).wait_send()
    for step in range(4):
        for piece in range(len(PIECES[step % 2])):
            for n in range(3):
                x_desc(step, piece, n, me).wait_send()


def _store(h, k1, v1, k2, v2, ho, ok1, ov1, ok2, ov2, sem):
    copies = [pltpu.make_async_copy(a, b, sem.at[i])
              for i, (a, b) in enumerate(((k1, ok1), (v1, ov1), (k2, ok2), (v2, ov2), (h, ho)))]
    for c in copies:
        c.start()
    for c in copies:
        c.wait()


def solution(mesh):
    seq_spec = P('dp', 'tp', None, None)
    head_spec = P('dp', None, 'tp', None)
    col_spec = P(None, None, 'tp')
    ff_spec = P(None, None, None, 'tp')
    inv_freq = (THETA ** (-2.0 * np.arange(32, dtype=np.float64) / 64)).astype(np.float32)
    inv_row = np.tile(inv_freq, 4)[None, :]

    def local_step(hidden, lengths, choice, keys_one, vals_one, keys_two, vals_two, g_attn, w_q, w_k, w_v, w_o, g_mlp, w_router, w_gate, w_up, w_down):
        shapes = (jax.ShapeDtypeStruct((B, D), BF16),) + (jax.ShapeDtypeStruct((B, 2 * SEQ, 64), BF16),) * 4
        any_spec = pl.BlockSpec(memory_space=pl.ANY)
        vmem_spec = pl.BlockSpec(memory_space=pltpu.VMEM)
        V = pltpu.VMEM
        DMA = pltpu.SemaphoreType.DMA
        outs = pl.pallas_call(
            _kernel,
            out_shape=tuple(V(s.shape, s.dtype) for s in shapes),
            in_specs=[any_spec] * 18,
            out_specs=(vmem_spec,) * 5,
            scratch_shapes=[
                V((B, D), BF16), V((1, B), jnp.int32), V((2, 8, B), jnp.int32), V((4, B, BLK, 8, 64), BF16),
                V((2, D), BF16), V((2, D, 256), BF16), V((2, D, 128), BF16), V((2, D, 128), BF16), V((2, 256, D), BF16),
                V((2, D), BF16), V((2, EXP, D), BF16), V((2, EXP, D, FL), BF16), V((2, EXP, D, FL), BF16), V((2, EXP, FL, D), BF16),
                V((1, 128), F32),
                V((B * BLK * 8, 64), F32), V((4, NTP, B, BLK, 128), BF16), V((4, NTP, B, BLK, 128), BF16),
                V((4, B, D), BF16), V((4, NTP, B, D), BF16), V((B, EXP * FL), BF16),
                DMA((12,)), DMA((4,)), DMA((2, EXP // GCH)), DMA((2, EXP // GCH)), DMA((2, EXP // DCH)),
                DMA((4, 3)), DMA((4, NTP)), DMA((4, NP, 3)), DMA((4, NTP, NP)),
            ],
            compiler_params=pltpu.CompilerParams(collective_id=0, has_side_effects=True, vmem_limit_bytes=64_000_000),
        )(hidden, lengths.reshape(1, B), jnp.transpose(choice, (0, 2, 1)), keys_one, vals_one, keys_two, vals_two,
          g_attn, w_q, w_k, w_v, w_o, g_mlp, jnp.transpose(w_router, (0, 2, 1)), w_gate, w_up, w_down, jnp.asarray(inv_row))
        outs = pl.pallas_call(
            _store,
            out_shape=shapes,
            in_specs=[vmem_spec] * 5,
            out_specs=(any_spec,) * 5,
            scratch_shapes=[DMA((5,))],
        )(*[pltpu.with_memory_space_constraint(o, pltpu.VMEM) for o in outs])
        return (outs[0],) + tuple(o.reshape(B, SEQ, 2, 64) for o in outs[1:])

    return jax.shard_map(local_step, mesh=mesh, in_specs=(P('dp', None), P('dp'), P(None, 'dp', None), seq_spec, seq_spec, seq_spec, seq_spec, P(), col_spec, col_spec, col_spec, P(None, 'tp', None), P(), P(), ff_spec, ff_spec, P(None, None, 'tp', None)), out_specs=(P('dp', None), head_spec, head_spec, head_spec, head_spec), check_vma=False)
```

```python
import functools

import numpy as np

import jax
import jax.numpy as jnp
from jax import lax
from jax.experimental import pallas as pl
from jax.experimental.pallas import tpu as pltpu
from jax.sharding import PartitionSpec as P

EPS = 1e-5
THETA = 1000000.0
MESH = pl.DeviceIdType.MESH
B = 16
D = 1024
SEQ = 64
BLK = 16
NTP = 4
EXP = 32
FL = 128
GCH = 4
DCH = 8
PIECES = (((0, 1024),), ((0, 512), (512, 512)))
NP = 2
F32 = jnp.float32
BF16 = jnp.bfloat16


def _norm(h_f, gain_row):
    scale = lax.rsqrt(jnp.mean(h_f * h_f, axis=-1, keepdims=True) + EPS)
    return (h_f * scale * gain_row).astype(BF16)


def _rope(x, cosv, sinv, low):
    rot = jnp.where(low, -pltpu.roll(x, 96, 1), pltpu.roll(x, 32, 1))
    return x * cosv + rot * sinv


def _kernel(hid_h, len_h, cho_h, k1_h, v1_h, k2_h, v2_h, ga_h, wq_h, wk_h, wv_h, wo_h, gm_h, wr_h, wg_h, wu_h, wd_h, inv_h,
            hout, ok1, ov1, ok2, ov2,
            hid, lens, cho, raw, ga, wq, wk, wv, wo, gm, wr, wg, wu, wd, inv,
            spread, snd, kall, xown, xrecv, act,
            sem_s, sem_raw, sem_g, sem_u, sem_d, send_c, recv_c, send_x, recv_x):
    me = lax.axis_index("tp")
    chip, core = me // 2, me % 2
    partner = chip * 2 + (1 - core)
    cross_a = (1 - chip) * 2 + core
    cross_b = (1 - chip) * 2 + (1 - core)
    peers = (cross_a, cross_b, partner)

    barrier = pltpu.get_barrier_semaphore()
    for p in peers:
        pl.semaphore_signal(barrier, inc=1, device_id={"tp": p}, device_id_type=MESH)

    raw_src = (k1_h, v1_h, k2_h, v2_h)

    def raw_copy(c):
        return pltpu.make_async_copy(raw_src[c], raw.at[c], sem_raw.at[c])

    smalls = ((hid_h, hid), (len_h, lens), (cho_h, cho), (ga_h, ga), (gm_h, gm), (inv_h, inv),
              (wq_h, wq), (wk_h, wk), (wv_h, wv), (wo_h, wo), (wr_h, wr))

    def small_copy(i):
        return pltpu.make_async_copy(smalls[i][0], smalls[i][1], sem_s.at[i])

    def g_copy(l, i):
        sl = pl.ds(i * GCH, GCH)
        return pltpu.make_async_copy(wg_h.at[l, sl], wg.at[l, sl], sem_g.at[l, i])

    def u_copy(l, i):
        sl = pl.ds(i * GCH, GCH)
        return pltpu.make_async_copy(wu_h.at[l, sl], wu.at[l, sl], sem_u.at[l, i])

    def d_copy(l, i):
        sl = pl.ds(i * DCH, DCH)
        return pltpu.make_async_copy(wd_h.at[l, sl], wd.at[l, sl], sem_d.at[l, i])

    raw_copy(0).start()
    raw_copy(1).start()
    for i in range(len(smalls)):
        small_copy(i).start()
    raw_copy(2).start()
    raw_copy(3).start()

    def start_layer(l):
        def gu(i, _):
            g_copy(l, i).start()
            u_copy(l, i).start()
            return 0
        lax.fori_loop(0, EXP // GCH, gu, 0)

        def dn(i, _):
            d_copy(l, i).start()
            return 0
        lax.fori_loop(0, EXP // DCH, dn, 0)

    def cache_desc(c, n, part, slot):
        rows = pl.ds(0, B) if part is None else pl.ds(part * (B // 2), B // 2)
        k = part or 0
        return pltpu.make_async_remote_copy(
            src_ref=snd.at[c, peers[n], rows], dst_ref=kall.at[c, slot, rows],
            send_sem=send_c.at[c, n, k], recv_sem=recv_c.at[c, slot, k],
            device_id={"tp": peers[n]}, device_id_type=MESH)

    def parts(c, n):
        return (0, 1) if (c, n) == (3, 1) else (None,)

    def cache_copy(c, n, part=None):
        return cache_desc(c, n, part, me)

    def cache_wait(c):
        for n in range(3):
            for part in parts(c, n):
                cache_desc(c, n, part, peers[n]).wait_recv()

    def repack(c):
        raw_copy(c).wait()
        spread[...] = raw[c].reshape(B * BLK * 8, 64).astype(F32)
        for p in range(NTP):
            lo = spread[pl.ds(2 * p, B * BLK, stride=8), :]
            hi = spread[pl.ds(2 * p + 1, B * BLK, stride=8), :]
            snd[c, p] = jnp.concatenate([lo, hi], axis=1).astype(BF16).reshape(B, BLK, 128)
        kall[c, me] = snd[c, me]

    start_layer(0)
    start_layer(1)
    repack(0)
    pl.semaphore_wait(barrier, 3)
    for n in range(3):
        cache_copy(0, n).start()
    repack(1)
    for n in range(3):
        cache_copy(1, n).start()
    repack(2)
    repack(3)
    for c in (2, 3):
        cache_copy(c, 2).start()

    for i in range(len(smalls)):
        small_copy(i).wait()

    eye = lax.broadcasted_iota(jnp.int32, (B, B), 0) == lax.broadcasted_iota(jnp.int32, (B, B), 1)
    len_row = jnp.broadcast_to(lens[...].astype(F32), (B, B))
    len_col = jnp.sum(jnp.where(eye, len_row, 0.0), axis=1, keepdims=True)
    len_b = jnp.broadcast_to(len_col, (B, 128))
    angle = len_b * inv[...]
    cosv, sinv = jnp.cos(angle), jnp.sin(angle)
    lane = lax.broadcasted_iota(jnp.int32, (B, 128), 1)
    low = (lane % 64) < 32
    left = lane < 64
    col = lax.broadcasted_iota(jnp.int32, (64, 1024), 1)
    row = lax.broadcasted_iota(jnp.int32, (64, 1024), 0)
    len64 = jnp.concatenate([len_col] * 4, axis=0)
    pos = ((col // 256) * BLK + col % BLK).astype(F32)
    valid = (((col // BLK) % B) == (row % B)) & (pos < len64)

    h_f = hid[...].astype(F32)

    def emit(c, new):
        new3 = jnp.broadcast_to(new[:, None, :], (B, BLK, 128))
        len3 = jnp.broadcast_to(len_b[:, None, :], (B, BLK, 128))
        pos3 = lax.broadcasted_iota(jnp.int32, (B, BLK, 128), 1).astype(F32)
        for s in range(NTP):
            x = jnp.where(pos3 + float(s * BLK) == len3, new3, kall[c, s].astype(F32)).reshape(B * BLK, 128)
            spread[pl.ds(0, B * BLK, stride=2), :] = x[:, :64]
            spread[pl.ds(1, B * BLK, stride=2), :] = x[:, 64:]
            outs[c][:, pl.ds(s * 2 * BLK, 2 * BLK), :] = spread[pl.ds(0, 2 * B * BLK), :].astype(BF16).reshape(B, 2 * BLK, 64)

    def x_desc(step, piece, n, slot):
        sl = pl.ds(*PIECES[step % 2][piece])
        return pltpu.make_async_remote_copy(
            src_ref=xown.at[step, :, sl], dst_ref=xrecv.at[step, slot, :, sl],
            send_sem=send_x.at[step, piece, n], recv_sem=recv_x.at[step, slot, piece],
            device_id={"tp": peers[n]}, device_id_type=MESH)

    def x_send(step, piece, val):
        sl = pl.ds(*PIECES[step % 2][piece])
        xown[step, :, sl] = val
        for n in range(3):
            x_desc(step, piece, n, me).start()
        xrecv[step, me, :, sl] = val

    def x_sum(step):
        for piece in range(len(PIECES[step % 2])):
            for n in range(3):
                x_desc(step, piece, n, peers[n]).wait_recv()
        tot = xrecv[step, 0].astype(F32)
        for s in range(1, NTP):
            tot = tot + xrecv[step, s].astype(F32)
        return tot

    outs = (ok1, ov1, ok2, ov2)

    for l in range(2):
        a = _norm(h_f, ga[pl.ds(l, 1), :].astype(F32))
        qf = jnp.dot(a, wq[l], preferred_element_type=F32)
        kf = jnp.dot(a, wk[l], preferred_element_type=F32)
        vf = jnp.dot(a, wv[l], preferred_element_type=F32)
        q0 = _rope(qf[:, :128], cosv, sinv, low)
        q1 = _rope(qf[:, 128:], cosv, sinv, low)
        knew = _rope(kf, cosv, sinv, low).astype(BF16).astype(F32)
        vnew = vf.astype(BF16).astype(F32)
        zero = jnp.zeros_like(q0)
        qrows = jnp.concatenate([
            jnp.where(left, q0, zero), jnp.where(left, pltpu.roll(q0, 64, 1), zero),
            jnp.where(left, zero, pltpu.roll(q1, 64, 1)), jnp.where(left, zero, q1)], axis=0).astype(BF16)
        kc, vc = 2 * l, 2 * l + 1
        cache_wait(kc)
        k2d = kall[kc].reshape(NTP * B * BLK, 128)
        sc = lax.dot_general(qrows, k2d, (((1,), (1,)), ((), ())), preferred_element_type=F32) * 0.125
        sc = jnp.where(valid, sc, -1e30)
        ns = jnp.sum(qrows.astype(F32) * jnp.concatenate([knew] * 4, axis=0), axis=1, keepdims=True) * 0.125
        top = jnp.maximum(jnp.max(sc, axis=1, keepdims=True), ns)
        ex, nex = jnp.exp(sc - top), jnp.exp(ns - top)
        den = jnp.sum(ex, axis=1, keepdims=True) + nex
        prob = (ex / den).astype(BF16)
        nprob = (nex / den).astype(BF16).astype(F32)
        cache_wait(vc)
        v2d = kall[vc].reshape(NTP * B * BLK, 128)
        ov = jnp.dot(prob, v2d, preferred_element_type=F32) + nprob * jnp.concatenate([vnew] * 4, axis=0)
        attn = jnp.concatenate([jnp.where(left, ov[0:16], ov[48:64]), jnp.where(left, ov[16:32], ov[32:48])], axis=1).astype(BF16)
        wo_rows = jnp.concatenate([wo[l, pl.ds(0, 64), :], wo[l, pl.ds(192, 64), :], wo[l, pl.ds(64, 128), :]], axis=0)
        x_send(2 * l, 0, jnp.dot(attn, wo_rows, preferred_element_type=F32).astype(BF16))
        if l == 0:
            cache_copy(2, 0).start()
            cache_copy(2, 1).start()
            cache_copy(3, 0).start()
            cache_copy(3, 1, 0).start()
        emit(kc, knew)
        emit(vc, vnew)
        for i in range(EXP // GCH):
            g_copy(l, i).wait()
            u_copy(l, i).wait()
        for i in range(EXP // DCH):
            d_copy(l, i).wait()
        h1 = (h_f + x_sum(2 * l)).astype(BF16).astype(F32)
        m = _norm(h1, gm[pl.ds(l, 1), :].astype(F32))

        lg = lax.dot_general(wr[l], m, (((1,), (1,)), ((), ())), preferred_element_type=F32)
        eid = lax.broadcasted_iota(jnp.int32, (EXP, B), 0)
        chosen = eid < 0
        for k in range(8):
            chosen = chosen | (cho[l, pl.ds(k, 1), :] == eid)
        lg = jnp.where(chosen, lg, -jnp.inf)
        ex = jnp.where(chosen, jnp.exp(lg - jnp.max(lg, axis=0, keepdims=True)), 0.0)
        gate_t = ex / jnp.sum(ex, axis=0, keepdims=True)
        gate = gate_t.T
        for e in range(EXP):
            w = jnp.concatenate([wg[l, e], wu[l, e]], axis=1)
            gu = jnp.dot(m, w, preferred_element_type=F32)
            g, u = gu[:, :FL], gu[:, FL:]
            act[:, pl.ds(e * FL, FL)] = (g * jax.nn.sigmoid(g) * u * jnp.broadcast_to(gate[:, e:e + 1], (B, FL))).astype(BF16)
        def down(piece, pairs, acc):
            first, width = PIECES[1][piece]
            for e in pairs:
                rhs = wd[l, pl.ds(e, 2), :, pl.ds(first, width)].reshape(2 * FL, width)
                acc = acc + jnp.dot(act[:, pl.ds(e * FL, 2 * FL)], rhs, preferred_element_type=F32)
            return acc

        acc0 = down(0, range(0, EXP, 2), jnp.zeros((B, PIECES[1][0][1]), F32))
        acc1 = down(1, range(0, 8, 2), jnp.zeros((B, PIECES[1][1][1]), F32))
        x_send(2 * l + 1, 0, acc0.astype(BF16))
        acc1 = down(1, range(8, EXP, 2), acc1)
        x_send(2 * l + 1, 1, acc1.astype(BF16))
        if l == 0:
            cache_copy(3, 1, 1).start()
        h_f = (h1 + x_sum(2 * l + 1)).astype(BF16).astype(F32)

    hout[...] = h_f.astype(BF16)
    for c in range(4):
        for n in range(3):
            for part in parts(c, n):
                cache_copy(c, n, part).wait_send()
    for step in range(4):
        for piece in range(len(PIECES[step % 2])):
            for n in range(3):
                x_desc(step, piece, n, me).wait_send()


def _store(h, k1, v1, k2, v2, ho, ok1, ov1, ok2, ov2, sem):
    copies = [pltpu.make_async_copy(a, b, sem.at[i])
              for i, (a, b) in enumerate(((k1, ok1), (v1, ov1), (k2, ok2), (v2, ov2), (h, ho)))]
    for c in copies:
        c.start()
    for c in copies:
        c.wait()


def solution(mesh):
    seq_spec = P('dp', 'tp', None, None)
    head_spec = P('dp', None, 'tp', None)
    col_spec = P(None, None, 'tp')
    ff_spec = P(None, None, None, 'tp')
    inv_freq = (THETA ** (-2.0 * np.arange(32, dtype=np.float64) / 64)).astype(np.float32)
    inv_row = np.tile(inv_freq, 4)[None, :]

    def local_step(hidden, lengths, choice, keys_one, vals_one, keys_two, vals_two, g_attn, w_q, w_k, w_v, w_o, g_mlp, w_router, w_gate, w_up, w_down):
        shapes = (jax.ShapeDtypeStruct((B, D), BF16),) + (jax.ShapeDtypeStruct((B, 2 * SEQ, 64), BF16),) * 4
        any_spec = pl.BlockSpec(memory_space=pl.ANY)
        vmem_spec = pl.BlockSpec(memory_space=pltpu.VMEM)
        V = pltpu.VMEM
        DMA = pltpu.SemaphoreType.DMA
        outs = pl.pallas_call(
            _kernel,
            out_shape=tuple(V(s.shape, s.dtype) for s in shapes),
            in_specs=[any_spec] * 18,
            out_specs=(vmem_spec,) * 5,
            scratch_shapes=[
                V((B, D), BF16), V((1, B), jnp.int32), V((2, 8, B), jnp.int32), V((4, B, BLK, 8, 64), BF16),
                V((2, D), BF16), V((2, D, 256), BF16), V((2, D, 128), BF16), V((2, D, 128), BF16), V((2, 256, D), BF16),
                V((2, D), BF16), V((2, EXP, D), BF16), V((2, EXP, D, FL), BF16), V((2, EXP, D, FL), BF16), V((2, EXP, FL, D), BF16),
                V((1, 128), F32),
                V((B * BLK * 8, 64), F32), V((4, NTP, B, BLK, 128), BF16), V((4, NTP, B, BLK, 128), BF16),
                V((4, B, D), BF16), V((4, NTP, B, D), BF16), V((B, EXP * FL), BF16),
                DMA((12,)), DMA((4,)), DMA((2, EXP // GCH)), DMA((2, EXP // GCH)), DMA((2, EXP // DCH)),
                DMA((4, 3, 2)), DMA((4, NTP, 2)), DMA((4, NP, 3)), DMA((4, NTP, NP)),
            ],
            compiler_params=pltpu.CompilerParams(collective_id=0, has_side_effects=True, vmem_limit_bytes=64_000_000),
        )(hidden, lengths.reshape(1, B), jnp.transpose(choice, (0, 2, 1)), keys_one, vals_one, keys_two, vals_two,
          g_attn, w_q, w_k, w_v, w_o, g_mlp, jnp.transpose(w_router, (0, 2, 1)), w_gate, w_up, w_down, jnp.asarray(inv_row))
        outs = pl.pallas_call(
            _store,
            out_shape=shapes,
            in_specs=[vmem_spec] * 5,
            out_specs=(any_spec,) * 5,
            scratch_shapes=[DMA((5,))],
        )(*[pltpu.with_memory_space_constraint(o, pltpu.VMEM) for o in outs])
        return (outs[0],) + tuple(o.reshape(B, SEQ, 2, 64) for o in outs[1:])

    return jax.shard_map(local_step, mesh=mesh, in_specs=(P('dp', None), P('dp'), P(None, 'dp', None), seq_spec, seq_spec, seq_spec, seq_spec, P(), col_spec, col_spec, col_spec, P(None, 'tp', None), P(), P(), ff_spec, ff_spec, P(None, None, 'tp', None)), out_specs=(P('dp', None), head_spec, head_spec, head_spec, head_spec), check_vma=False)
```

```python
import functools

import numpy as np

import jax
import jax.numpy as jnp
from jax import lax
from jax.experimental import pallas as pl
from jax.experimental.pallas import tpu as pltpu
from jax.sharding import PartitionSpec as P

EPS = 1e-5
THETA = 1000000.0
MESH = pl.DeviceIdType.MESH
B = 16
D = 1024
SEQ = 64
BLK = 16
NTP = 4
EXP = 32
FL = 128
GCH = 4
DCH = 8
PIECES = (((0, 1024),), ((0, 512), (512, 512)))
NP = 2
F32 = jnp.float32
BF16 = jnp.bfloat16


def _norm(h_f, gain_row):
    scale = lax.rsqrt(jnp.mean(h_f * h_f, axis=-1, keepdims=True) + EPS)
    return (h_f * scale * gain_row).astype(BF16)


def _rope(x, cosv, sinv, low):
    rot = jnp.where(low, -pltpu.roll(x, 96, 1), pltpu.roll(x, 32, 1))
    return x * cosv + rot * sinv


def _kernel(hid_h, len_h, cho_h, k1_h, v1_h, k2_h, v2_h, ga_h, wq_h, wk_h, wv_h, wo_h, gm_h, wr_h, wg_h, wu_h, wd_h, inv_h,
            hout, ok1, ov1, ok2, ov2,
            hid, lens, cho, raw, ga, wq, wk, wv, wo, gm, wr, wg, wu, wd, inv,
            spread, snd, kall, xown, xrecv, act,
            sem_s, sem_raw, sem_g, sem_u, sem_d, send_c, recv_c, send_x, recv_x):
    me = lax.axis_index("tp")
    chip, core = me // 2, me % 2
    partner = chip * 2 + (1 - core)
    cross_a = (1 - chip) * 2 + core
    cross_b = (1 - chip) * 2 + (1 - core)
    peers = (cross_a, cross_b, partner)

    barrier = pltpu.get_barrier_semaphore()
    for p in peers:
        pl.semaphore_signal(barrier, inc=1, device_id={"tp": p}, device_id_type=MESH)

    raw_src = (k1_h, v1_h, k2_h, v2_h)

    def raw_copy(c):
        return pltpu.make_async_copy(raw_src[c], raw.at[c], sem_raw.at[c])

    smalls = ((hid_h, hid), (len_h, lens), (cho_h, cho), (ga_h, ga), (gm_h, gm), (inv_h, inv),
              (wq_h, wq), (wk_h, wk), (wv_h, wv), (wo_h, wo), (wr_h, wr))

    def small_copy(i):
        return pltpu.make_async_copy(smalls[i][0], smalls[i][1], sem_s.at[i])

    def g_copy(l, i):
        sl = pl.ds(i * GCH, GCH)
        return pltpu.make_async_copy(wg_h.at[l, sl], wg.at[l, sl], sem_g.at[l, i])

    def u_copy(l, i):
        sl = pl.ds(i * GCH, GCH)
        return pltpu.make_async_copy(wu_h.at[l, sl], wu.at[l, sl], sem_u.at[l, i])

    def d_copy(l, i):
        sl = pl.ds(i * DCH, DCH)
        return pltpu.make_async_copy(wd_h.at[l, sl], wd.at[l, sl], sem_d.at[l, i])

    raw_copy(0).start()
    raw_copy(1).start()
    for i in range(len(smalls)):
        small_copy(i).start()
    raw_copy(2).start()
    raw_copy(3).start()

    def start_layer(l):
        def gu(i, _):
            g_copy(l, i).start()
            u_copy(l, i).start()
            return 0
        lax.fori_loop(0, EXP // GCH, gu, 0)

        def dn(i, _):
            d_copy(l, i).start()
            return 0
        lax.fori_loop(0, EXP // DCH, dn, 0)

    def cache_desc(c, n, part, slot):
        rows = pl.ds(0, B) if part is None else pl.ds(part * (B // 2), B // 2)
        k = part or 0
        return pltpu.make_async_remote_copy(
            src_ref=snd.at[c, peers[n], rows], dst_ref=kall.at[c, slot, rows],
            send_sem=send_c.at[c, n, k], recv_sem=recv_c.at[c, slot, k],
            device_id={"tp": peers[n]}, device_id_type=MESH)

    def parts(c, n):
        return (None,)

    def cache_copy(c, n, part=None):
        return cache_desc(c, n, part, me)

    def cache_wait(c):
        for n in range(3):
            for part in parts(c, n):
                cache_desc(c, n, part, peers[n]).wait_recv()

    def repack(c):
        raw_copy(c).wait()
        spread[...] = raw[c].reshape(B * BLK * 8, 64).astype(F32)
        for p in range(NTP):
            lo = spread[pl.ds(2 * p, B * BLK, stride=8), :]
            hi = spread[pl.ds(2 * p + 1, B * BLK, stride=8), :]
            snd[c, p] = jnp.concatenate([lo, hi], axis=1).astype(BF16).reshape(B, BLK, 128)
        kall[c, me] = snd[c, me]

    start_layer(0)
    repack(0)
    pl.semaphore_wait(barrier, 3)
    for n in range(3):
        cache_copy(0, n).start()
    repack(1)
    for n in range(3):
        cache_copy(1, n).start()
    repack(2)
    cache_copy(2, 0).start()
    cache_copy(2, 2).start()
    repack(3)
    cache_copy(3, 2).start()

    for i in range(len(smalls)):
        small_copy(i).wait()

    eye = lax.broadcasted_iota(jnp.int32, (B, B), 0) == lax.broadcasted_iota(jnp.int32, (B, B), 1)
    len_row = jnp.broadcast_to(lens[...].astype(F32), (B, B))
    len_col = jnp.sum(jnp.where(eye, len_row, 0.0), axis=1, keepdims=True)
    len_b = jnp.broadcast_to(len_col, (B, 128))
    angle = len_b * inv[...]
    cosv, sinv = jnp.cos(angle), jnp.sin(angle)
    lane = lax.broadcasted_iota(jnp.int32, (B, 128), 1)
    low = (lane % 64) < 32
    left = lane < 64
    col = lax.broadcasted_iota(jnp.int32, (64, 1024), 1)
    row = lax.broadcasted_iota(jnp.int32, (64, 1024), 0)
    len64 = jnp.concatenate([len_col] * 4, axis=0)
    pos = ((col // 256) * BLK + col % BLK).astype(F32)
    valid = (((col // BLK) % B) == (row % B)) & (pos < len64)

    h_f = hid[...].astype(F32)

    def emit(c, new):
        new3 = jnp.broadcast_to(new[:, None, :], (B, BLK, 128))
        len3 = jnp.broadcast_to(len_b[:, None, :], (B, BLK, 128))
        pos3 = lax.broadcasted_iota(jnp.int32, (B, BLK, 128), 1).astype(F32)
        for s in range(NTP):
            x = jnp.where(pos3 + float(s * BLK) == len3, new3, kall[c, s].astype(F32)).reshape(B * BLK, 128)
            spread[pl.ds(0, B * BLK, stride=2), :] = x[:, :64]
            spread[pl.ds(1, B * BLK, stride=2), :] = x[:, 64:]
            outs[c][:, pl.ds(s * 2 * BLK, 2 * BLK), :] = spread[pl.ds(0, 2 * B * BLK), :].astype(BF16).reshape(B, 2 * BLK, 64)

    def x_desc(step, piece, n, slot):
        sl = pl.ds(*PIECES[step % 2][piece])
        return pltpu.make_async_remote_copy(
            src_ref=xown.at[step, :, sl], dst_ref=xrecv.at[step, slot, :, sl],
            send_sem=send_x.at[step, piece, n], recv_sem=recv_x.at[step, slot, piece],
            device_id={"tp": peers[n]}, device_id_type=MESH)

    def x_send(step, piece, val):
        sl = pl.ds(*PIECES[step % 2][piece])
        xown[step, :, sl] = val
        for n in range(3):
            x_desc(step, piece, n, me).start()
        xrecv[step, me, :, sl] = val

    def x_sum(step):
        for piece in range(len(PIECES[step % 2])):
            for n in range(3):
                x_desc(step, piece, n, peers[n]).wait_recv()
        tot = xrecv[step, 0].astype(F32)
        for s in range(1, NTP):
            tot = tot + xrecv[step, s].astype(F32)
        return tot

    outs = (ok1, ov1, ok2, ov2)

    for l in range(2):
        a = _norm(h_f, ga[pl.ds(l, 1), :].astype(F32))
        qf = jnp.dot(a, wq[l], preferred_element_type=F32)
        kf = jnp.dot(a, wk[l], preferred_element_type=F32)
        vf = jnp.dot(a, wv[l], preferred_element_type=F32)
        q0 = _rope(qf[:, :128], cosv, sinv, low)
        q1 = _rope(qf[:, 128:], cosv, sinv, low)
        knew = _rope(kf, cosv, sinv, low).astype(BF16).astype(F32)
        vnew = vf.astype(BF16).astype(F32)
        zero = jnp.zeros_like(q0)
        qrows = jnp.concatenate([
            jnp.where(left, q0, zero), jnp.where(left, pltpu.roll(q0, 64, 1), zero),
            jnp.where(left, zero, pltpu.roll(q1, 64, 1)), jnp.where(left, zero, q1)], axis=0).astype(BF16)
        kc, vc = 2 * l, 2 * l + 1
        cache_wait(kc)
        k2d = kall[kc].reshape(NTP * B * BLK, 128)
        sc = lax.dot_general(qrows, k2d, (((1,), (1,)), ((), ())), preferred_element_type=F32) * 0.125
        sc = jnp.where(valid, sc, -1e30)
        ns = jnp.sum(qrows.astype(F32) * jnp.concatenate([knew] * 4, axis=0), axis=1, keepdims=True) * 0.125
        top = jnp.maximum(jnp.max(sc, axis=1, keepdims=True), ns)
        ex, nex = jnp.exp(sc - top), jnp.exp(ns - top)
        den = jnp.sum(ex, axis=1, keepdims=True) + nex
        prob = (ex / den).astype(BF16)
        nprob = (nex / den).astype(BF16).astype(F32)
        cache_wait(vc)
        v2d = kall[vc].reshape(NTP * B * BLK, 128)
        ov = jnp.dot(prob, v2d, preferred_element_type=F32) + nprob * jnp.concatenate([vnew] * 4, axis=0)
        attn = jnp.concatenate([jnp.where(left, ov[0:16], ov[48:64]), jnp.where(left, ov[16:32], ov[32:48])], axis=1).astype(BF16)
        wo_rows = jnp.concatenate([wo[l, pl.ds(0, 64), :], wo[l, pl.ds(192, 64), :], wo[l, pl.ds(64, 128), :]], axis=0)
        x_send(2 * l, 0, jnp.dot(attn, wo_rows, preferred_element_type=F32).astype(BF16))
        if l == 0:
            cache_copy(2, 1).start()
            cache_copy(3, 0).start()
            cache_copy(3, 1).start()
        emit(kc, knew)
        emit(vc, vnew)
        for i in range(EXP // GCH):
            g_copy(l, i).wait()
            u_copy(l, i).wait()
        for i in range(EXP // DCH):
            d_copy(l, i).wait()
        if l == 0:
            start_layer(1)
        h1 = (h_f + x_sum(2 * l)).astype(BF16).astype(F32)
        m = _norm(h1, gm[pl.ds(l, 1), :].astype(F32))

        lg = lax.dot_general(wr[l], m, (((1,), (1,)), ((), ())), preferred_element_type=F32)
        eid = lax.broadcasted_iota(jnp.int32, (EXP, B), 0)
        chosen = eid < 0
        for k in range(8):
            chosen = chosen | (cho[l, pl.ds(k, 1), :] == eid)
        lg = jnp.where(chosen, lg, -jnp.inf)
        ex = jnp.where(chosen, jnp.exp(lg - jnp.max(lg, axis=0, keepdims=True)), 0.0)
        gate_t = ex / jnp.sum(ex, axis=0, keepdims=True)
        gate = gate_t.T
        for e in range(EXP):
            w = jnp.concatenate([wg[l, e], wu[l, e]], axis=1)
            gu = jnp.dot(m, w, preferred_element_type=F32)
            g, u = gu[:, :FL], gu[:, FL:]
            act[:, pl.ds(e * FL, FL)] = (g * jax.nn.sigmoid(g) * u * jnp.broadcast_to(gate[:, e:e + 1], (B, FL))).astype(BF16)
        def down(piece, pairs, acc):
            first, width = PIECES[1][piece]
            for e in pairs:
                rhs = wd[l, pl.ds(e, 2), :, pl.ds(first, width)].reshape(2 * FL, width)
                acc = acc + jnp.dot(act[:, pl.ds(e * FL, 2 * FL)], rhs, preferred_element_type=F32)
            return acc

        acc0 = down(0, range(0, EXP, 2), jnp.zeros((B, PIECES[1][0][1]), F32))
        acc1 = down(1, range(0, 8, 2), jnp.zeros((B, PIECES[1][1][1]), F32))
        x_send(2 * l + 1, 0, acc0.astype(BF16))
        acc1 = down(1, range(8, EXP, 2), acc1)
        x_send(2 * l + 1, 1, acc1.astype(BF16))
        h_f = (h1 + x_sum(2 * l + 1)).astype(BF16).astype(F32)

    hout[...] = h_f.astype(BF16)
    for c in range(4):
        for n in range(3):
            for part in parts(c, n):
                cache_copy(c, n, part).wait_send()
    for step in range(4):
        for piece in range(len(PIECES[step % 2])):
            for n in range(3):
                x_desc(step, piece, n, me).wait_send()


def _store(h, k1, v1, k2, v2, ho, ok1, ov1, ok2, ov2, sem):
    copies = [pltpu.make_async_copy(a, b, sem.at[i])
              for i, (a, b) in enumerate(((k1, ok1), (v1, ov1), (k2, ok2), (v2, ov2), (h, ho)))]
    for c in copies:
        c.start()
    for c in copies:
        c.wait()


def solution(mesh):
    seq_spec = P('dp', 'tp', None, None)
    head_spec = P('dp', None, 'tp', None)
    col_spec = P(None, None, 'tp')
    ff_spec = P(None, None, None, 'tp')
    inv_freq = (THETA ** (-2.0 * np.arange(32, dtype=np.float64) / 64)).astype(np.float32)
    inv_row = np.tile(inv_freq, 4)[None, :]

    def local_step(hidden, lengths, choice, keys_one, vals_one, keys_two, vals_two, g_attn, w_q, w_k, w_v, w_o, g_mlp, w_router, w_gate, w_up, w_down):
        shapes = (jax.ShapeDtypeStruct((B, D), BF16),) + (jax.ShapeDtypeStruct((B, 2 * SEQ, 64), BF16),) * 4
        any_spec = pl.BlockSpec(memory_space=pl.ANY)
        vmem_spec = pl.BlockSpec(memory_space=pltpu.VMEM)
        V = pltpu.VMEM
        DMA = pltpu.SemaphoreType.DMA
        outs = pl.pallas_call(
            _kernel,
            out_shape=tuple(V(s.shape, s.dtype) for s in shapes),
            in_specs=[any_spec] * 18,
            out_specs=(vmem_spec,) * 5,
            scratch_shapes=[
                V((B, D), BF16), V((1, B), jnp.int32), V((2, 8, B), jnp.int32), V((4, B, BLK, 8, 64), BF16),
                V((2, D), BF16), V((2, D, 256), BF16), V((2, D, 128), BF16), V((2, D, 128), BF16), V((2, 256, D), BF16),
                V((2, D), BF16), V((2, EXP, D), BF16), V((2, EXP, D, FL), BF16), V((2, EXP, D, FL), BF16), V((2, EXP, FL, D), BF16),
                V((1, 128), F32),
                V((B * BLK * 8, 64), F32), V((4, NTP, B, BLK, 128), BF16), V((4, NTP, B, BLK, 128), BF16),
                V((4, B, D), BF16), V((4, NTP, B, D), BF16), V((B, EXP * FL), BF16),
                DMA((12,)), DMA((4,)), DMA((2, EXP // GCH)), DMA((2, EXP // GCH)), DMA((2, EXP // DCH)),
                DMA((4, 3, 2)), DMA((4, NTP, 2)), DMA((4, NP, 3)), DMA((4, NTP, NP)),
            ],
            compiler_params=pltpu.CompilerParams(collective_id=0, has_side_effects=True, vmem_limit_bytes=64_000_000),
        )(hidden, lengths.reshape(1, B), jnp.transpose(choice, (0, 2, 1)), keys_one, vals_one, keys_two, vals_two,
          g_attn, w_q, w_k, w_v, w_o, g_mlp, jnp.transpose(w_router, (0, 2, 1)), w_gate, w_up, w_down, jnp.asarray(inv_row))
        outs = pl.pallas_call(
            _store,
            out_shape=shapes,
            in_specs=[vmem_spec] * 5,
            out_specs=(any_spec,) * 5,
            scratch_shapes=[DMA((5,))],
        )(*[pltpu.with_memory_space_constraint(o, pltpu.VMEM) for o in outs])
        return (outs[0],) + tuple(o.reshape(B, SEQ, 2, 64) for o in outs[1:])

    return jax.shard_map(local_step, mesh=mesh, in_specs=(P('dp', None), P('dp'), P(None, 'dp', None), seq_spec, seq_spec, seq_spec, seq_spec, P(), col_spec, col_spec, col_spec, P(None, 'tp', None), P(), P(), ff_spec, ff_spec, P(None, None, 'tp', None)), out_specs=(P('dp', None), head_spec, head_spec, head_spec, head_spec), check_vma=False)
```

```python
import functools

import numpy as np

import jax
import jax.numpy as jnp
from jax import lax
from jax.experimental import pallas as pl
from jax.experimental.pallas import tpu as pltpu
from jax.sharding import PartitionSpec as P

EPS = 1e-5
THETA = 1000000.0
MESH = pl.DeviceIdType.MESH
B = 16
D = 1024
SEQ = 64
BLK = 16
NTP = 4
EXP = 32
FL = 128
GCH = 4
DCH = 8
PIECES = (((0, 1024),), ((0, 512), (512, 512)))
NP = 2
F32 = jnp.float32
BF16 = jnp.bfloat16


def _norm(h_f, gain_row):
    scale = lax.rsqrt(jnp.mean(h_f * h_f, axis=-1, keepdims=True) + EPS)
    return (h_f * scale * gain_row).astype(BF16)


def _rope(x, cosv, sinv, low):
    rot = jnp.where(low, -pltpu.roll(x, 96, 1), pltpu.roll(x, 32, 1))
    return x * cosv + rot * sinv


def _kernel(hid_h, len_h, cho_h, k1_h, v1_h, k2_h, v2_h, ga_h, wq_h, wk_h, wv_h, wo_h, gm_h, wr_h, wg_h, wu_h, wd_h, inv_h,
            hout, ok1, ov1, ok2, ov2,
            hid, lens, cho, raw, ga, wq, wk, wv, wo, gm, wr, wg, wu, wd, inv,
            spread, snd, kall, xown, xrecv, act,
            sem_s, sem_raw, sem_g, sem_u, sem_d, send_c, recv_c, send_x, recv_x):
    me = lax.axis_index("tp")
    chip, core = me // 2, me % 2
    partner = chip * 2 + (1 - core)
    cross_a = (1 - chip) * 2 + core
    cross_b = (1 - chip) * 2 + (1 - core)
    peers = (cross_a, cross_b, partner)

    barrier = pltpu.get_barrier_semaphore()
    for p in peers:
        pl.semaphore_signal(barrier, inc=1, device_id={"tp": p}, device_id_type=MESH)

    raw_src = (k1_h, v1_h, k2_h, v2_h)
    pending = {}

    def raw_copy(c):
        return pltpu.make_async_copy(raw_src[c], raw.at[c], sem_raw.at[c])

    smalls = ((hid_h, hid), (len_h, lens), (cho_h, cho), (ga_h, ga), (gm_h, gm), (inv_h, inv),
              (wq_h, wq), (wk_h, wk), (wv_h, wv), (wo_h, wo), (wr_h, wr))

    def small_copy(i):
        return pltpu.make_async_copy(smalls[i][0], smalls[i][1], sem_s.at[i])

    def g_copy(l, i):
        sl = pl.ds(i * GCH, GCH)
        return pltpu.make_async_copy(wg_h.at[l, sl], wg.at[l, sl], sem_g.at[l, i])

    def u_copy(l, i):
        sl = pl.ds(i * GCH, GCH)
        return pltpu.make_async_copy(wu_h.at[l, sl], wu.at[l, sl], sem_u.at[l, i])

    def d_copy(l, i):
        sl = pl.ds(i * DCH, DCH)
        return pltpu.make_async_copy(wd_h.at[l, sl], wd.at[l, sl], sem_d.at[l, i])

    raw_copy(0).start()
    raw_copy(1).start()
    for i in range(len(smalls)):
        small_copy(i).start()
    raw_copy(2).start()
    raw_copy(3).start()

    def start_layer(l):
        for i in range(EXP // GCH):
            g_copy(l, i).start()
            u_copy(l, i).start()
            pending["g", l, i] = g_copy(l, i).wait
            pending["u", l, i] = u_copy(l, i).wait
        for i in range(EXP // DCH):
            d_copy(l, i).start()
            pending["d", l, i] = d_copy(l, i).wait

    def finish(*prefix):
        for key in [k for k in pending if k[:len(prefix)] == prefix]:
            pending.pop(key)()

    def cache_desc(c, n, slot):
        return pltpu.make_async_remote_copy(
            src_ref=snd.at[c, peers[n]], dst_ref=kall.at[c, slot],
            send_sem=send_c.at[c, n], recv_sem=recv_c.at[c, slot],
            device_id={"tp": peers[n]}, device_id_type=MESH)

    def cache_send(c, n):
        cache_desc(c, n, me).start()
        pending["cs", c, n] = cache_desc(c, n, me).wait_send
        pending["cr", c, n] = cache_desc(c, n, peers[n]).wait_recv

    def repack(c):
        spread[...] = raw[c].reshape(B * BLK * 8, 64).astype(F32)
        for p in range(NTP):
            lo = spread[pl.ds(2 * p, B * BLK, stride=8), :]
            hi = spread[pl.ds(2 * p + 1, B * BLK, stride=8), :]
            snd[c, p] = jnp.concatenate([lo, hi], axis=1).astype(BF16).reshape(B, BLK, 128)
        kall[c, me] = snd[c, me]

    raw_copy(0).wait()
    repack(0)
    pl.semaphore_wait(barrier, 3)
    for n in range(3):
        cache_send(0, n)
    raw_copy(1).wait()
    repack(1)
    for n in range(3):
        cache_send(1, n)
    for i in range(len(smalls)):
        small_copy(i).wait()
    raw_copy(2).wait()
    raw_copy(3).wait()
    start_layer(0)
    repack(2)
    cache_send(2, 0)
    cache_send(2, 2)
    repack(3)
    cache_send(3, 2)


    eye = lax.broadcasted_iota(jnp.int32, (B, B), 0) == lax.broadcasted_iota(jnp.int32, (B, B), 1)
    len_row = jnp.broadcast_to(lens[...].astype(F32), (B, B))
    len_col = jnp.sum(jnp.where(eye, len_row, 0.0), axis=1, keepdims=True)
    len_b = jnp.broadcast_to(len_col, (B, 128))
    angle = len_b * inv[...]
    cosv, sinv = jnp.cos(angle), jnp.sin(angle)
    lane = lax.broadcasted_iota(jnp.int32, (B, 128), 1)
    low = (lane % 64) < 32
    left = lane < 64
    col = lax.broadcasted_iota(jnp.int32, (64, 1024), 1)
    row = lax.broadcasted_iota(jnp.int32, (64, 1024), 0)
    len64 = jnp.concatenate([len_col] * 4, axis=0)
    pos = ((col // 256) * BLK + col % BLK).astype(F32)
    valid = (((col // BLK) % B) == (row % B)) & (pos < len64)

    h_f = hid[...].astype(F32)

    def emit(c, new):
        new3 = jnp.broadcast_to(new[:, None, :], (B, BLK, 128))
        len3 = jnp.broadcast_to(len_b[:, None, :], (B, BLK, 128))
        pos3 = lax.broadcasted_iota(jnp.int32, (B, BLK, 128), 1).astype(F32)
        for s in range(NTP):
            x = jnp.where(pos3 + float(s * BLK) == len3, new3, kall[c, s].astype(F32)).reshape(B * BLK, 128)
            spread[pl.ds(0, B * BLK, stride=2), :] = x[:, :64]
            spread[pl.ds(1, B * BLK, stride=2), :] = x[:, 64:]
            outs[c][:, pl.ds(s * 2 * BLK, 2 * BLK), :] = spread[pl.ds(0, 2 * B * BLK), :].astype(BF16).reshape(B, 2 * BLK, 64)

    def x_desc(step, piece, n, slot):
        sl = pl.ds(*PIECES[step % 2][piece])
        return pltpu.make_async_remote_copy(
            src_ref=xown.at[step, :, sl], dst_ref=xrecv.at[step, slot, :, sl],
            send_sem=send_x.at[step, piece, n], recv_sem=recv_x.at[step, slot, piece],
            device_id={"tp": peers[n]}, device_id_type=MESH)

    def x_send(step, piece, val):
        sl = pl.ds(*PIECES[step % 2][piece])
        xown[step, :, sl] = val
        for n in range(3):
            x_desc(step, piece, n, me).start()
            pending["xs", step, piece, n] = x_desc(step, piece, n, me).wait_send
            pending["xr", step, piece, n] = x_desc(step, piece, n, peers[n]).wait_recv
        xrecv[step, me, :, sl] = val

    def x_sum(step):
        finish("xr", step)
        tot = xrecv[step, 0].astype(F32)
        for s in range(1, NTP):
            tot = tot + xrecv[step, s].astype(F32)
        return tot

    outs = (ok1, ov1, ok2, ov2)

    for l in range(2):
        a = _norm(h_f, ga[pl.ds(l, 1), :].astype(F32))
        qf = jnp.dot(a, wq[l], preferred_element_type=F32)
        kf = jnp.dot(a, wk[l], preferred_element_type=F32)
        vf = jnp.dot(a, wv[l], preferred_element_type=F32)
        q0 = _rope(qf[:, :128], cosv, sinv, low)
        q1 = _rope(qf[:, 128:], cosv, sinv, low)
        knew = _rope(kf, cosv, sinv, low).astype(BF16).astype(F32)
        vnew = vf.astype(BF16).astype(F32)
        zero = jnp.zeros_like(q0)
        qrows = jnp.concatenate([
            jnp.where(left, q0, zero), jnp.where(left, pltpu.roll(q0, 64, 1), zero),
            jnp.where(left, zero, pltpu.roll(q1, 64, 1)), jnp.where(left, zero, q1)], axis=0).astype(BF16)
        kc, vc = 2 * l, 2 * l + 1
        finish("cr", kc)
        k2d = kall[kc].reshape(NTP * B * BLK, 128)
        sc = lax.dot_general(qrows, k2d, (((1,), (1,)), ((), ())), preferred_element_type=F32) * 0.125
        sc = jnp.where(valid, sc, -1e30)
        ns = jnp.sum(qrows.astype(F32) * jnp.concatenate([knew] * 4, axis=0), axis=1, keepdims=True) * 0.125
        top = jnp.maximum(jnp.max(sc, axis=1, keepdims=True), ns)
        ex, nex = jnp.exp(sc - top), jnp.exp(ns - top)
        den = jnp.sum(ex, axis=1, keepdims=True) + nex
        prob = (ex / den).astype(BF16)
        nprob = (nex / den).astype(BF16).astype(F32)
        finish("cr", vc)
        v2d = kall[vc].reshape(NTP * B * BLK, 128)
        ov = jnp.dot(prob, v2d, preferred_element_type=F32) + nprob * jnp.concatenate([vnew] * 4, axis=0)
        attn = jnp.concatenate([jnp.where(left, ov[0:16], ov[48:64]), jnp.where(left, ov[16:32], ov[32:48])], axis=1).astype(BF16)
        wo_rows = jnp.concatenate([wo[l, pl.ds(0, 64), :], wo[l, pl.ds(192, 64), :], wo[l, pl.ds(64, 128), :]], axis=0)
        x_send(2 * l, 0, jnp.dot(attn, wo_rows, preferred_element_type=F32).astype(BF16))
        if l == 0:
            cache_send(2, 1)
            cache_send(3, 0)
            cache_send(3, 1)
        emit(kc, knew)
        emit(vc, vnew)
        for kind in "gud":
            finish(kind, l)
        if l == 0:
            start_layer(1)
        h1 = (h_f + x_sum(2 * l)).astype(BF16).astype(F32)
        m = _norm(h1, gm[pl.ds(l, 1), :].astype(F32))

        lg = lax.dot_general(wr[l], m, (((1,), (1,)), ((), ())), preferred_element_type=F32)
        eid = lax.broadcasted_iota(jnp.int32, (EXP, B), 0)
        chosen = eid < 0
        for k in range(8):
            chosen = chosen | (cho[l, pl.ds(k, 1), :] == eid)
        lg = jnp.where(chosen, lg, -jnp.inf)
        ex = jnp.where(chosen, jnp.exp(lg - jnp.max(lg, axis=0, keepdims=True)), 0.0)
        gate_t = ex / jnp.sum(ex, axis=0, keepdims=True)
        gate = gate_t.T
        for e in range(EXP):
            w = jnp.concatenate([wg[l, e], wu[l, e]], axis=1)
            gu = jnp.dot(m, w, preferred_element_type=F32)
            g, u = gu[:, :FL], gu[:, FL:]
            act[:, pl.ds(e * FL, FL)] = (g * jax.nn.sigmoid(g) * u * jnp.broadcast_to(gate[:, e:e + 1], (B, FL))).astype(BF16)
        def down(piece, pairs, acc):
            first, width = PIECES[1][piece]
            for e in pairs:
                rhs = wd[l, pl.ds(e, 2), :, pl.ds(first, width)].reshape(2 * FL, width)
                acc = acc + jnp.dot(act[:, pl.ds(e * FL, 2 * FL)], rhs, preferred_element_type=F32)
            return acc

        acc0 = down(0, range(0, EXP, 2), jnp.zeros((B, PIECES[1][0][1]), F32))
        acc1 = down(1, range(0, 8, 2), jnp.zeros((B, PIECES[1][1][1]), F32))
        x_send(2 * l + 1, 0, acc0.astype(BF16))
        acc1 = down(1, range(8, EXP, 2), acc1)
        x_send(2 * l + 1, 1, acc1.astype(BF16))
        h_f = (h1 + x_sum(2 * l + 1)).astype(BF16).astype(F32)

    hout[...] = h_f.astype(BF16)
    finish()


def _store(h, k1, v1, k2, v2, ho, ok1, ov1, ok2, ov2, sem):
    copies = [pltpu.make_async_copy(a, b, sem.at[i])
              for i, (a, b) in enumerate(((k1, ok1), (v1, ov1), (k2, ok2), (v2, ov2), (h, ho)))]
    for c in copies:
        c.start()
    for c in copies:
        c.wait()


def solution(mesh):
    seq_spec = P('dp', 'tp', None, None)
    head_spec = P('dp', None, 'tp', None)
    col_spec = P(None, None, 'tp')
    ff_spec = P(None, None, None, 'tp')
    inv_freq = (THETA ** (-2.0 * np.arange(32, dtype=np.float64) / 64)).astype(np.float32)
    inv_row = np.tile(inv_freq, 4)[None, :]

    def local_step(hidden, lengths, choice, keys_one, vals_one, keys_two, vals_two, g_attn, w_q, w_k, w_v, w_o, g_mlp, w_router, w_gate, w_up, w_down):
        shapes = (jax.ShapeDtypeStruct((B, D), BF16),) + (jax.ShapeDtypeStruct((B, 2 * SEQ, 64), BF16),) * 4
        any_spec = pl.BlockSpec(memory_space=pl.ANY)
        vmem_spec = pl.BlockSpec(memory_space=pltpu.VMEM)
        V = pltpu.VMEM
        DMA = pltpu.SemaphoreType.DMA
        outs = pl.pallas_call(
            _kernel,
            out_shape=tuple(V(s.shape, s.dtype) for s in shapes),
            in_specs=[any_spec] * 18,
            out_specs=(vmem_spec,) * 5,
            scratch_shapes=[
                V((B, D), BF16), V((1, B), jnp.int32), V((2, 8, B), jnp.int32), V((4, B, BLK, 8, 64), BF16),
                V((2, D), BF16), V((2, D, 256), BF16), V((2, D, 128), BF16), V((2, D, 128), BF16), V((2, 256, D), BF16),
                V((2, D), BF16), V((2, EXP, D), BF16), V((2, EXP, D, FL), BF16), V((2, EXP, D, FL), BF16), V((2, EXP, FL, D), BF16),
                V((1, 128), F32),
                V((B * BLK * 8, 64), F32), V((4, NTP, B, BLK, 128), BF16), V((4, NTP, B, BLK, 128), BF16),
                V((4, B, D), BF16), V((4, NTP, B, D), BF16), V((B, EXP * FL), BF16),
                DMA((12,)), DMA((4,)), DMA((2, EXP // GCH)), DMA((2, EXP // GCH)), DMA((2, EXP // DCH)),
                DMA((4, 3)), DMA((4, NTP)), DMA((4, NP, 3)), DMA((4, NTP, NP)),
            ],
            compiler_params=pltpu.CompilerParams(collective_id=0, has_side_effects=True, vmem_limit_bytes=64_000_000),
        )(hidden, lengths.reshape(1, B), jnp.transpose(choice, (0, 2, 1)), keys_one, vals_one, keys_two, vals_two,
          g_attn, w_q, w_k, w_v, w_o, g_mlp, jnp.transpose(w_router, (0, 2, 1)), w_gate, w_up, w_down, jnp.asarray(inv_row))
        outs = pl.pallas_call(
            _store,
            out_shape=shapes,
            in_specs=[vmem_spec] * 5,
            out_specs=(any_spec,) * 5,
            scratch_shapes=[DMA((5,))],
        )(*[pltpu.with_memory_space_constraint(o, pltpu.VMEM) for o in outs])
        return (outs[0],) + tuple(o.reshape(B, SEQ, 2, 64) for o in outs[1:])

    return jax.shard_map(local_step, mesh=mesh, in_specs=(P('dp', None), P('dp'), P(None, 'dp', None), seq_spec, seq_spec, seq_spec, seq_spec, P(), col_spec, col_spec, col_spec, P(None, 'tp', None), P(), P(), ff_spec, ff_spec, P(None, None, 'tp', None)), out_specs=(P('dp', None), head_spec, head_spec, head_spec, head_spec), check_vma=False)
```

```python
import functools

import numpy as np

import jax
import jax.numpy as jnp
from jax import lax
from jax.experimental import pallas as pl
from jax.experimental.pallas import tpu as pltpu
from jax.sharding import PartitionSpec as P

EPS = 1e-5
THETA = 1000000.0
MESH = pl.DeviceIdType.MESH
B = 16
D = 1024
SEQ = 64
BLK = 16
NTP = 4
EXP = 32
FL = 128
GCH = 4
DCH = 8
PIECES = (((0, 1024),), ((0, 512), (512, 512)))
NP = 2
F32 = jnp.float32
BF16 = jnp.bfloat16


def _norm(h_f, gain_row):
    scale = lax.rsqrt(jnp.mean(h_f * h_f, axis=-1, keepdims=True) + EPS)
    return (h_f * scale * gain_row).astype(BF16)


def _rope(x, cosv, sinv, low):
    rot = jnp.where(low, -pltpu.roll(x, 96, 1), pltpu.roll(x, 32, 1))
    return x * cosv + rot * sinv


def _kernel(hid_h, len_h, cho_h, k1_h, v1_h, k2_h, v2_h, ga_h, wq_h, wk_h, wv_h, wo_h, gm_h, wr_h, wg_h, wu_h, wd_h, inv_h,
            hout, ok1, ov1, ok2, ov2,
            hid, lens, cho, raw, ga, wq, wk, wv, wo, gm, wr, wg, wu, wd, inv,
            spread, snd, kall, xown, xrecv, act,
            sem_s, sem_raw, sem_g, sem_u, sem_d, send_c, recv_c, send_x, recv_x):
    me = lax.axis_index("tp")
    chip, core = me // 2, me % 2
    partner = chip * 2 + (1 - core)
    cross_a = (1 - chip) * 2 + core
    cross_b = (1 - chip) * 2 + (1 - core)
    peers = (cross_a, cross_b, partner)

    barrier = pltpu.get_barrier_semaphore()
    for p in peers:
        pl.semaphore_signal(barrier, inc=1, device_id={"tp": p}, device_id_type=MESH)

    raw_src = (k1_h, v1_h, k2_h, v2_h)
    pending = {}

    def raw_copy(c):
        return pltpu.make_async_copy(raw_src[c], raw.at[c], sem_raw.at[c])

    smalls = ((hid_h, hid), (len_h, lens), (cho_h, cho), (ga_h, ga), (gm_h, gm), (inv_h, inv),
              (wq_h, wq), (wk_h, wk), (wv_h, wv), (wo_h, wo), (wr_h, wr))

    def small_copy(i):
        return pltpu.make_async_copy(smalls[i][0], smalls[i][1], sem_s.at[i])

    def g_copy(l, i):
        sl = pl.ds(i * GCH, GCH)
        return pltpu.make_async_copy(wg_h.at[l, sl], wg.at[l, sl], sem_g.at[l, i])

    def u_copy(l, i):
        sl = pl.ds(i * GCH, GCH)
        return pltpu.make_async_copy(wu_h.at[l, sl], wu.at[l, sl], sem_u.at[l, i])

    def d_copy(l, i):
        sl = pl.ds(i * DCH, DCH)
        return pltpu.make_async_copy(wd_h.at[l, sl], wd.at[l, sl], sem_d.at[l, i])

    raw_copy(0).start()
    raw_copy(1).start()

    def start_layer(l):
        for i in range(EXP // GCH):
            g_copy(l, i).start()
            u_copy(l, i).start()
            pending["g", l, i] = g_copy(l, i).wait
            pending["u", l, i] = u_copy(l, i).wait
        for i in range(EXP // DCH):
            d_copy(l, i).start()
            pending["d", l, i] = d_copy(l, i).wait

    def finish(*prefix):
        for key in [k for k in pending if k[:len(prefix)] == prefix]:
            pending.pop(key)()

    def cache_desc(c, n, slot):
        return pltpu.make_async_remote_copy(
            src_ref=snd.at[c, peers[n]], dst_ref=kall.at[c, slot],
            send_sem=send_c.at[c, n], recv_sem=recv_c.at[c, slot],
            device_id={"tp": peers[n]}, device_id_type=MESH)

    def cache_send(c, n):
        cache_desc(c, n, me).start()
        pending["cs", c, n] = cache_desc(c, n, me).wait_send
        pending["cr", c, n] = cache_desc(c, n, peers[n]).wait_recv

    def repack(c):
        spread[...] = raw[c].reshape(B * BLK * 8, 64).astype(F32)
        for p in range(NTP):
            lo = spread[pl.ds(2 * p, B * BLK, stride=8), :]
            hi = spread[pl.ds(2 * p + 1, B * BLK, stride=8), :]
            snd[c, p] = jnp.concatenate([lo, hi], axis=1).astype(BF16).reshape(B, BLK, 128)
        kall[c, me] = snd[c, me]

    raw_copy(0).wait()
    for i in range(len(smalls)):
        small_copy(i).start()
    repack(0)
    pl.semaphore_wait(barrier, 3)
    for n in range(3):
        cache_send(0, n)
    raw_copy(1).wait()
    raw_copy(2).start()
    raw_copy(3).start()
    repack(1)
    for n in range(3):
        cache_send(1, n)
    for i in range(len(smalls)):
        small_copy(i).wait()
    raw_copy(2).wait()
    raw_copy(3).wait()
    start_layer(0)
    repack(2)
    cache_send(2, 0)
    cache_send(2, 2)
    repack(3)
    cache_send(3, 2)


    eye = lax.broadcasted_iota(jnp.int32, (B, B), 0) == lax.broadcasted_iota(jnp.int32, (B, B), 1)
    len_row = jnp.broadcast_to(lens[...].astype(F32), (B, B))
    len_col = jnp.sum(jnp.where(eye, len_row, 0.0), axis=1, keepdims=True)
    len_b = jnp.broadcast_to(len_col, (B, 128))
    angle = len_b * inv[...]
    cosv, sinv = jnp.cos(angle), jnp.sin(angle)
    lane = lax.broadcasted_iota(jnp.int32, (B, 128), 1)
    low = (lane % 64) < 32
    left = lane < 64
    col = lax.broadcasted_iota(jnp.int32, (64, 1024), 1)
    row = lax.broadcasted_iota(jnp.int32, (64, 1024), 0)
    len64 = jnp.concatenate([len_col] * 4, axis=0)
    pos = ((col // 256) * BLK + col % BLK).astype(F32)
    valid = (((col // BLK) % B) == (row % B)) & (pos < len64)

    h_f = hid[...].astype(F32)

    def emit(c, new):
        new3 = jnp.broadcast_to(new[:, None, :], (B, BLK, 128))
        len3 = jnp.broadcast_to(len_b[:, None, :], (B, BLK, 128))
        pos3 = lax.broadcasted_iota(jnp.int32, (B, BLK, 128), 1).astype(F32)
        for s in range(NTP):
            x = jnp.where(pos3 + float(s * BLK) == len3, new3, kall[c, s].astype(F32)).reshape(B * BLK, 128)
            spread[pl.ds(0, B * BLK, stride=2), :] = x[:, :64]
            spread[pl.ds(1, B * BLK, stride=2), :] = x[:, 64:]
            outs[c][:, pl.ds(s * 2 * BLK, 2 * BLK), :] = spread[pl.ds(0, 2 * B * BLK), :].astype(BF16).reshape(B, 2 * BLK, 64)

    def x_desc(step, piece, n, slot):
        sl = pl.ds(*PIECES[step % 2][piece])
        return pltpu.make_async_remote_copy(
            src_ref=xown.at[step, :, sl], dst_ref=xrecv.at[step, slot, :, sl],
            send_sem=send_x.at[step, piece, n], recv_sem=recv_x.at[step, slot, piece],
            device_id={"tp": peers[n]}, device_id_type=MESH)

    def x_send(step, piece, val):
        sl = pl.ds(*PIECES[step % 2][piece])
        xown[step, :, sl] = val
        for n in range(3):
            x_desc(step, piece, n, me).start()
            pending["xs", step, piece, n] = x_desc(step, piece, n, me).wait_send
            pending["xr", step, piece, n] = x_desc(step, piece, n, peers[n]).wait_recv
        xrecv[step, me, :, sl] = val

    def x_sum(step):
        finish("xr", step)
        tot = xrecv[step, 0].astype(F32)
        for s in range(1, NTP):
            tot = tot + xrecv[step, s].astype(F32)
        return tot

    outs = (ok1, ov1, ok2, ov2)

    for l in range(2):
        a = _norm(h_f, ga[pl.ds(l, 1), :].astype(F32))
        qf = jnp.dot(a, wq[l], preferred_element_type=F32)
        kf = jnp.dot(a, wk[l], preferred_element_type=F32)
        vf = jnp.dot(a, wv[l], preferred_element_type=F32)
        q0 = _rope(qf[:, :128], cosv, sinv, low)
        q1 = _rope(qf[:, 128:], cosv, sinv, low)
        knew = _rope(kf, cosv, sinv, low).astype(BF16).astype(F32)
        vnew = vf.astype(BF16).astype(F32)
        zero = jnp.zeros_like(q0)
        qrows = jnp.concatenate([
            jnp.where(left, q0, zero), jnp.where(left, pltpu.roll(q0, 64, 1), zero),
            jnp.where(left, zero, pltpu.roll(q1, 64, 1)), jnp.where(left, zero, q1)], axis=0).astype(BF16)
        kc, vc = 2 * l, 2 * l + 1
        finish("cr", kc)
        k2d = kall[kc].reshape(NTP * B * BLK, 128)
        sc = lax.dot_general(qrows, k2d, (((1,), (1,)), ((), ())), preferred_element_type=F32) * 0.125
        sc = jnp.where(valid, sc, -1e30)
        ns = jnp.sum(qrows.astype(F32) * jnp.concatenate([knew] * 4, axis=0), axis=1, keepdims=True) * 0.125
        top = jnp.maximum(jnp.max(sc, axis=1, keepdims=True), ns)
        ex, nex = jnp.exp(sc - top), jnp.exp(ns - top)
        den = jnp.sum(ex, axis=1, keepdims=True) + nex
        prob = (ex / den).astype(BF16)
        nprob = (nex / den).astype(BF16).astype(F32)
        finish("cr", vc)
        v2d = kall[vc].reshape(NTP * B * BLK, 128)
        ov = jnp.dot(prob, v2d, preferred_element_type=F32) + nprob * jnp.concatenate([vnew] * 4, axis=0)
        attn = jnp.concatenate([jnp.where(left, ov[0:16], ov[48:64]), jnp.where(left, ov[16:32], ov[32:48])], axis=1).astype(BF16)
        wo_rows = jnp.concatenate([wo[l, pl.ds(0, 64), :], wo[l, pl.ds(192, 64), :], wo[l, pl.ds(64, 128), :]], axis=0)
        x_send(2 * l, 0, jnp.dot(attn, wo_rows, preferred_element_type=F32).astype(BF16))
        if l == 0:
            cache_send(2, 1)
            cache_send(3, 0)
            cache_send(3, 1)
        emit(kc, knew)
        emit(vc, vnew)
        for kind in "gud":
            finish(kind, l)
        if l == 0:
            start_layer(1)
        h1 = (h_f + x_sum(2 * l)).astype(BF16).astype(F32)
        m = _norm(h1, gm[pl.ds(l, 1), :].astype(F32))

        lg = lax.dot_general(wr[l], m, (((1,), (1,)), ((), ())), preferred_element_type=F32)
        eid = lax.broadcasted_iota(jnp.int32, (EXP, B), 0)
        chosen = eid < 0
        for k in range(8):
            chosen = chosen | (cho[l, pl.ds(k, 1), :] == eid)
        lg = jnp.where(chosen, lg, -jnp.inf)
        ex = jnp.where(chosen, jnp.exp(lg - jnp.max(lg, axis=0, keepdims=True)), 0.0)
        gate_t = ex / jnp.sum(ex, axis=0, keepdims=True)
        gate = gate_t.T
        for e in range(EXP):
            w = jnp.concatenate([wg[l, e], wu[l, e]], axis=1)
            gu = jnp.dot(m, w, preferred_element_type=F32)
            g, u = gu[:, :FL], gu[:, FL:]
            act[:, pl.ds(e * FL, FL)] = (g * jax.nn.sigmoid(g) * u * jnp.broadcast_to(gate[:, e:e + 1], (B, FL))).astype(BF16)
        def down(piece, pairs, acc):
            first, width = PIECES[1][piece]
            for e in pairs:
                rhs = wd[l, pl.ds(e, 2), :, pl.ds(first, width)].reshape(2 * FL, width)
                acc = acc + jnp.dot(act[:, pl.ds(e * FL, 2 * FL)], rhs, preferred_element_type=F32)
            return acc

        acc0 = down(0, range(0, EXP, 2), jnp.zeros((B, PIECES[1][0][1]), F32))
        acc1 = down(1, range(0, 8, 2), jnp.zeros((B, PIECES[1][1][1]), F32))
        x_send(2 * l + 1, 0, acc0.astype(BF16))
        acc1 = down(1, range(8, EXP, 2), acc1)
        x_send(2 * l + 1, 1, acc1.astype(BF16))
        h_f = (h1 + x_sum(2 * l + 1)).astype(BF16).astype(F32)

    hout[...] = h_f.astype(BF16)
    finish()


def _store(h, k1, v1, k2, v2, ho, ok1, ov1, ok2, ov2, sem):
    copies = [pltpu.make_async_copy(a, b, sem.at[i])
              for i, (a, b) in enumerate(((k1, ok1), (v1, ov1), (k2, ok2), (v2, ov2), (h, ho)))]
    for c in copies:
        c.start()
    for c in copies:
        c.wait()


def solution(mesh):
    seq_spec = P('dp', 'tp', None, None)
    head_spec = P('dp', None, 'tp', None)
    col_spec = P(None, None, 'tp')
    ff_spec = P(None, None, None, 'tp')
    inv_freq = (THETA ** (-2.0 * np.arange(32, dtype=np.float64) / 64)).astype(np.float32)
    inv_row = np.tile(inv_freq, 4)[None, :]

    def local_step(hidden, lengths, choice, keys_one, vals_one, keys_two, vals_two, g_attn, w_q, w_k, w_v, w_o, g_mlp, w_router, w_gate, w_up, w_down):
        shapes = (jax.ShapeDtypeStruct((B, D), BF16),) + (jax.ShapeDtypeStruct((B, 2 * SEQ, 64), BF16),) * 4
        any_spec = pl.BlockSpec(memory_space=pl.ANY)
        vmem_spec = pl.BlockSpec(memory_space=pltpu.VMEM)
        V = pltpu.VMEM
        DMA = pltpu.SemaphoreType.DMA
        outs = pl.pallas_call(
            _kernel,
            out_shape=tuple(V(s.shape, s.dtype) for s in shapes),
            in_specs=[any_spec] * 18,
            out_specs=(vmem_spec,) * 5,
            scratch_shapes=[
                V((B, D), BF16), V((1, B), jnp.int32), V((2, 8, B), jnp.int32), V((4, B, BLK, 8, 64), BF16),
                V((2, D), BF16), V((2, D, 256), BF16), V((2, D, 128), BF16), V((2, D, 128), BF16), V((2, 256, D), BF16),
                V((2, D), BF16), V((2, EXP, D), BF16), V((2, EXP, D, FL), BF16), V((2, EXP, D, FL), BF16), V((2, EXP, FL, D), BF16),
                V((1, 128), F32),
                V((B * BLK * 8, 64), F32), V((4, NTP, B, BLK, 128), BF16), V((4, NTP, B, BLK, 128), BF16),
                V((4, B, D), BF16), V((4, NTP, B, D), BF16), V((B, EXP * FL), BF16),
                DMA((12,)), DMA((4,)), DMA((2, EXP // GCH)), DMA((2, EXP // GCH)), DMA((2, EXP // DCH)),
                DMA((4, 3)), DMA((4, NTP)), DMA((4, NP, 3)), DMA((4, NTP, NP)),
            ],
            compiler_params=pltpu.CompilerParams(collective_id=0, has_side_effects=True, vmem_limit_bytes=64_000_000),
        )(hidden, lengths.reshape(1, B), jnp.transpose(choice, (0, 2, 1)), keys_one, vals_one, keys_two, vals_two,
          g_attn, w_q, w_k, w_v, w_o, g_mlp, jnp.transpose(w_router, (0, 2, 1)), w_gate, w_up, w_down, jnp.asarray(inv_row))
        outs = pl.pallas_call(
            _store,
            out_shape=shapes,
            in_specs=[vmem_spec] * 5,
            out_specs=(any_spec,) * 5,
            scratch_shapes=[DMA((5,))],
        )(*[pltpu.with_memory_space_constraint(o, pltpu.VMEM) for o in outs])
        return (outs[0],) + tuple(o.reshape(B, SEQ, 2, 64) for o in outs[1:])

    return jax.shard_map(local_step, mesh=mesh, in_specs=(P('dp', None), P('dp'), P(None, 'dp', None), seq_spec, seq_spec, seq_spec, seq_spec, P(), col_spec, col_spec, col_spec, P(None, 'tp', None), P(), P(), ff_spec, ff_spec, P(None, None, 'tp', None)), out_specs=(P('dp', None), head_spec, head_spec, head_spec, head_spec), check_vma=False)
```

```python
import functools

import numpy as np

import jax
import jax.numpy as jnp
from jax import lax
from jax.experimental import pallas as pl
from jax.experimental.pallas import tpu as pltpu
from jax.sharding import PartitionSpec as P

EPS = 1e-5
THETA = 1000000.0
MESH = pl.DeviceIdType.MESH
B = 16
D = 1024
SEQ = 64
BLK = 16
NTP = 4
EXP = 32
FL = 128
GCH = 4
DCH = 8
PIECES = (((0, 1024),), ((0, 512), (512, 512)))
NP = 2
F32 = jnp.float32
BF16 = jnp.bfloat16


def _norm(h_f, gain_row):
    scale = lax.rsqrt(jnp.mean(h_f * h_f, axis=-1, keepdims=True) + EPS)
    return (h_f * scale * gain_row).astype(BF16)


def _rope(x, cosv, sinv, low):
    rot = jnp.where(low, -pltpu.roll(x, 96, 1), pltpu.roll(x, 32, 1))
    return x * cosv + rot * sinv


def _kernel(hid_h, len_h, cho_h, k1_h, v1_h, k2_h, v2_h, ga_h, wq_h, wk_h, wv_h, wo_h, gm_h, wr_h, wg_h, wu_h, wd_h, inv_h,
            hout, ok1, ov1, ok2, ov2,
            hid, lens, cho, raw, ga, wq, wk, wv, wo, gm, wr, wg, wu, wd, inv,
            spread, snd, kall, xown, xrecv, act,
            sem_s, sem_raw, sem_w, send_c, recv_c, send_x, recv_x):
    me = lax.axis_index("tp")
    chip, core = me // 2, me % 2
    partner = chip * 2 + (1 - core)
    cross_a = (1 - chip) * 2 + core
    cross_b = (1 - chip) * 2 + (1 - core)
    peers = (cross_a, cross_b, partner)

    barrier = pltpu.get_barrier_semaphore()
    for p in peers:
        pl.semaphore_signal(barrier, inc=1, device_id={"tp": p}, device_id_type=MESH)

    raw_src = (k1_h, v1_h, k2_h, v2_h)

    def raw_copy(c):
        return pltpu.make_async_copy(raw_src[c], raw.at[c], sem_raw.at[c])

    smalls = ((hid_h, hid), (len_h, lens), (cho_h, cho), (ga_h, ga), (gm_h, gm), (inv_h, inv),
              (wq_h, wq), (wk_h, wk), (wv_h, wv), (wo_h, wo), (wr_h, wr))

    def small_copy(i):
        return pltpu.make_async_copy(smalls[i][0], smalls[i][1], sem_s.at[i])

    def w_copy(l, k):
        src, dst = ((wg_h, wg), (wu_h, wu), (wd_h, wd))[k]
        return pltpu.make_async_copy(src.at[l], dst.at[l], sem_w.at[l, k])

    raw_copy(0).start()
    raw_copy(1).start()

    def start_layer(l):
        for k in range(3):
            w_copy(l, k).start()

    def cache_send(c, n):
        pltpu.make_async_remote_copy(
            src_ref=snd.at[c, peers[n]], dst_ref=kall.at[c, me],
            send_sem=send_c.at[0], recv_sem=recv_c.at[c],
            device_id={"tp": peers[n]}, device_id_type=MESH).start()

    def cache_wait(c):
        pltpu.make_async_remote_copy(
            src_ref=snd.at[c, pl.ds(0, 3)], dst_ref=kall.at[c, pl.ds(0, 3)],
            send_sem=send_c.at[0], recv_sem=recv_c.at[c],
            device_id={"tp": partner}, device_id_type=MESH).wait_recv()

    def repack(c):
        spread[...] = raw[c].reshape(B * BLK * 8, 64).astype(F32)
        for p in range(NTP):
            lo = spread[pl.ds(2 * p, B * BLK, stride=8), :]
            hi = spread[pl.ds(2 * p + 1, B * BLK, stride=8), :]
            snd[c, p] = jnp.concatenate([lo, hi], axis=1).astype(BF16).reshape(B, BLK, 128)
        kall[c, me] = snd[c, me]

    raw_copy(0).wait()
    for i in range(len(smalls)):
        small_copy(i).start()
    repack(0)
    pl.semaphore_wait(barrier, 3)
    for n in range(3):
        cache_send(0, n)
    raw_copy(1).wait()
    raw_copy(2).start()
    raw_copy(3).start()
    repack(1)
    for n in range(3):
        cache_send(1, n)
    for i in range(len(smalls)):
        small_copy(i).wait()
    raw_copy(2).wait()
    raw_copy(3).wait()
    start_layer(0)
    repack(2)
    cache_send(2, 0)
    cache_send(2, 2)
    repack(3)
    cache_send(3, 2)


    eye = lax.broadcasted_iota(jnp.int32, (B, B), 0) == lax.broadcasted_iota(jnp.int32, (B, B), 1)
    len_row = jnp.broadcast_to(lens[...].astype(F32), (B, B))
    len_col = jnp.sum(jnp.where(eye, len_row, 0.0), axis=1, keepdims=True)
    len_b = jnp.broadcast_to(len_col, (B, 128))
    angle = len_b * inv[...]
    cosv, sinv = jnp.cos(angle), jnp.sin(angle)
    lane = lax.broadcasted_iota(jnp.int32, (B, 128), 1)
    low = (lane % 64) < 32
    left = lane < 64
    col = lax.broadcasted_iota(jnp.int32, (64, 1024), 1)
    row = lax.broadcasted_iota(jnp.int32, (64, 1024), 0)
    len64 = jnp.concatenate([len_col] * 4, axis=0)
    pos = ((col // 256) * BLK + col % BLK).astype(F32)
    valid = (((col // BLK) % B) == (row % B)) & (pos < len64)

    h_f = hid[...].astype(F32)

    def emit(c, new):
        new3 = jnp.broadcast_to(new[:, None, :], (B, BLK, 128))
        len3 = jnp.broadcast_to(len_b[:, None, :], (B, BLK, 128))
        pos3 = lax.broadcasted_iota(jnp.int32, (B, BLK, 128), 1).astype(F32)
        for s in range(NTP):
            x = jnp.where(pos3 + float(s * BLK) == len3, new3, kall[c, s].astype(F32)).reshape(B * BLK, 128)
            spread[pl.ds(0, B * BLK, stride=2), :] = x[:, :64]
            spread[pl.ds(1, B * BLK, stride=2), :] = x[:, 64:]
            outs[c][:, pl.ds(s * 2 * BLK, 2 * BLK), :] = spread[pl.ds(0, 2 * B * BLK), :].astype(BF16).reshape(B, 2 * BLK, 64)

    def x_send(step, piece, val):
        sl = pl.ds(*PIECES[step % 2][piece])
        xown[step, :, sl] = val
        for n in range(3):
            pltpu.make_async_remote_copy(
                src_ref=xown.at[step, :, sl], dst_ref=xrecv.at[step, me, :, sl],
                send_sem=send_x.at[0], recv_sem=recv_x.at[step],
                device_id={"tp": peers[n]}, device_id_type=MESH).start()
        xrecv[step, me, :, sl] = val

    def x_sum(step):
        pltpu.make_async_remote_copy(
            src_ref=xrecv.at[step, pl.ds(0, 3)], dst_ref=xrecv.at[step, pl.ds(0, 3)],
            send_sem=send_x.at[0], recv_sem=recv_x.at[step],
            device_id={"tp": partner}, device_id_type=MESH).wait_recv()
        tot = xrecv[step, 0].astype(F32)
        for s in range(1, NTP):
            tot = tot + xrecv[step, s].astype(F32)
        return tot

    outs = (ok1, ov1, ok2, ov2)

    for l in range(2):
        a = _norm(h_f, ga[pl.ds(l, 1), :].astype(F32))
        qf = jnp.dot(a, wq[l], preferred_element_type=F32)
        kf = jnp.dot(a, wk[l], preferred_element_type=F32)
        vf = jnp.dot(a, wv[l], preferred_element_type=F32)
        q0 = _rope(qf[:, :128], cosv, sinv, low)
        q1 = _rope(qf[:, 128:], cosv, sinv, low)
        knew = _rope(kf, cosv, sinv, low).astype(BF16).astype(F32)
        vnew = vf.astype(BF16).astype(F32)
        zero = jnp.zeros_like(q0)
        qrows = jnp.concatenate([
            jnp.where(left, q0, zero), jnp.where(left, pltpu.roll(q0, 64, 1), zero),
            jnp.where(left, zero, pltpu.roll(q1, 64, 1)), jnp.where(left, zero, q1)], axis=0).astype(BF16)
        kc, vc = 2 * l, 2 * l + 1
        cache_wait(kc)
        k2d = kall[kc].reshape(NTP * B * BLK, 128)
        sc = lax.dot_general(qrows, k2d, (((1,), (1,)), ((), ())), preferred_element_type=F32) * 0.125
        sc = jnp.where(valid, sc, -1e30)
        ns = jnp.sum(qrows.astype(F32) * jnp.concatenate([knew] * 4, axis=0), axis=1, keepdims=True) * 0.125
        top = jnp.maximum(jnp.max(sc, axis=1, keepdims=True), ns)
        ex, nex = jnp.exp(sc - top), jnp.exp(ns - top)
        den = jnp.sum(ex, axis=1, keepdims=True) + nex
        prob = (ex / den).astype(BF16)
        nprob = (nex / den).astype(BF16).astype(F32)
        cache_wait(vc)
        v2d = kall[vc].reshape(NTP * B * BLK, 128)
        ov = jnp.dot(prob, v2d, preferred_element_type=F32) + nprob * jnp.concatenate([vnew] * 4, axis=0)
        attn = jnp.concatenate([jnp.where(left, ov[0:16], ov[48:64]), jnp.where(left, ov[16:32], ov[32:48])], axis=1).astype(BF16)
        wo_rows = jnp.concatenate([wo[l, pl.ds(0, 64), :], wo[l, pl.ds(192, 64), :], wo[l, pl.ds(64, 128), :]], axis=0)
        x_send(2 * l, 0, jnp.dot(attn, wo_rows, preferred_element_type=F32).astype(BF16))
        if l == 0:
            cache_send(2, 1)
            cache_send(3, 0)
            cache_send(3, 1)
        emit(kc, knew)
        emit(vc, vnew)
        for k in range(3):
            w_copy(l, k).wait()
        if l == 0:
            start_layer(1)
        h1 = (h_f + x_sum(2 * l)).astype(BF16).astype(F32)
        m = _norm(h1, gm[pl.ds(l, 1), :].astype(F32))

        lg = lax.dot_general(wr[l], m, (((1,), (1,)), ((), ())), preferred_element_type=F32)
        eid = lax.broadcasted_iota(jnp.int32, (EXP, B), 0)
        chosen = eid < 0
        for k in range(8):
            chosen = chosen | (cho[l, pl.ds(k, 1), :] == eid)
        lg = jnp.where(chosen, lg, -jnp.inf)
        ex = jnp.where(chosen, jnp.exp(lg - jnp.max(lg, axis=0, keepdims=True)), 0.0)
        gate_t = ex / jnp.sum(ex, axis=0, keepdims=True)
        gate = gate_t.T
        for e in range(EXP):
            w = jnp.concatenate([wg[l, e], wu[l, e]], axis=1)
            gu = jnp.dot(m, w, preferred_element_type=F32)
            g, u = gu[:, :FL], gu[:, FL:]
            act[:, pl.ds(e * FL, FL)] = (g * jax.nn.sigmoid(g) * u * jnp.broadcast_to(gate[:, e:e + 1], (B, FL))).astype(BF16)
        def down(piece, pairs, acc):
            first, width = PIECES[1][piece]
            for e in pairs:
                rhs = wd[l, pl.ds(e, 2), :, pl.ds(first, width)].reshape(2 * FL, width)
                acc = acc + jnp.dot(act[:, pl.ds(e * FL, 2 * FL)], rhs, preferred_element_type=F32)
            return acc

        acc0 = down(0, range(0, EXP, 2), jnp.zeros((B, PIECES[1][0][1]), F32))
        acc1 = down(1, range(0, 8, 2), jnp.zeros((B, PIECES[1][1][1]), F32))
        x_send(2 * l + 1, 0, acc0.astype(BF16))
        acc1 = down(1, range(8, EXP, 2), acc1)
        x_send(2 * l + 1, 1, acc1.astype(BF16))
        h_f = (h1 + x_sum(2 * l + 1)).astype(BF16).astype(F32)

    hout[...] = h_f.astype(BF16)
    pltpu.make_async_remote_copy(
        src_ref=snd.at[:, pl.ds(0, 3)], dst_ref=kall.at[:, pl.ds(0, 3)], send_sem=send_c.at[0], recv_sem=recv_c.at[0],
        device_id={"tp": partner}, device_id_type=MESH).wait_send()
    pltpu.make_async_remote_copy(
        src_ref=xrecv.at[:, pl.ds(0, 3)], dst_ref=xrecv.at[:, pl.ds(0, 3)], send_sem=send_x.at[0], recv_sem=recv_x.at[0],
        device_id={"tp": partner}, device_id_type=MESH).wait_send()


def _store(h, k1, v1, k2, v2, ho, ok1, ov1, ok2, ov2, sem):
    copies = [pltpu.make_async_copy(a, b, sem.at[i])
              for i, (a, b) in enumerate(((k1, ok1), (v1, ov1), (k2, ok2), (v2, ov2), (h, ho)))]
    for c in copies:
        c.start()
    for c in copies:
        c.wait()


def solution(mesh):
    seq_spec = P('dp', 'tp', None, None)
    head_spec = P('dp', None, 'tp', None)
    col_spec = P(None, None, 'tp')
    ff_spec = P(None, None, None, 'tp')
    inv_freq = (THETA ** (-2.0 * np.arange(32, dtype=np.float64) / 64)).astype(np.float32)
    inv_row = np.tile(inv_freq, 4)[None, :]

    def local_step(hidden, lengths, choice, keys_one, vals_one, keys_two, vals_two, g_attn, w_q, w_k, w_v, w_o, g_mlp, w_router, w_gate, w_up, w_down):
        shapes = (jax.ShapeDtypeStruct((B, D), BF16),) + (jax.ShapeDtypeStruct((B, 2 * SEQ, 64), BF16),) * 4
        any_spec = pl.BlockSpec(memory_space=pl.ANY)
        vmem_spec = pl.BlockSpec(memory_space=pltpu.VMEM)
        V = pltpu.VMEM
        DMA = pltpu.SemaphoreType.DMA
        outs = pl.pallas_call(
            _kernel,
            out_shape=tuple(V(s.shape, s.dtype) for s in shapes),
            in_specs=[any_spec] * 18,
            out_specs=(vmem_spec,) * 5,
            scratch_shapes=[
                V((B, D), BF16), V((1, B), jnp.int32), V((2, 8, B), jnp.int32), V((4, B, BLK, 8, 64), BF16),
                V((2, D), BF16), V((2, D, 256), BF16), V((2, D, 128), BF16), V((2, D, 128), BF16), V((2, 256, D), BF16),
                V((2, D), BF16), V((2, EXP, D), BF16), V((2, EXP, D, FL), BF16), V((2, EXP, D, FL), BF16), V((2, EXP, FL, D), BF16),
                V((1, 128), F32),
                V((B * BLK * 8, 64), F32), V((4, NTP, B, BLK, 128), BF16), V((4, NTP, B, BLK, 128), BF16),
                V((4, B, D), BF16), V((4, NTP, B, D), BF16), V((B, EXP * FL), BF16),
                DMA((11,)), DMA((4,)), DMA((2, 3)), DMA((1,)), DMA((4,)), DMA((1,)), DMA((4,)),
            ],
            compiler_params=pltpu.CompilerParams(collective_id=0, has_side_effects=True, vmem_limit_bytes=64_000_000),
        )(hidden, lengths.reshape(1, B), jnp.transpose(choice, (0, 2, 1)), keys_one, vals_one, keys_two, vals_two,
          g_attn, w_q, w_k, w_v, w_o, g_mlp, jnp.transpose(w_router, (0, 2, 1)), w_gate, w_up, w_down, jnp.asarray(inv_row))
        outs = pl.pallas_call(
            _store,
            out_shape=shapes,
            in_specs=[vmem_spec] * 5,
            out_specs=(any_spec,) * 5,
            scratch_shapes=[DMA((5,))],
        )(*[pltpu.with_memory_space_constraint(o, pltpu.VMEM) for o in outs])
        return (outs[0],) + tuple(o.reshape(B, SEQ, 2, 64) for o in outs[1:])

    return jax.shard_map(local_step, mesh=mesh, in_specs=(P('dp', None), P('dp'), P(None, 'dp', None), seq_spec, seq_spec, seq_spec, seq_spec, P(), col_spec, col_spec, col_spec, P(None, 'tp', None), P(), P(), ff_spec, ff_spec, P(None, None, 'tp', None)), out_specs=(P('dp', None), head_spec, head_spec, head_spec, head_spec), check_vma=False)
```

```python
import functools

import numpy as np

import jax
import jax.numpy as jnp
from jax import lax
from jax.experimental import pallas as pl
from jax.experimental.pallas import tpu as pltpu
from jax.sharding import PartitionSpec as P

EPS = 1e-5
THETA = 1000000.0
MESH = pl.DeviceIdType.MESH
B = 16
D = 1024
SEQ = 64
BLK = 16
NTP = 4
EXP = 32
FL = 128
PIECES = (((0, 1024),), ((0, 512), (512, 512)))
NP = 2
F32 = jnp.float32
BF16 = jnp.bfloat16


def _norm(h_f, gain_row):
    scale = lax.rsqrt(jnp.mean(h_f * h_f, axis=-1, keepdims=True) + EPS)
    return (h_f * scale * gain_row).astype(BF16)


def _rope(x, cosv, sinv, low):
    rot = jnp.where(low, -pltpu.roll(x, 96, 1), pltpu.roll(x, 32, 1))
    return x * cosv + rot * sinv


def _kernel(hid_h, len_h, cho_h, k1_h, v1_h, k2_h, v2_h, ga_h, wq_h, wk_h, wv_h, wo_h, gm_h, wr_h, wg_h, wu_h, wd_h, inv_h,
            hout, ok1, ov1, ok2, ov2,
            hid, lens, cho, raw, ga, wq, wk, wv, wo, gm, wr, wg, wu, wd, inv,
            spread, snd, kall, xown, xrecv, act, qown, qx, sown, sx, emat,
            sem_s, sem_raw, sem_w, send_c, recv_c, send_x, recv_x, send_q, recv_q, send_s, recv_s):
    me = lax.axis_index("tp")
    chip, core = me // 2, me % 2
    partner = chip * 2 + (1 - core)
    cross_a = (1 - chip) * 2 + core
    cross_b = (1 - chip) * 2 + (1 - core)
    peers = (cross_a, cross_b, partner)

    barrier = pltpu.get_barrier_semaphore()
    for p in peers:
        pl.semaphore_signal(barrier, inc=1, device_id={"tp": p}, device_id_type=MESH)

    raw_src = (k1_h, v1_h, k2_h, v2_h)

    def raw_copy(c):
        return pltpu.make_async_copy(raw_src[c], raw.at[c], sem_raw.at[c])

    smalls = ((hid_h, hid), (len_h, lens), (cho_h, cho), (ga_h, ga), (gm_h, gm), (inv_h, inv),
              (wq_h, wq), (wk_h, wk), (wv_h, wv), (wo_h, wo), (wr_h, wr))

    def small_copy(i):
        return pltpu.make_async_copy(smalls[i][0], smalls[i][1], sem_s.at[i])

    def w_copy(l, k):
        src, dst = ((wg_h, wg), (wu_h, wu), (wd_h, wd))[k]
        return pltpu.make_async_copy(src.at[l], dst.at[l], sem_w.at[l, k])

    FIRST = (0, 1, 3, 5, 6, 7, 8)
    for i in FIRST:
        small_copy(i).start()
    raw_copy(1).start()
    raw_copy(0).start()

    def start_layer(l):
        for k in range(3):
            w_copy(l, k).start()

    def cache_send(c, n):
        pltpu.make_async_remote_copy(
            src_ref=snd.at[c, peers[n]], dst_ref=kall.at[c, me],
            send_sem=send_c.at[0], recv_sem=recv_c.at[c],
            device_id={"tp": peers[n]}, device_id_type=MESH).start()

    def cache_wait(c):
        pltpu.make_async_remote_copy(
            src_ref=snd.at[c, pl.ds(0, 3)], dst_ref=kall.at[c, pl.ds(0, 3)],
            send_sem=send_c.at[0], recv_sem=recv_c.at[c],
            device_id={"tp": partner}, device_id_type=MESH).wait_recv()

    def repack(c):
        spread[...] = raw[c].reshape(B * BLK * 8, 64).astype(F32)
        for p in range(NTP):
            lo = spread[pl.ds(2 * p, B * BLK, stride=8), :]
            hi = spread[pl.ds(2 * p + 1, B * BLK, stride=8), :]
            snd[c, p] = jnp.concatenate([lo, hi], axis=1).astype(BF16).reshape(B, BLK, 128)
        kall[c, me] = snd[c, me]

    for i in FIRST:
        small_copy(i).wait()

    eye = lax.broadcasted_iota(jnp.int32, (B, B), 0) == lax.broadcasted_iota(jnp.int32, (B, B), 1)
    len_row = jnp.broadcast_to(lens[...].astype(F32), (B, B))
    len_col = jnp.sum(jnp.where(eye, len_row, 0.0), axis=1, keepdims=True)
    len_b = jnp.broadcast_to(len_col, (B, 128))
    angle = len_b * inv[...]
    cosv, sinv = jnp.cos(angle), jnp.sin(angle)
    lane = lax.broadcasted_iota(jnp.int32, (B, 128), 1)
    low = (lane % 64) < 32
    left = lane < 64
    col = lax.broadcasted_iota(jnp.int32, (64, 1024), 1)
    row = lax.broadcasted_iota(jnp.int32, (64, 1024), 0)
    len64 = jnp.concatenate([len_col] * 4, axis=0)
    pos = ((col // 256) * BLK + col % BLK).astype(F32)
    valid = (((col // BLK) % B) == (row % B)) & (pos < len64)

    h_f = hid[...].astype(F32)

    def project(l, h_f):
        a = _norm(h_f, ga[pl.ds(l, 1), :].astype(F32))
        qf = jnp.dot(a, wq[l], preferred_element_type=F32)
        kf = jnp.dot(a, wk[l], preferred_element_type=F32)
        vf = jnp.dot(a, wv[l], preferred_element_type=F32)
        q = jnp.concatenate([_rope(qf[:, :128], cosv, sinv, low), _rope(qf[:, 128:], cosv, sinv, low)], axis=1).astype(BF16)
        return q, _rope(kf, cosv, sinv, low).astype(BF16).astype(F32), vf.astype(BF16).astype(F32)

    def head_rows(q):
        q0, q1 = q[:, :128].astype(F32), q[:, 128:].astype(F32)
        zero = jnp.zeros_like(q0)
        return jnp.concatenate([
            jnp.where(left, q0, zero), jnp.where(left, pltpu.roll(q0, 64, 1), zero),
            jnp.where(left, zero, pltpu.roll(q1, 64, 1)), jnp.where(left, zero, q1)], axis=0).astype(BF16)

    def swap(src, dst, send, recv, n):
        pltpu.make_async_remote_copy(src_ref=src, dst_ref=dst, send_sem=send.at[0], recv_sem=recv.at[0],
                                     device_id={"tp": peers[n]}, device_id_type=MESH).start()

    def swapped(ref, send, recv):
        return pltpu.make_async_remote_copy(src_ref=ref.at[pl.ds(0, 3)], dst_ref=ref.at[pl.ds(0, 3)], send_sem=send.at[0],
                                            recv_sem=recv.at[0], device_id={"tp": partner}, device_id_type=MESH)

    q, knew, vnew = project(0, h_f)
    qown[...] = q
    pl.semaphore_wait(barrier, 3)
    for n in range(3):
        swap(qown, qx.at[me], send_q, recv_q, n)
    qx[me] = q
    raw_copy(1).wait()
    repack(1)
    for n in range(3):
        cache_send(1, n)
    raw_copy(0).wait()
    for i in range(len(smalls)):
        if i not in FIRST:
            small_copy(i).start()
    raw_copy(2).start()
    raw_copy(3).start()
    repack(0)
    lane8 = lax.broadcasted_iota(jnp.int32, (8, 128), 1) // BLK
    colk = lax.broadcasted_iota(jnp.int32, (64, 256), 1)
    rowk = lax.broadcasted_iota(jnp.int32, (64, 256), 0)
    own_b = ((colk // BLK) % B) == (rowk % B)
    ecol = lax.broadcasted_iota(jnp.int32, (128, 1024), 1)
    erow = lax.broadcasted_iota(jnp.int32, (128, 1024), 0)
    emat[...] = jnp.where((ecol // 256) * BLK + ecol % BLK == erow, 1.0, 0.0).astype(BF16)
    swapped(qx, send_q, recv_q).wait_recv()
    for p in range(NTP):
        sk = lax.dot_general(head_rows(qx[p]), snd[0, p].reshape(B * BLK, 128), (((1,), (1,)), ((), ())), preferred_element_type=F32) * 0.125
        sk = jnp.where(own_b, sk, 0.0)
        sk = sk[:, :128] + sk[:, 128:]
        for shift in (64, 32, 16):
            sk = sk + pltpu.roll(sk, shift, 1)
        packed = sk[0:8]
        for k in range(1, 8):
            packed = jnp.where(lane8 == k, sk[8 * k:8 * k + 8], packed)
        sown[p] = packed
    for n in range(3):
        swap(sown.at[peers[n]], sx.at[me], send_s, recv_s, n)
    sx[me] = sown[me]
    for i in range(len(smalls)):
        if i not in FIRST:
            small_copy(i).wait()
    raw_copy(2).wait()
    raw_copy(3).wait()
    start_layer(0)
    repack(2)
    cache_send(2, 0)
    cache_send(2, 2)
    repack(3)
    cache_send(3, 2)
    cache_send(0, 2)

    def emit(c, new):
        new3 = jnp.broadcast_to(new[:, None, :], (B, BLK, 128))
        len3 = jnp.broadcast_to(len_b[:, None, :], (B, BLK, 128))
        pos3 = lax.broadcasted_iota(jnp.int32, (B, BLK, 128), 1).astype(F32)
        for s in range(NTP):
            x = jnp.where(pos3 + float(s * BLK) == len3, new3, kall[c, s].astype(F32)).reshape(B * BLK, 128)
            spread[pl.ds(0, B * BLK, stride=2), :] = x[:, :64]
            spread[pl.ds(1, B * BLK, stride=2), :] = x[:, 64:]
            outs[c][:, pl.ds(s * 2 * BLK, 2 * BLK), :] = spread[pl.ds(0, 2 * B * BLK), :].astype(BF16).reshape(B, 2 * BLK, 64)

    def x_send(step, piece, val):
        sl = pl.ds(*PIECES[step % 2][piece])
        xown[step, :, sl] = val
        for n in range(3):
            pltpu.make_async_remote_copy(
                src_ref=xown.at[step, :, sl], dst_ref=xrecv.at[step, me, :, sl],
                send_sem=send_x.at[0], recv_sem=recv_x.at[step],
                device_id={"tp": peers[n]}, device_id_type=MESH).start()
        xrecv[step, me, :, sl] = val

    def x_sum(step):
        pltpu.make_async_remote_copy(
            src_ref=xrecv.at[step, pl.ds(0, 3)], dst_ref=xrecv.at[step, pl.ds(0, 3)],
            send_sem=send_x.at[0], recv_sem=recv_x.at[step],
            device_id={"tp": partner}, device_id_type=MESH).wait_recv()
        tot = xrecv[step, 0].astype(F32)
        for s in range(1, NTP):
            tot = tot + xrecv[step, s].astype(F32)
        return tot

    outs = (ok1, ov1, ok2, ov2)

    for l in range(2):
        if l == 1:
            q, knew, vnew = project(l, h_f)
        qrows = head_rows(q)
        kc, vc = 2 * l, 2 * l + 1
        ns = jnp.sum(qrows.astype(F32) * jnp.concatenate([knew] * 4, axis=0), axis=1, keepdims=True) * 0.125
        if l == 0:
            swapped(sx, send_s, recv_s).wait_recv()
            rows = []
            for k in range(8):
                acc = jnp.zeros((8, 128), F32)
                for sd in range(NTP):
                    shift = (BLK * (sd - k)) % 128
                    part = sx[sd] if shift == 0 else pltpu.roll(sx[sd], shift, 1)
                    acc = jnp.where(lane8 == sd, part, acc)
                rows.append(acc)
            sc = jnp.concatenate(rows, axis=0)
            ok = lax.broadcasted_iota(jnp.int32, (64, 128), 1).astype(F32) < len64
        else:
            cache_wait(kc)
            k2d = kall[kc].reshape(NTP * B * BLK, 128)
            sc = lax.dot_general(qrows, k2d, (((1,), (1,)), ((), ())), preferred_element_type=F32) * 0.125
            ok = valid
        sc = jnp.where(ok, sc, -1e30)
        top = jnp.maximum(jnp.max(sc, axis=1, keepdims=True), ns)
        ex, nex = jnp.exp(sc - top), jnp.exp(ns - top)
        den = jnp.sum(ex, axis=1, keepdims=True) + nex
        prob = (ex / den).astype(BF16)
        nprob = (nex / den).astype(BF16).astype(F32)
        if l == 0:
            wide = jnp.dot(prob, emat[...], preferred_element_type=F32)
            prob = jnp.where(valid, wide, 0.0).astype(BF16)
        cache_wait(vc)
        v2d = kall[vc].reshape(NTP * B * BLK, 128)
        ov = jnp.dot(prob, v2d, preferred_element_type=F32) + nprob * jnp.concatenate([vnew] * 4, axis=0)
        attn = jnp.concatenate([jnp.where(left, ov[0:16], ov[48:64]), jnp.where(left, ov[16:32], ov[32:48])], axis=1).astype(BF16)
        wo_rows = jnp.concatenate([wo[l, pl.ds(0, 64), :], wo[l, pl.ds(192, 64), :], wo[l, pl.ds(64, 128), :]], axis=0)
        x_send(2 * l, 0, jnp.dot(attn, wo_rows, preferred_element_type=F32).astype(BF16))
        if l == 0:
            cache_send(2, 1)
            cache_send(3, 0)
            cache_send(3, 1)
        else:
            cache_send(0, 0)
            cache_send(0, 1)
            emit(kc, knew)
        emit(vc, vnew)
        for k in range(3):
            w_copy(l, k).wait()
        if l == 0:
            start_layer(1)
        h1 = (h_f + x_sum(2 * l)).astype(BF16).astype(F32)
        m = _norm(h1, gm[pl.ds(l, 1), :].astype(F32))

        lg = lax.dot_general(wr[l], m, (((1,), (1,)), ((), ())), preferred_element_type=F32)
        eid = lax.broadcasted_iota(jnp.int32, (EXP, B), 0)
        chosen = eid < 0
        for k in range(8):
            chosen = chosen | (cho[l, pl.ds(k, 1), :] == eid)
        lg = jnp.where(chosen, lg, -jnp.inf)
        ex = jnp.where(chosen, jnp.exp(lg - jnp.max(lg, axis=0, keepdims=True)), 0.0)
        gate_t = ex / jnp.sum(ex, axis=0, keepdims=True)
        gate = gate_t.T
        for e in range(EXP):
            w = jnp.concatenate([wg[l, e], wu[l, e]], axis=1)
            gu = jnp.dot(m, w, preferred_element_type=F32)
            g, u = gu[:, :FL], gu[:, FL:]
            act[:, pl.ds(e * FL, FL)] = (g * jax.nn.sigmoid(g) * u * jnp.broadcast_to(gate[:, e:e + 1], (B, FL))).astype(BF16)
        def down(piece, pairs, acc):
            first, width = PIECES[1][piece]
            for e in pairs:
                rhs = wd[l, pl.ds(e, 2), :, pl.ds(first, width)].reshape(2 * FL, width)
                acc = acc + jnp.dot(act[:, pl.ds(e * FL, 2 * FL)], rhs, preferred_element_type=F32)
            return acc

        acc0 = down(0, range(0, EXP, 2), jnp.zeros((B, PIECES[1][0][1]), F32))
        acc1 = down(1, range(0, 8, 2), jnp.zeros((B, PIECES[1][1][1]), F32))
        x_send(2 * l + 1, 0, acc0.astype(BF16))
        acc1 = down(1, range(8, EXP, 2), acc1)
        x_send(2 * l + 1, 1, acc1.astype(BF16))
        if l == 0:
            kone = knew
        else:
            cache_wait(0)
            emit(0, kone)
        h_f = (h1 + x_sum(2 * l + 1)).astype(BF16).astype(F32)

    hout[...] = h_f.astype(BF16)
    swapped(qx, send_q, recv_q).wait_send()
    swapped(sx, send_s, recv_s).wait_send()
    pltpu.make_async_remote_copy(
        src_ref=snd.at[:, pl.ds(0, 3)], dst_ref=kall.at[:, pl.ds(0, 3)], send_sem=send_c.at[0], recv_sem=recv_c.at[0],
        device_id={"tp": partner}, device_id_type=MESH).wait_send()
    pltpu.make_async_remote_copy(
        src_ref=xrecv.at[:, pl.ds(0, 3)], dst_ref=xrecv.at[:, pl.ds(0, 3)], send_sem=send_x.at[0], recv_sem=recv_x.at[0],
        device_id={"tp": partner}, device_id_type=MESH).wait_send()


def _store(h, k1, v1, k2, v2, ho, ok1, ov1, ok2, ov2, sem):
    copies = [pltpu.make_async_copy(a, b, sem.at[i])
              for i, (a, b) in enumerate(((k1, ok1), (v1, ov1), (k2, ok2), (v2, ov2), (h, ho)))]
    for c in copies:
        c.start()
    for c in copies:
        c.wait()


def solution(mesh):
    seq_spec = P('dp', 'tp', None, None)
    head_spec = P('dp', None, 'tp', None)
    col_spec = P(None, None, 'tp')
    ff_spec = P(None, None, None, 'tp')
    inv_freq = (THETA ** (-2.0 * np.arange(32, dtype=np.float64) / 64)).astype(np.float32)
    inv_row = np.tile(inv_freq, 4)[None, :]

    def local_step(hidden, lengths, choice, keys_one, vals_one, keys_two, vals_two, g_attn, w_q, w_k, w_v, w_o, g_mlp, w_router, w_gate, w_up, w_down):
        shapes = (jax.ShapeDtypeStruct((B, D), BF16),) + (jax.ShapeDtypeStruct((B, 2 * SEQ, 64), BF16),) * 4
        any_spec = pl.BlockSpec(memory_space=pl.ANY)
        vmem_spec = pl.BlockSpec(memory_space=pltpu.VMEM)
        V = pltpu.VMEM
        DMA = pltpu.SemaphoreType.DMA
        outs = pl.pallas_call(
            _kernel,
            out_shape=tuple(V(s.shape, s.dtype) for s in shapes),
            in_specs=[any_spec] * 18,
            out_specs=(vmem_spec,) * 5,
            scratch_shapes=[
                V((B, D), BF16), V((1, B), jnp.int32), V((2, 8, B), jnp.int32), V((4, B, BLK, 8, 64), BF16),
                V((2, D), BF16), V((2, D, 256), BF16), V((2, D, 128), BF16), V((2, D, 128), BF16), V((2, 256, D), BF16),
                V((2, D), BF16), V((2, EXP, D), BF16), V((2, EXP, D, FL), BF16), V((2, EXP, D, FL), BF16), V((2, EXP, FL, D), BF16),
                V((1, 128), F32),
                V((B * BLK * 8, 64), F32), V((4, NTP, B, BLK, 128), BF16), V((4, NTP, B, BLK, 128), BF16),
                V((4, B, D), BF16), V((4, NTP, B, D), BF16), V((B, EXP * FL), BF16), V((B, 256), BF16), V((NTP, B, 256), BF16), V((NTP, 8, 128), F32), V((NTP, 8, 128), F32), V((128, 1024), BF16),
                DMA((11,)), DMA((4,)), DMA((2, 3)), DMA((1,)), DMA((4,)), DMA((1,)), DMA((4,)), DMA((1,)), DMA((1,)), DMA((1,)), DMA((1,)),
            ],
            compiler_params=pltpu.CompilerParams(collective_id=0, has_side_effects=True, vmem_limit_bytes=64_000_000),
        )(hidden, lengths.reshape(1, B), jnp.transpose(choice, (0, 2, 1)), keys_one, vals_one, keys_two, vals_two,
          g_attn, w_q, w_k, w_v, w_o, g_mlp, jnp.transpose(w_router, (0, 2, 1)), w_gate, w_up, w_down, jnp.asarray(inv_row))
        outs = pl.pallas_call(
            _store,
            out_shape=shapes,
            in_specs=[vmem_spec] * 5,
            out_specs=(any_spec,) * 5,
            scratch_shapes=[DMA((5,))],
        )(*[pltpu.with_memory_space_constraint(o, pltpu.VMEM) for o in outs])
        return (outs[0],) + tuple(o.reshape(B, SEQ, 2, 64) for o in outs[1:])

    return jax.shard_map(local_step, mesh=mesh, in_specs=(P('dp', None), P('dp'), P(None, 'dp', None), seq_spec, seq_spec, seq_spec, seq_spec, P(), col_spec, col_spec, col_spec, P(None, 'tp', None), P(), P(), ff_spec, ff_spec, P(None, None, 'tp', None)), out_specs=(P('dp', None), head_spec, head_spec, head_spec, head_spec), check_vma=False)
```

```python
import functools

import numpy as np

import jax
import jax.numpy as jnp
from jax import lax
from jax.experimental import pallas as pl
from jax.experimental.pallas import tpu as pltpu
from jax.sharding import PartitionSpec as P

EPS = 1e-5
THETA = 1000000.0
MESH = pl.DeviceIdType.MESH
B = 16
D = 1024
SEQ = 64
BLK = 16
NTP = 4
EXP = 32
FL = 128
PIECES = (((0, 1024),), ((0, 512), (512, 512)))
NP = 2
F32 = jnp.float32
BF16 = jnp.bfloat16


def _norm(h_f, gain_row):
    scale = lax.rsqrt(jnp.mean(h_f * h_f, axis=-1, keepdims=True) + EPS)
    return (h_f * scale * gain_row).astype(BF16)


def _rope(x, cosv, sinv, low):
    rot = jnp.where(low, -pltpu.roll(x, 96, 1), pltpu.roll(x, 32, 1))
    return x * cosv + rot * sinv


def _kernel(hid_h, len_h, cho_h, k1_h, v1_h, k2_h, v2_h, ga_h, wq_h, wk_h, wv_h, wo_h, gm_h, wr_h, wg_h, wu_h, wd_h, inv_h,
            hout, ok1, ov1, ok2, ov2,
            hid, lens, cho, raw, ga, wq, wk, wv, wo, gm, wr, wg, wu, wd, inv,
            spread, snd, kall, xown, xrecv, act, qown, qx, sown, sx, emat,
            sem_s, sem_raw, sem_w, send_c, recv_c, send_x, recv_x, send_q, recv_q, send_s, recv_s):
    me = lax.axis_index("tp")
    chip, core = me // 2, me % 2
    partner = chip * 2 + (1 - core)
    cross_a = (1 - chip) * 2 + core
    cross_b = (1 - chip) * 2 + (1 - core)
    peers = (cross_a, cross_b, partner)

    barrier = pltpu.get_barrier_semaphore()
    for p in peers:
        pl.semaphore_signal(barrier, inc=1, device_id={"tp": p}, device_id_type=MESH)

    raw_src = (k1_h, v1_h, k2_h, v2_h)

    def raw_copy(c):
        return pltpu.make_async_copy(raw_src[c], raw.at[c], sem_raw.at[c])

    smalls = ((hid_h, hid), (len_h, lens), (cho_h, cho), (ga_h, ga), (gm_h, gm), (inv_h, inv),
              (wq_h, wq), (wk_h, wk), (wv_h, wv), (wo_h, wo), (wr_h, wr))

    def small_copy(i):
        return pltpu.make_async_copy(smalls[i][0], smalls[i][1], sem_s.at[i])

    def w_copy(l, k):
        src, dst = ((wg_h, wg), (wu_h, wu), (wd_h, wd))[k]
        return pltpu.make_async_copy(src.at[l], dst.at[l], sem_w.at[l, k])

    FIRST = (0, 1, 3, 5, 6, 7, 8)
    for i in FIRST:
        small_copy(i).start()
    raw_copy(1).start()
    raw_copy(0).start()

    def start_layer(l):
        for i in range(0, EXP, 4):
            for k in range(3):
                src, dst = ((wg_h, wg), (wu_h, wu), (wd_h, wd))[k]
                sl = pl.ds(i, 4)
                pltpu.make_async_copy(src.at[l, sl], dst.at[l, sl], sem_w.at[l, k]).start()

    def cache_send(c, n):
        pltpu.make_async_remote_copy(
            src_ref=snd.at[c, peers[n]], dst_ref=kall.at[c, me],
            send_sem=send_c.at[0], recv_sem=recv_c.at[c],
            device_id={"tp": peers[n]}, device_id_type=MESH).start()

    def cache_wait(c):
        pltpu.make_async_remote_copy(
            src_ref=snd.at[c, pl.ds(0, 3)], dst_ref=kall.at[c, pl.ds(0, 3)],
            send_sem=send_c.at[0], recv_sem=recv_c.at[c],
            device_id={"tp": partner}, device_id_type=MESH).wait_recv()

    def repack(c):
        spread[...] = raw[c].reshape(B * BLK * 8, 64).astype(F32)
        for p in range(NTP):
            lo = spread[pl.ds(2 * p, B * BLK, stride=8), :]
            hi = spread[pl.ds(2 * p + 1, B * BLK, stride=8), :]
            snd[c, p] = jnp.concatenate([lo, hi], axis=1).astype(BF16).reshape(B, BLK, 128)
        kall[c, me] = snd[c, me]

    for i in FIRST:
        small_copy(i).wait()

    eye = lax.broadcasted_iota(jnp.int32, (B, B), 0) == lax.broadcasted_iota(jnp.int32, (B, B), 1)
    len_row = jnp.broadcast_to(lens[...].astype(F32), (B, B))
    len_col = jnp.sum(jnp.where(eye, len_row, 0.0), axis=1, keepdims=True)
    len_b = jnp.broadcast_to(len_col, (B, 128))
    angle = len_b * inv[...]
    cosv, sinv = jnp.cos(angle), jnp.sin(angle)
    lane = lax.broadcasted_iota(jnp.int32, (B, 128), 1)
    low = (lane % 64) < 32
    left = lane < 64
    col = lax.broadcasted_iota(jnp.int32, (64, 1024), 1)
    row = lax.broadcasted_iota(jnp.int32, (64, 1024), 0)
    len64 = jnp.concatenate([len_col] * 4, axis=0)
    pos = ((col // 256) * BLK + col % BLK).astype(F32)
    valid = (((col // BLK) % B) == (row % B)) & (pos < len64)

    h_f = hid[...].astype(F32)

    def project(l, h_f):
        a = _norm(h_f, ga[pl.ds(l, 1), :].astype(F32))
        qf = jnp.dot(a, wq[l], preferred_element_type=F32)
        kf = jnp.dot(a, wk[l], preferred_element_type=F32)
        vf = jnp.dot(a, wv[l], preferred_element_type=F32)
        q = jnp.concatenate([_rope(qf[:, :128], cosv, sinv, low), _rope(qf[:, 128:], cosv, sinv, low)], axis=1).astype(BF16)
        return q, _rope(kf, cosv, sinv, low).astype(BF16).astype(F32), vf.astype(BF16).astype(F32)

    def head_rows(q):
        q0, q1 = q[:, :128].astype(F32), q[:, 128:].astype(F32)
        zero = jnp.zeros_like(q0)
        return jnp.concatenate([
            jnp.where(left, q0, zero), jnp.where(left, pltpu.roll(q0, 64, 1), zero),
            jnp.where(left, zero, pltpu.roll(q1, 64, 1)), jnp.where(left, zero, q1)], axis=0).astype(BF16)

    def swap(src, dst, send, recv, n):
        pltpu.make_async_remote_copy(src_ref=src, dst_ref=dst, send_sem=send.at[0], recv_sem=recv.at[0],
                                     device_id={"tp": peers[n]}, device_id_type=MESH).start()

    def swapped(ref, send, recv):
        return pltpu.make_async_remote_copy(src_ref=ref.at[pl.ds(0, 3)], dst_ref=ref.at[pl.ds(0, 3)], send_sem=send.at[0],
                                            recv_sem=recv.at[0], device_id={"tp": partner}, device_id_type=MESH)

    q, knew, vnew = project(0, h_f)
    qown[...] = q
    pl.semaphore_wait(barrier, 3)
    for n in range(3):
        swap(qown, qx.at[me], send_q, recv_q, n)
    qx[me] = q
    raw_copy(1).wait()
    repack(1)
    for n in range(3):
        cache_send(1, n)
    raw_copy(0).wait()
    for i in range(len(smalls)):
        if i not in FIRST:
            small_copy(i).start()
    raw_copy(2).start()
    raw_copy(3).start()
    start_layer(0)
    repack(0)
    lane8 = lax.broadcasted_iota(jnp.int32, (8, 128), 1) // BLK
    colk = lax.broadcasted_iota(jnp.int32, (64, 256), 1)
    rowk = lax.broadcasted_iota(jnp.int32, (64, 256), 0)
    own_b = ((colk // BLK) % B) == (rowk % B)
    ecol = lax.broadcasted_iota(jnp.int32, (128, 1024), 1)
    erow = lax.broadcasted_iota(jnp.int32, (128, 1024), 0)
    emat[...] = jnp.where((ecol // 256) * BLK + ecol % BLK == erow, 1.0, 0.0).astype(BF16)
    swapped(qx, send_q, recv_q).wait_recv()
    for p in range(NTP):
        sk = lax.dot_general(head_rows(qx[p]), snd[0, p].reshape(B * BLK, 128), (((1,), (1,)), ((), ())), preferred_element_type=F32) * 0.125
        sk = jnp.where(own_b, sk, 0.0)
        sk = sk[:, :128] + sk[:, 128:]
        for shift in (64, 32, 16):
            sk = sk + pltpu.roll(sk, shift, 1)
        packed = sk[0:8]
        for k in range(1, 8):
            packed = jnp.where(lane8 == k, sk[8 * k:8 * k + 8], packed)
        sown[p] = packed
    for n in range(3):
        swap(sown.at[peers[n]], sx.at[me], send_s, recv_s, n)
    sx[me] = sown[me]
    for i in range(len(smalls)):
        if i not in FIRST:
            small_copy(i).wait()
    raw_copy(2).wait()
    raw_copy(3).wait()
    repack(2)
    cache_send(2, 0)
    cache_send(2, 2)
    repack(3)
    cache_send(3, 2)
    cache_send(0, 2)

    def emit(c, new):
        new3 = jnp.broadcast_to(new[:, None, :], (B, BLK, 128))
        len3 = jnp.broadcast_to(len_b[:, None, :], (B, BLK, 128))
        pos3 = lax.broadcasted_iota(jnp.int32, (B, BLK, 128), 1).astype(F32)
        for s in range(NTP):
            x = jnp.where(pos3 + float(s * BLK) == len3, new3, kall[c, s].astype(F32)).reshape(B * BLK, 128)
            spread[pl.ds(0, B * BLK, stride=2), :] = x[:, :64]
            spread[pl.ds(1, B * BLK, stride=2), :] = x[:, 64:]
            outs[c][:, pl.ds(s * 2 * BLK, 2 * BLK), :] = spread[pl.ds(0, 2 * B * BLK), :].astype(BF16).reshape(B, 2 * BLK, 64)

    def x_send(step, piece, val):
        sl = pl.ds(*PIECES[step % 2][piece])
        xown[step, :, sl] = val
        for n in range(3):
            pltpu.make_async_remote_copy(
                src_ref=xown.at[step, :, sl], dst_ref=xrecv.at[step, me, :, sl],
                send_sem=send_x.at[0], recv_sem=recv_x.at[step],
                device_id={"tp": peers[n]}, device_id_type=MESH).start()
        xrecv[step, me, :, sl] = val

    def x_sum(step):
        pltpu.make_async_remote_copy(
            src_ref=xrecv.at[step, pl.ds(0, 3)], dst_ref=xrecv.at[step, pl.ds(0, 3)],
            send_sem=send_x.at[0], recv_sem=recv_x.at[step],
            device_id={"tp": partner}, device_id_type=MESH).wait_recv()
        tot = xrecv[step, 0].astype(F32)
        for s in range(1, NTP):
            tot = tot + xrecv[step, s].astype(F32)
        return tot

    outs = (ok1, ov1, ok2, ov2)

    for l in range(2):
        if l == 1:
            q, knew, vnew = project(l, h_f)
        qrows = head_rows(q)
        kc, vc = 2 * l, 2 * l + 1
        ns = jnp.sum(qrows.astype(F32) * jnp.concatenate([knew] * 4, axis=0), axis=1, keepdims=True) * 0.125
        if l == 0:
            swapped(sx, send_s, recv_s).wait_recv()
            rows = []
            for k in range(8):
                acc = jnp.zeros((8, 128), F32)
                for sd in range(NTP):
                    shift = (BLK * (sd - k)) % 128
                    part = sx[sd] if shift == 0 else pltpu.roll(sx[sd], shift, 1)
                    acc = jnp.where(lane8 == sd, part, acc)
                rows.append(acc)
            sc = jnp.concatenate(rows, axis=0)
            ok = lax.broadcasted_iota(jnp.int32, (64, 128), 1).astype(F32) < len64
        else:
            cache_wait(kc)
            k2d = kall[kc].reshape(NTP * B * BLK, 128)
            sc = lax.dot_general(qrows, k2d, (((1,), (1,)), ((), ())), preferred_element_type=F32) * 0.125
            ok = valid
        sc = jnp.where(ok, sc, -1e30)
        top = jnp.maximum(jnp.max(sc, axis=1, keepdims=True), ns)
        ex, nex = jnp.exp(sc - top), jnp.exp(ns - top)
        den = jnp.sum(ex, axis=1, keepdims=True) + nex
        prob = (ex / den).astype(BF16)
        nprob = (nex / den).astype(BF16).astype(F32)
        if l == 0:
            wide = jnp.dot(prob, emat[...], preferred_element_type=F32)
            prob = jnp.where(valid, wide, 0.0).astype(BF16)
        cache_wait(vc)
        v2d = kall[vc].reshape(NTP * B * BLK, 128)
        ov = jnp.dot(prob, v2d, preferred_element_type=F32) + nprob * jnp.concatenate([vnew] * 4, axis=0)
        attn = jnp.concatenate([jnp.where(left, ov[0:16], ov[48:64]), jnp.where(left, ov[16:32], ov[32:48])], axis=1).astype(BF16)
        wo_rows = jnp.concatenate([wo[l, pl.ds(0, 64), :], wo[l, pl.ds(192, 64), :], wo[l, pl.ds(64, 128), :]], axis=0)
        x_send(2 * l, 0, jnp.dot(attn, wo_rows, preferred_element_type=F32).astype(BF16))
        if l == 0:
            cache_send(2, 1)
            cache_send(3, 0)
            cache_send(3, 1)
        else:
            cache_send(0, 0)
            cache_send(0, 1)
            emit(kc, knew)
        emit(vc, vnew)
        for k in range(3):
            w_copy(l, k).wait()
        if l == 0:
            start_layer(1)
        h1 = (h_f + x_sum(2 * l)).astype(BF16).astype(F32)
        m = _norm(h1, gm[pl.ds(l, 1), :].astype(F32))

        lg = lax.dot_general(wr[l], m, (((1,), (1,)), ((), ())), preferred_element_type=F32)
        eid = lax.broadcasted_iota(jnp.int32, (EXP, B), 0)
        chosen = eid < 0
        for k in range(8):
            chosen = chosen | (cho[l, pl.ds(k, 1), :] == eid)
        lg = jnp.where(chosen, lg, -jnp.inf)
        ex = jnp.where(chosen, jnp.exp(lg - jnp.max(lg, axis=0, keepdims=True)), 0.0)
        gate_t = ex / jnp.sum(ex, axis=0, keepdims=True)
        gate = gate_t.T
        for e in range(EXP):
            w = jnp.concatenate([wg[l, e], wu[l, e]], axis=1)
            gu = jnp.dot(m, w, preferred_element_type=F32)
            g, u = gu[:, :FL], gu[:, FL:]
            act[:, pl.ds(e * FL, FL)] = (g * jax.nn.sigmoid(g) * u * jnp.broadcast_to(gate[:, e:e + 1], (B, FL))).astype(BF16)
        def down(piece, pairs, acc):
            first, width = PIECES[1][piece]
            for e in pairs:
                rhs = wd[l, pl.ds(e, 2), :, pl.ds(first, width)].reshape(2 * FL, width)
                acc = acc + jnp.dot(act[:, pl.ds(e * FL, 2 * FL)], rhs, preferred_element_type=F32)
            return acc

        acc0 = down(0, range(0, EXP, 2), jnp.zeros((B, PIECES[1][0][1]), F32))
        acc1 = down(1, range(0, 8, 2), jnp.zeros((B, PIECES[1][1][1]), F32))
        x_send(2 * l + 1, 0, acc0.astype(BF16))
        acc1 = down(1, range(8, EXP, 2), acc1)
        x_send(2 * l + 1, 1, acc1.astype(BF16))
        if l == 0:
            kone = knew
        else:
            cache_wait(0)
            emit(0, kone)
        h_f = (h1 + x_sum(2 * l + 1)).astype(BF16).astype(F32)

    hout[...] = h_f.astype(BF16)
    swapped(qx, send_q, recv_q).wait_send()
    swapped(sx, send_s, recv_s).wait_send()
    pltpu.make_async_remote_copy(
        src_ref=snd.at[:, pl.ds(0, 3)], dst_ref=kall.at[:, pl.ds(0, 3)], send_sem=send_c.at[0], recv_sem=recv_c.at[0],
        device_id={"tp": partner}, device_id_type=MESH).wait_send()
    pltpu.make_async_remote_copy(
        src_ref=xrecv.at[:, pl.ds(0, 3)], dst_ref=xrecv.at[:, pl.ds(0, 3)], send_sem=send_x.at[0], recv_sem=recv_x.at[0],
        device_id={"tp": partner}, device_id_type=MESH).wait_send()


def _store(h, k1, v1, k2, v2, ho, ok1, ov1, ok2, ov2, sem):
    copies = [pltpu.make_async_copy(a, b, sem.at[i])
              for i, (a, b) in enumerate(((k1, ok1), (v1, ov1), (k2, ok2), (v2, ov2), (h, ho)))]
    for c in copies:
        c.start()
    for c in copies:
        c.wait()


def solution(mesh):
    seq_spec = P('dp', 'tp', None, None)
    head_spec = P('dp', None, 'tp', None)
    col_spec = P(None, None, 'tp')
    ff_spec = P(None, None, None, 'tp')
    inv_freq = (THETA ** (-2.0 * np.arange(32, dtype=np.float64) / 64)).astype(np.float32)
    inv_row = np.tile(inv_freq, 4)[None, :]

    def local_step(hidden, lengths, choice, keys_one, vals_one, keys_two, vals_two, g_attn, w_q, w_k, w_v, w_o, g_mlp, w_router, w_gate, w_up, w_down):
        shapes = (jax.ShapeDtypeStruct((B, D), BF16),) + (jax.ShapeDtypeStruct((B, 2 * SEQ, 64), BF16),) * 4
        any_spec = pl.BlockSpec(memory_space=pl.ANY)
        vmem_spec = pl.BlockSpec(memory_space=pltpu.VMEM)
        V = pltpu.VMEM
        DMA = pltpu.SemaphoreType.DMA
        outs = pl.pallas_call(
            _kernel,
            out_shape=tuple(V(s.shape, s.dtype) for s in shapes),
            in_specs=[any_spec] * 18,
            out_specs=(vmem_spec,) * 5,
            scratch_shapes=[
                V((B, D), BF16), V((1, B), jnp.int32), V((2, 8, B), jnp.int32), V((4, B, BLK, 8, 64), BF16),
                V((2, D), BF16), V((2, D, 256), BF16), V((2, D, 128), BF16), V((2, D, 128), BF16), V((2, 256, D), BF16),
                V((2, D), BF16), V((2, EXP, D), BF16), V((2, EXP, D, FL), BF16), V((2, EXP, D, FL), BF16), V((2, EXP, FL, D), BF16),
                V((1, 128), F32),
                V((B * BLK * 8, 64), F32), V((4, NTP, B, BLK, 128), BF16), V((4, NTP, B, BLK, 128), BF16),
                V((4, B, D), BF16), V((4, NTP, B, D), BF16), V((B, EXP * FL), BF16), V((B, 256), BF16), V((NTP, B, 256), BF16), V((NTP, 8, 128), F32), V((NTP, 8, 128), F32), V((128, 1024), BF16),
                DMA((11,)), DMA((4,)), DMA((2, 3)), DMA((1,)), DMA((4,)), DMA((1,)), DMA((4,)), DMA((1,)), DMA((1,)), DMA((1,)), DMA((1,)),
            ],
            compiler_params=pltpu.CompilerParams(collective_id=0, has_side_effects=True, vmem_limit_bytes=64_000_000),
        )(hidden, lengths.reshape(1, B), jnp.transpose(choice, (0, 2, 1)), keys_one, vals_one, keys_two, vals_two,
          g_attn, w_q, w_k, w_v, w_o, g_mlp, jnp.transpose(w_router, (0, 2, 1)), w_gate, w_up, w_down, jnp.asarray(inv_row))
        outs = pl.pallas_call(
            _store,
            out_shape=shapes,
            in_specs=[vmem_spec] * 5,
            out_specs=(any_spec,) * 5,
            scratch_shapes=[DMA((5,))],
        )(*[pltpu.with_memory_space_constraint(o, pltpu.VMEM) for o in outs])
        return (outs[0],) + tuple(o.reshape(B, SEQ, 2, 64) for o in outs[1:])

    return jax.shard_map(local_step, mesh=mesh, in_specs=(P('dp', None), P('dp'), P(None, 'dp', None), seq_spec, seq_spec, seq_spec, seq_spec, P(), col_spec, col_spec, col_spec, P(None, 'tp', None), P(), P(), ff_spec, ff_spec, P(None, None, 'tp', None)), out_specs=(P('dp', None), head_spec, head_spec, head_spec, head_spec), check_vma=False)
```

```python
import functools

import numpy as np

import jax
import jax.numpy as jnp
from jax import lax
from jax.experimental import pallas as pl
from jax.experimental.pallas import tpu as pltpu
from jax.sharding import PartitionSpec as P

EPS = 1e-5
THETA = 1000000.0
MESH = pl.DeviceIdType.MESH
B = 16
D = 1024
SEQ = 64
BLK = 16
NTP = 4
EXP = 32
FL = 128
PIECES = (((0, 1024),), ((0, 512), (512, 512)))
NP = 2
F32 = jnp.float32
BF16 = jnp.bfloat16


def _norm(h_f, gain_row):
    scale = lax.rsqrt(jnp.mean(h_f * h_f, axis=-1, keepdims=True) + EPS)
    return (h_f * scale * gain_row).astype(BF16)


def _rope(x, cosv, sinv, low):
    rot = jnp.where(low, -pltpu.roll(x, 96, 1), pltpu.roll(x, 32, 1))
    return x * cosv + rot * sinv


def _kernel(hid_h, len_h, cho_h, k1_h, v1_h, k2_h, v2_h, ga_h, wq_h, wk_h, wv_h, wo_h, gm_h, wr_h, wg_h, wu_h, wd_h, inv_h,
            hout, ok1, ov1, ok2, ov2,
            hid, lens, cho, raw, ga, wq, wk, wv, wo, gm, wr, wg, wu, wd, inv,
            spread, snd, kall, xown, xrecv, act, qown, qx, sown, sx, emat,
            sem_s, sem_raw, sem_w, send_c, recv_c, send_x, recv_x, send_q, recv_q, send_s, recv_s):
    me = lax.axis_index("tp")
    chip, core = me // 2, me % 2
    partner = chip * 2 + (1 - core)
    cross_a = (1 - chip) * 2 + core
    cross_b = (1 - chip) * 2 + (1 - core)
    peers = (cross_a, cross_b, partner)

    barrier = pltpu.get_barrier_semaphore()
    for p in peers:
        pl.semaphore_signal(barrier, inc=1, device_id={"tp": p}, device_id_type=MESH)

    raw_src = (k1_h, v1_h, k2_h, v2_h)

    def raw_copy(c):
        return pltpu.make_async_copy(raw_src[c], raw.at[c], sem_raw.at[c])

    smalls = ((hid_h, hid), (len_h, lens), (cho_h, cho), (ga_h, ga), (gm_h, gm), (inv_h, inv),
              (wq_h.at[0], wq.at[0]), (wk_h.at[0], wk.at[0]), (wv_h.at[0], wv.at[0]), (wo_h, wo), (wr_h, wr),
              (wq_h.at[1], wq.at[1]), (wk_h.at[1], wk.at[1]), (wv_h.at[1], wv.at[1]))

    def small_copy(i):
        return pltpu.make_async_copy(smalls[i][0], smalls[i][1], sem_s.at[i])

    def w_copy(l, k):
        src, dst = ((wg_h, wg), (wu_h, wu), (wd_h, wd))[k]
        return pltpu.make_async_copy(src.at[l], dst.at[l], sem_w.at[l, k])

    FIRST = (0, 1, 3, 5, 6, 7, 8)
    for i in FIRST:
        small_copy(i).start()
    raw_copy(1).start()

    def start_layer(l):
        for k in range(3):
            w_copy(l, k).start()

    def cache_send(c, n):
        pltpu.make_async_remote_copy(
            src_ref=snd.at[c, peers[n]], dst_ref=kall.at[c, me],
            send_sem=send_c.at[0], recv_sem=recv_c.at[c],
            device_id={"tp": peers[n]}, device_id_type=MESH).start()

    def cache_wait(c):
        pltpu.make_async_remote_copy(
            src_ref=snd.at[c, pl.ds(0, 3)], dst_ref=kall.at[c, pl.ds(0, 3)],
            send_sem=send_c.at[0], recv_sem=recv_c.at[c],
            device_id={"tp": partner}, device_id_type=MESH).wait_recv()

    def repack(c):
        spread[...] = raw[c].reshape(B * BLK * 8, 64).astype(F32)
        for p in range(NTP):
            lo = spread[pl.ds(2 * p, B * BLK, stride=8), :]
            hi = spread[pl.ds(2 * p + 1, B * BLK, stride=8), :]
            snd[c, p] = jnp.concatenate([lo, hi], axis=1).astype(BF16).reshape(B, BLK, 128)
        kall[c, me] = snd[c, me]

    for i in FIRST:
        small_copy(i).wait()
    raw_copy(0).start()
    for i in (2, 4, 9, 10):
        small_copy(i).start()
    raw_copy(2).start()
    raw_copy(3).start()
    w_copy(0, 0).start()

    eye = lax.broadcasted_iota(jnp.int32, (B, B), 0) == lax.broadcasted_iota(jnp.int32, (B, B), 1)
    len_row = jnp.broadcast_to(lens[...].astype(F32), (B, B))
    len_col = jnp.sum(jnp.where(eye, len_row, 0.0), axis=1, keepdims=True)
    len_b = jnp.broadcast_to(len_col, (B, 128))
    angle = len_b * inv[...]
    cosv, sinv = jnp.cos(angle), jnp.sin(angle)
    lane = lax.broadcasted_iota(jnp.int32, (B, 128), 1)
    low = (lane % 64) < 32
    left = lane < 64
    col = lax.broadcasted_iota(jnp.int32, (64, 1024), 1)
    row = lax.broadcasted_iota(jnp.int32, (64, 1024), 0)
    len64 = jnp.concatenate([len_col] * 4, axis=0)
    pos = ((col // 256) * BLK + col % BLK).astype(F32)
    valid = (((col // BLK) % B) == (row % B)) & (pos < len64)

    h_f = hid[...].astype(F32)

    def project(l, h_f):
        a = _norm(h_f, ga[pl.ds(l, 1), :].astype(F32))
        qf = jnp.dot(a, wq[l], preferred_element_type=F32)
        kf = jnp.dot(a, wk[l], preferred_element_type=F32)
        vf = jnp.dot(a, wv[l], preferred_element_type=F32)
        q = jnp.concatenate([_rope(qf[:, :128], cosv, sinv, low), _rope(qf[:, 128:], cosv, sinv, low)], axis=1).astype(BF16)
        return q, _rope(kf, cosv, sinv, low).astype(BF16).astype(F32), vf.astype(BF16).astype(F32)

    def head_rows(q):
        q0, q1 = q[:, :128].astype(F32), q[:, 128:].astype(F32)
        zero = jnp.zeros_like(q0)
        return jnp.concatenate([
            jnp.where(left, q0, zero), jnp.where(left, pltpu.roll(q0, 64, 1), zero),
            jnp.where(left, zero, pltpu.roll(q1, 64, 1)), jnp.where(left, zero, q1)], axis=0).astype(BF16)

    def swap(src, dst, send, recv, n):
        pltpu.make_async_remote_copy(src_ref=src, dst_ref=dst, send_sem=send.at[0], recv_sem=recv.at[0],
                                     device_id={"tp": peers[n]}, device_id_type=MESH).start()

    def swapped(ref, send, recv):
        return pltpu.make_async_remote_copy(src_ref=ref.at[pl.ds(0, 3)], dst_ref=ref.at[pl.ds(0, 3)], send_sem=send.at[0],
                                            recv_sem=recv.at[0], device_id={"tp": partner}, device_id_type=MESH)

    q, knew, vnew = project(0, h_f)
    qown[...] = q
    pl.semaphore_wait(barrier, 3)
    for n in range(3):
        swap(qown, qx.at[me], send_q, recv_q, n)
    qx[me] = q
    raw_copy(1).wait()
    repack(1)
    for n in range(3):
        cache_send(1, n)
    raw_copy(0).wait()
    repack(0)
    lane8 = lax.broadcasted_iota(jnp.int32, (8, 128), 1) // BLK
    colk = lax.broadcasted_iota(jnp.int32, (64, 256), 1)
    rowk = lax.broadcasted_iota(jnp.int32, (64, 256), 0)
    own_b = ((colk // BLK) % B) == (rowk % B)
    ecol = lax.broadcasted_iota(jnp.int32, (128, 1024), 1)
    erow = lax.broadcasted_iota(jnp.int32, (128, 1024), 0)
    emat[...] = jnp.where((ecol // 256) * BLK + ecol % BLK == erow, 1.0, 0.0).astype(BF16)
    for i in (2, 4, 9, 10):
        small_copy(i).wait()
    raw_copy(2).wait()
    raw_copy(3).wait()
    w_copy(0, 1).start()
    w_copy(0, 2).start()
    for i in (11, 12, 13):
        small_copy(i).start()
    swapped(qx, send_q, recv_q).wait_recv()
    for p in range(NTP):
        sk = lax.dot_general(head_rows(qx[p]), snd[0, p].reshape(B * BLK, 128), (((1,), (1,)), ((), ())), preferred_element_type=F32) * 0.125
        sk = jnp.where(own_b, sk, 0.0)
        sk = sk[:, :128] + sk[:, 128:]
        for shift in (64, 32, 16):
            sk = sk + pltpu.roll(sk, shift, 1)
        packed = sk[0:8]
        for k in range(1, 8):
            packed = jnp.where(lane8 == k, sk[8 * k:8 * k + 8], packed)
        sown[p] = packed
    for n in range(3):
        swap(sown.at[peers[n]], sx.at[me], send_s, recv_s, n)
    sx[me] = sown[me]
    repack(2)
    cache_send(2, 0)
    cache_send(2, 2)
    repack(3)
    cache_send(3, 2)
    cache_send(0, 2)

    def emit(c, new):
        new3 = jnp.broadcast_to(new[:, None, :], (B, BLK, 128))
        len3 = jnp.broadcast_to(len_b[:, None, :], (B, BLK, 128))
        pos3 = lax.broadcasted_iota(jnp.int32, (B, BLK, 128), 1).astype(F32)
        for s in range(NTP):
            x = jnp.where(pos3 + float(s * BLK) == len3, new3, kall[c, s].astype(F32)).reshape(B * BLK, 128)
            spread[pl.ds(0, B * BLK, stride=2), :] = x[:, :64]
            spread[pl.ds(1, B * BLK, stride=2), :] = x[:, 64:]
            outs[c][:, pl.ds(s * 2 * BLK, 2 * BLK), :] = spread[pl.ds(0, 2 * B * BLK), :].astype(BF16).reshape(B, 2 * BLK, 64)

    def x_send(step, piece, val):
        sl = pl.ds(*PIECES[step % 2][piece])
        xown[step, :, sl] = val
        for n in range(3):
            pltpu.make_async_remote_copy(
                src_ref=xown.at[step, :, sl], dst_ref=xrecv.at[step, me, :, sl],
                send_sem=send_x.at[0], recv_sem=recv_x.at[step],
                device_id={"tp": peers[n]}, device_id_type=MESH).start()
        xrecv[step, me, :, sl] = val

    def x_sum(step):
        pltpu.make_async_remote_copy(
            src_ref=xrecv.at[step, pl.ds(0, 3)], dst_ref=xrecv.at[step, pl.ds(0, 3)],
            send_sem=send_x.at[0], recv_sem=recv_x.at[step],
            device_id={"tp": partner}, device_id_type=MESH).wait_recv()
        tot = xrecv[step, 0].astype(F32)
        for s in range(1, NTP):
            tot = tot + xrecv[step, s].astype(F32)
        return tot

    outs = (ok1, ov1, ok2, ov2)

    for l in range(2):
        if l == 1:
            q, knew, vnew = project(l, h_f)
        qrows = head_rows(q)
        kc, vc = 2 * l, 2 * l + 1
        ns = jnp.sum(qrows.astype(F32) * jnp.concatenate([knew] * 4, axis=0), axis=1, keepdims=True) * 0.125
        if l == 0:
            swapped(sx, send_s, recv_s).wait_recv()
            rows = []
            for k in range(8):
                acc = jnp.zeros((8, 128), F32)
                for sd in range(NTP):
                    shift = (BLK * (sd - k)) % 128
                    part = sx[sd] if shift == 0 else pltpu.roll(sx[sd], shift, 1)
                    acc = jnp.where(lane8 == sd, part, acc)
                rows.append(acc)
            sc = jnp.concatenate(rows, axis=0)
            ok = lax.broadcasted_iota(jnp.int32, (64, 128), 1).astype(F32) < len64
        else:
            cache_wait(kc)
            k2d = kall[kc].reshape(NTP * B * BLK, 128)
            sc = lax.dot_general(qrows, k2d, (((1,), (1,)), ((), ())), preferred_element_type=F32) * 0.125
            ok = valid
        sc = jnp.where(ok, sc, -1e30)
        top = jnp.maximum(jnp.max(sc, axis=1, keepdims=True), ns)
        ex, nex = jnp.exp(sc - top), jnp.exp(ns - top)
        den = jnp.sum(ex, axis=1, keepdims=True) + nex
        prob = (ex / den).astype(BF16)
        nprob = (nex / den).astype(BF16).astype(F32)
        if l == 0:
            wide = jnp.dot(prob, emat[...], preferred_element_type=F32)
            prob = jnp.where(valid, wide, 0.0).astype(BF16)
        cache_wait(vc)
        v2d = kall[vc].reshape(NTP * B * BLK, 128)
        ov = jnp.dot(prob, v2d, preferred_element_type=F32) + nprob * jnp.concatenate([vnew] * 4, axis=0)
        attn = jnp.concatenate([jnp.where(left, ov[0:16], ov[48:64]), jnp.where(left, ov[16:32], ov[32:48])], axis=1).astype(BF16)
        wo_rows = jnp.concatenate([wo[l, pl.ds(0, 64), :], wo[l, pl.ds(192, 64), :], wo[l, pl.ds(64, 128), :]], axis=0)
        x_send(2 * l, 0, jnp.dot(attn, wo_rows, preferred_element_type=F32).astype(BF16))
        if l == 0:
            cache_send(2, 1)
            cache_send(3, 0)
            cache_send(3, 1)
        else:
            cache_send(0, 0)
            cache_send(0, 1)
            emit(kc, knew)
        emit(vc, vnew)
        for k in range(3):
            w_copy(l, k).wait()
        if l == 0:
            start_layer(1)
            for i in (11, 12, 13):
                small_copy(i).wait()
        h1 = (h_f + x_sum(2 * l)).astype(BF16).astype(F32)
        m = _norm(h1, gm[pl.ds(l, 1), :].astype(F32))

        lg = lax.dot_general(wr[l], m, (((1,), (1,)), ((), ())), preferred_element_type=F32)
        eid = lax.broadcasted_iota(jnp.int32, (EXP, B), 0)
        chosen = eid < 0
        for k in range(8):
            chosen = chosen | (cho[l, pl.ds(k, 1), :] == eid)
        lg = jnp.where(chosen, lg, -jnp.inf)
        ex = jnp.where(chosen, jnp.exp(lg - jnp.max(lg, axis=0, keepdims=True)), 0.0)
        gate_t = ex / jnp.sum(ex, axis=0, keepdims=True)
        gate = gate_t.T
        for e in range(EXP):
            w = jnp.concatenate([wg[l, e], wu[l, e]], axis=1)
            gu = jnp.dot(m, w, preferred_element_type=F32)
            g, u = gu[:, :FL], gu[:, FL:]
            act[:, pl.ds(e * FL, FL)] = (g * jax.nn.sigmoid(g) * u * jnp.broadcast_to(gate[:, e:e + 1], (B, FL))).astype(BF16)
        def down(piece, pairs, acc):
            first, width = PIECES[1][piece]
            for e in pairs:
                rhs = wd[l, pl.ds(e, 2), :, pl.ds(first, width)].reshape(2 * FL, width)
                acc = acc + jnp.dot(act[:, pl.ds(e * FL, 2 * FL)], rhs, preferred_element_type=F32)
            return acc

        acc0 = down(0, range(0, EXP, 2), jnp.zeros((B, PIECES[1][0][1]), F32))
        acc1 = down(1, range(0, 8, 2), jnp.zeros((B, PIECES[1][1][1]), F32))
        x_send(2 * l + 1, 0, acc0.astype(BF16))
        acc1 = down(1, range(8, EXP, 2), acc1)
        x_send(2 * l + 1, 1, acc1.astype(BF16))
        if l == 0:
            kone = knew
        else:
            cache_wait(0)
            emit(0, kone)
        h_f = (h1 + x_sum(2 * l + 1)).astype(BF16).astype(F32)

    hout[...] = h_f.astype(BF16)
    swapped(qx, send_q, recv_q).wait_send()
    swapped(sx, send_s, recv_s).wait_send()
    pltpu.make_async_remote_copy(
        src_ref=snd.at[:, pl.ds(0, 3)], dst_ref=kall.at[:, pl.ds(0, 3)], send_sem=send_c.at[0], recv_sem=recv_c.at[0],
        device_id={"tp": partner}, device_id_type=MESH).wait_send()
    pltpu.make_async_remote_copy(
        src_ref=xrecv.at[:, pl.ds(0, 3)], dst_ref=xrecv.at[:, pl.ds(0, 3)], send_sem=send_x.at[0], recv_sem=recv_x.at[0],
        device_id={"tp": partner}, device_id_type=MESH).wait_send()


def _store(h, k1, v1, k2, v2, ho, ok1, ov1, ok2, ov2, sem):
    copies = [pltpu.make_async_copy(a, b, sem.at[i])
              for i, (a, b) in enumerate(((k1, ok1), (v1, ov1), (k2, ok2), (v2, ov2), (h, ho)))]
    for c in copies:
        c.start()
    for c in copies:
        c.wait()


def solution(mesh):
    seq_spec = P('dp', 'tp', None, None)
    head_spec = P('dp', None, 'tp', None)
    col_spec = P(None, None, 'tp')
    ff_spec = P(None, None, None, 'tp')
    inv_freq = (THETA ** (-2.0 * np.arange(32, dtype=np.float64) / 64)).astype(np.float32)
    inv_row = np.tile(inv_freq, 4)[None, :]

    def local_step(hidden, lengths, choice, keys_one, vals_one, keys_two, vals_two, g_attn, w_q, w_k, w_v, w_o, g_mlp, w_router, w_gate, w_up, w_down):
        shapes = (jax.ShapeDtypeStruct((B, D), BF16),) + (jax.ShapeDtypeStruct((B, 2 * SEQ, 64), BF16),) * 4
        any_spec = pl.BlockSpec(memory_space=pl.ANY)
        vmem_spec = pl.BlockSpec(memory_space=pltpu.VMEM)
        V = pltpu.VMEM
        DMA = pltpu.SemaphoreType.DMA
        outs = pl.pallas_call(
            _kernel,
            out_shape=tuple(V(s.shape, s.dtype) for s in shapes),
            in_specs=[any_spec] * 18,
            out_specs=(vmem_spec,) * 5,
            scratch_shapes=[
                V((B, D), BF16), V((1, B), jnp.int32), V((2, 8, B), jnp.int32), V((4, B, BLK, 8, 64), BF16),
                V((2, D), BF16), V((2, D, 256), BF16), V((2, D, 128), BF16), V((2, D, 128), BF16), V((2, 256, D), BF16),
                V((2, D), BF16), V((2, EXP, D), BF16), V((2, EXP, D, FL), BF16), V((2, EXP, D, FL), BF16), V((2, EXP, FL, D), BF16),
                V((1, 128), F32),
                V((B * BLK * 8, 64), F32), V((4, NTP, B, BLK, 128), BF16), V((4, NTP, B, BLK, 128), BF16),
                V((4, B, D), BF16), V((4, NTP, B, D), BF16), V((B, EXP * FL), BF16), V((B, 256), BF16), V((NTP, B, 256), BF16), V((NTP, 8, 128), F32), V((NTP, 8, 128), F32), V((128, 1024), BF16),
                DMA((14,)), DMA((4,)), DMA((2, 3)), DMA((1,)), DMA((4,)), DMA((1,)), DMA((4,)), DMA((1,)), DMA((1,)), DMA((1,)), DMA((1,)),
            ],
            compiler_params=pltpu.CompilerParams(collective_id=0, has_side_effects=True, vmem_limit_bytes=64_000_000),
        )(hidden, lengths.reshape(1, B), jnp.transpose(choice, (0, 2, 1)), keys_one, vals_one, keys_two, vals_two,
          g_attn, w_q, w_k, w_v, w_o, g_mlp, jnp.transpose(w_router, (0, 2, 1)), w_gate, w_up, w_down, jnp.asarray(inv_row))
        outs = pl.pallas_call(
            _store,
            out_shape=shapes,
            in_specs=[vmem_spec] * 5,
            out_specs=(any_spec,) * 5,
            scratch_shapes=[DMA((5,))],
        )(*[pltpu.with_memory_space_constraint(o, pltpu.VMEM) for o in outs])
        return (outs[0],) + tuple(o.reshape(B, SEQ, 2, 64) for o in outs[1:])

    return jax.shard_map(local_step, mesh=mesh, in_specs=(P('dp', None), P('dp'), P(None, 'dp', None), seq_spec, seq_spec, seq_spec, seq_spec, P(), col_spec, col_spec, col_spec, P(None, 'tp', None), P(), P(), ff_spec, ff_spec, P(None, None, 'tp', None)), out_specs=(P('dp', None), head_spec, head_spec, head_spec, head_spec), check_vma=False)
```

```python
import functools

import numpy as np

import jax
import jax.numpy as jnp
from jax import lax
from jax.experimental import pallas as pl
from jax.experimental.pallas import tpu as pltpu
from jax.sharding import PartitionSpec as P

EPS = 1e-5
THETA = 1000000.0
MESH = pl.DeviceIdType.MESH
B = 16
D = 1024
SEQ = 64
BLK = 16
NTP = 4
EXP = 32
FL = 128
PIECES = (((0, 1024),), ((0, 512), (512, 512)))
NP = 2
F32 = jnp.float32
BF16 = jnp.bfloat16


def _norm(h_f, gain_row):
    scale = lax.rsqrt(jnp.mean(h_f * h_f, axis=-1, keepdims=True) + EPS)
    return (h_f * scale * gain_row).astype(BF16)


def _rope(x, cosv, sinv, low):
    rot = jnp.where(low, -pltpu.roll(x, 96, 1), pltpu.roll(x, 32, 1))
    return x * cosv + rot * sinv


def _kernel(hid_h, len_h, cho_h, k1_h, v1_h, k2_h, v2_h, ga_h, wq_h, wk_h, wv_h, wo_h, gm_h, wr_h, wg_h, wu_h, wd_h, inv_h,
            hout, ok1, ov1, ok2, ov2,
            hid, lens, cho, raw, ga, wq, wk, wv, wo, gm, wr, wg, wu, wd, inv,
            spread, snd, kall, xown, xrecv, act,
            sem_s, sem_raw, sem_w, send_c, recv_c, send_x, recv_x):
    me = lax.axis_index("tp")
    chip, core = me // 2, me % 2
    partner = chip * 2 + (1 - core)
    cross_a = (1 - chip) * 2 + core
    cross_b = (1 - chip) * 2 + (1 - core)
    peers = (cross_a, cross_b, partner)

    barrier = pltpu.get_barrier_semaphore()
    for p in peers:
        pl.semaphore_signal(barrier, inc=1, device_id={"tp": p}, device_id_type=MESH)

    raw_src = (k1_h, v1_h, k2_h, v2_h)

    def raw_copy(c):
        return pltpu.make_async_copy(raw_src[c], raw.at[c], sem_raw.at[c])

    smalls = ((hid_h, hid), (len_h, lens), (cho_h, cho), (ga_h, ga), (gm_h, gm), (inv_h, inv),
              (wq_h, wq), (wk_h, wk), (wv_h, wv), (wo_h, wo), (wr_h, wr))

    def small_copy(i):
        return pltpu.make_async_copy(smalls[i][0], smalls[i][1], sem_s.at[i])

    def w_copy(l, k):
        src, dst = ((wg_h, wg), (wu_h, wu), (wd_h, wd))[k]
        return pltpu.make_async_copy(src.at[l], dst.at[l], sem_w.at[l, k])

    raw_copy(0).start()
    raw_copy(1).start()

    def cache_send(c, n):
        pltpu.make_async_remote_copy(
            src_ref=snd.at[c, peers[n]], dst_ref=kall.at[c, me],
            send_sem=send_c.at[0], recv_sem=recv_c.at[c],
            device_id={"tp": peers[n]}, device_id_type=MESH).start()

    def cache_wait(c):
        pltpu.make_async_remote_copy(
            src_ref=snd.at[c, pl.ds(0, 3)], dst_ref=kall.at[c, pl.ds(0, 3)],
            send_sem=send_c.at[0], recv_sem=recv_c.at[c],
            device_id={"tp": partner}, device_id_type=MESH).wait_recv()

    def repack(c):
        spread[...] = raw[c].reshape(B * BLK * 8, 64).astype(F32)
        for p in range(NTP):
            lo = spread[pl.ds(2 * p, B * BLK, stride=8), :]
            hi = spread[pl.ds(2 * p + 1, B * BLK, stride=8), :]
            snd[c, p] = jnp.concatenate([lo, hi], axis=1).astype(BF16).reshape(B, BLK, 128)
        kall[c, me] = snd[c, me]

    raw_copy(0).wait()
    for i in range(len(smalls)):
        small_copy(i).start()
    repack(0)
    pl.semaphore_wait(barrier, 3)
    for n in range(3):
        cache_send(0, n)
    raw_copy(1).wait()
    raw_copy(2).start()
    raw_copy(3).start()
    repack(1)
    for n in range(3):
        cache_send(1, n)
    for i in range(len(smalls)):
        small_copy(i).wait()
    raw_copy(2).wait()
    raw_copy(3).wait()
    w_copy(0, 0).start()
    w_copy(0, 1).start()
    repack(2)
    cache_send(2, 0)
    cache_send(2, 2)
    repack(3)
    cache_send(3, 2)


    eye = lax.broadcasted_iota(jnp.int32, (B, B), 0) == lax.broadcasted_iota(jnp.int32, (B, B), 1)
    len_row = jnp.broadcast_to(lens[...].astype(F32), (B, B))
    len_col = jnp.sum(jnp.where(eye, len_row, 0.0), axis=1, keepdims=True)
    len_b = jnp.broadcast_to(len_col, (B, 128))
    angle = len_b * inv[...]
    cosv, sinv = jnp.cos(angle), jnp.sin(angle)
    lane = lax.broadcasted_iota(jnp.int32, (B, 128), 1)
    low = (lane % 64) < 32
    left = lane < 64
    col = lax.broadcasted_iota(jnp.int32, (64, 1024), 1)
    row = lax.broadcasted_iota(jnp.int32, (64, 1024), 0)
    len64 = jnp.concatenate([len_col] * 4, axis=0)
    pos = ((col // 256) * BLK + col % BLK).astype(F32)
    valid = (((col // BLK) % B) == (row % B)) & (pos < len64)

    h_f = hid[...].astype(F32)

    def emit(c, new):
        new3 = jnp.broadcast_to(new[:, None, :], (B, BLK, 128))
        len3 = jnp.broadcast_to(len_b[:, None, :], (B, BLK, 128))
        pos3 = lax.broadcasted_iota(jnp.int32, (B, BLK, 128), 1).astype(F32)
        for s in range(NTP):
            x = jnp.where(pos3 + float(s * BLK) == len3, new3, kall[c, s].astype(F32)).reshape(B * BLK, 128)
            spread[pl.ds(0, B * BLK, stride=2), :] = x[:, :64]
            spread[pl.ds(1, B * BLK, stride=2), :] = x[:, 64:]
            outs[c][:, pl.ds(s * 2 * BLK, 2 * BLK), :] = spread[pl.ds(0, 2 * B * BLK), :].astype(BF16).reshape(B, 2 * BLK, 64)

    def x_send(step, piece, val):
        sl = pl.ds(*PIECES[step % 2][piece])
        xown[step, :, sl] = val
        for n in range(3):
            pltpu.make_async_remote_copy(
                src_ref=xown.at[step, :, sl], dst_ref=xrecv.at[step, me, :, sl],
                send_sem=send_x.at[0], recv_sem=recv_x.at[step],
                device_id={"tp": peers[n]}, device_id_type=MESH).start()
        xrecv[step, me, :, sl] = val

    def x_sum(step):
        pltpu.make_async_remote_copy(
            src_ref=xrecv.at[step, pl.ds(0, 3)], dst_ref=xrecv.at[step, pl.ds(0, 3)],
            send_sem=send_x.at[0], recv_sem=recv_x.at[step],
            device_id={"tp": partner}, device_id_type=MESH).wait_recv()
        tot = xrecv[step, 0].astype(F32)
        for s in range(1, NTP):
            tot = tot + xrecv[step, s].astype(F32)
        return tot

    outs = (ok1, ov1, ok2, ov2)

    for l in range(2):
        a = _norm(h_f, ga[pl.ds(l, 1), :].astype(F32))
        qf = jnp.dot(a, wq[l], preferred_element_type=F32)
        kf = jnp.dot(a, wk[l], preferred_element_type=F32)
        vf = jnp.dot(a, wv[l], preferred_element_type=F32)
        q0 = _rope(qf[:, :128], cosv, sinv, low)
        q1 = _rope(qf[:, 128:], cosv, sinv, low)
        knew = _rope(kf, cosv, sinv, low).astype(BF16).astype(F32)
        vnew = vf.astype(BF16).astype(F32)
        zero = jnp.zeros_like(q0)
        qrows = jnp.concatenate([
            jnp.where(left, q0, zero), jnp.where(left, pltpu.roll(q0, 64, 1), zero),
            jnp.where(left, zero, pltpu.roll(q1, 64, 1)), jnp.where(left, zero, q1)], axis=0).astype(BF16)
        kc, vc = 2 * l, 2 * l + 1
        if l == 0:
            w_copy(0, 0).wait()
            w_copy(0, 1).wait()
            w_copy(0, 2).start()
        cache_wait(kc)
        k2d = kall[kc].reshape(NTP * B * BLK, 128)
        sc = lax.dot_general(qrows, k2d, (((1,), (1,)), ((), ())), preferred_element_type=F32) * 0.125
        sc = jnp.where(valid, sc, -1e30)
        ns = jnp.sum(qrows.astype(F32) * jnp.concatenate([knew] * 4, axis=0), axis=1, keepdims=True) * 0.125
        top = jnp.maximum(jnp.max(sc, axis=1, keepdims=True), ns)
        ex, nex = jnp.exp(sc - top), jnp.exp(ns - top)
        den = jnp.sum(ex, axis=1, keepdims=True) + nex
        prob = (ex / den).astype(BF16)
        nprob = (nex / den).astype(BF16).astype(F32)
        cache_wait(vc)
        v2d = kall[vc].reshape(NTP * B * BLK, 128)
        ov = jnp.dot(prob, v2d, preferred_element_type=F32) + nprob * jnp.concatenate([vnew] * 4, axis=0)
        attn = jnp.concatenate([jnp.where(left, ov[0:16], ov[48:64]), jnp.where(left, ov[16:32], ov[32:48])], axis=1).astype(BF16)
        wo_rows = jnp.concatenate([wo[l, pl.ds(0, 64), :], wo[l, pl.ds(192, 64), :], wo[l, pl.ds(64, 128), :]], axis=0)
        x_send(2 * l, 0, jnp.dot(attn, wo_rows, preferred_element_type=F32).astype(BF16))
        if l == 0:
            w_copy(1, 0).start()
            cache_send(2, 1)
            cache_send(3, 0)
            cache_send(3, 1)
        emit(kc, knew)
        emit(vc, vnew)
        if l == 0:
            w_copy(0, 2).wait()
            w_copy(1, 1).start()
            w_copy(1, 2).start()
        else:
            for k in range(3):
                w_copy(1, k).wait()
        h1 = (h_f + x_sum(2 * l)).astype(BF16).astype(F32)
        m = _norm(h1, gm[pl.ds(l, 1), :].astype(F32))

        lg = lax.dot_general(wr[l], m, (((1,), (1,)), ((), ())), preferred_element_type=F32)
        eid = lax.broadcasted_iota(jnp.int32, (EXP, B), 0)
        chosen = eid < 0
        for k in range(8):
            chosen = chosen | (cho[l, pl.ds(k, 1), :] == eid)
        lg = jnp.where(chosen, lg, -jnp.inf)
        ex = jnp.where(chosen, jnp.exp(lg - jnp.max(lg, axis=0, keepdims=True)), 0.0)
        gate_t = ex / jnp.sum(ex, axis=0, keepdims=True)
        gate = gate_t.T
        for e in range(EXP):
            w = jnp.concatenate([wg[l, e], wu[l, e]], axis=1)
            gu = jnp.dot(m, w, preferred_element_type=F32)
            g, u = gu[:, :FL], gu[:, FL:]
            act[:, pl.ds(e * FL, FL)] = (g * jax.nn.sigmoid(g) * u * jnp.broadcast_to(gate[:, e:e + 1], (B, FL))).astype(BF16)
        def down(piece, pairs, acc):
            first, width = PIECES[1][piece]
            for e in pairs:
                rhs = wd[l, pl.ds(e, 2), :, pl.ds(first, width)].reshape(2 * FL, width)
                acc = acc + jnp.dot(act[:, pl.ds(e * FL, 2 * FL)], rhs, preferred_element_type=F32)
            return acc

        acc0 = down(0, range(0, EXP, 2), jnp.zeros((B, PIECES[1][0][1]), F32))
        acc1 = down(1, range(0, 8, 2), jnp.zeros((B, PIECES[1][1][1]), F32))
        x_send(2 * l + 1, 0, acc0.astype(BF16))
        acc1 = down(1, range(8, EXP, 2), acc1)
        x_send(2 * l + 1, 1, acc1.astype(BF16))
        h_f = (h1 + x_sum(2 * l + 1)).astype(BF16).astype(F32)

    hout[...] = h_f.astype(BF16)
    pltpu.make_async_remote_copy(
        src_ref=snd.at[:, pl.ds(0, 3)], dst_ref=kall.at[:, pl.ds(0, 3)], send_sem=send_c.at[0], recv_sem=recv_c.at[0],
        device_id={"tp": partner}, device_id_type=MESH).wait_send()
    pltpu.make_async_remote_copy(
        src_ref=xrecv.at[:, pl.ds(0, 3)], dst_ref=xrecv.at[:, pl.ds(0, 3)], send_sem=send_x.at[0], recv_sem=recv_x.at[0],
        device_id={"tp": partner}, device_id_type=MESH).wait_send()


def _store(h, k1, v1, k2, v2, ho, ok1, ov1, ok2, ov2, sem):
    copies = [pltpu.make_async_copy(a, b, sem.at[i])
              for i, (a, b) in enumerate(((k1, ok1), (v1, ov1), (k2, ok2), (v2, ov2), (h, ho)))]
    for c in copies:
        c.start()
    for c in copies:
        c.wait()


def solution(mesh):
    seq_spec = P('dp', 'tp', None, None)
    head_spec = P('dp', None, 'tp', None)
    col_spec = P(None, None, 'tp')
    ff_spec = P(None, None, None, 'tp')
    inv_freq = (THETA ** (-2.0 * np.arange(32, dtype=np.float64) / 64)).astype(np.float32)
    inv_row = np.tile(inv_freq, 4)[None, :]

    def local_step(hidden, lengths, choice, keys_one, vals_one, keys_two, vals_two, g_attn, w_q, w_k, w_v, w_o, g_mlp, w_router, w_gate, w_up, w_down):
        shapes = (jax.ShapeDtypeStruct((B, D), BF16),) + (jax.ShapeDtypeStruct((B, 2 * SEQ, 64), BF16),) * 4
        any_spec = pl.BlockSpec(memory_space=pl.ANY)
        vmem_spec = pl.BlockSpec(memory_space=pltpu.VMEM)
        V = pltpu.VMEM
        DMA = pltpu.SemaphoreType.DMA
        outs = pl.pallas_call(
            _kernel,
            out_shape=tuple(V(s.shape, s.dtype) for s in shapes),
            in_specs=[any_spec] * 18,
            out_specs=(vmem_spec,) * 5,
            scratch_shapes=[
                V((B, D), BF16), V((1, B), jnp.int32), V((2, 8, B), jnp.int32), V((4, B, BLK, 8, 64), BF16),
                V((2, D), BF16), V((2, D, 256), BF16), V((2, D, 128), BF16), V((2, D, 128), BF16), V((2, 256, D), BF16),
                V((2, D), BF16), V((2, EXP, D), BF16), V((2, EXP, D, FL), BF16), V((2, EXP, D, FL), BF16), V((2, EXP, FL, D), BF16),
                V((1, 128), F32),
                V((B * BLK * 8, 64), F32), V((4, NTP, B, BLK, 128), BF16), V((4, NTP, B, BLK, 128), BF16),
                V((4, B, D), BF16), V((4, NTP, B, D), BF16), V((B, EXP * FL), BF16),
                DMA((11,)), DMA((4,)), DMA((2, 3)), DMA((1,)), DMA((4,)), DMA((1,)), DMA((4,)),
            ],
            compiler_params=pltpu.CompilerParams(collective_id=0, has_side_effects=True, vmem_limit_bytes=64_000_000),
        )(hidden, lengths.reshape(1, B), jnp.transpose(choice, (0, 2, 1)), keys_one, vals_one, keys_two, vals_two,
          g_attn, w_q, w_k, w_v, w_o, g_mlp, jnp.transpose(w_router, (0, 2, 1)), w_gate, w_up, w_down, jnp.asarray(inv_row))
        outs = pl.pallas_call(
            _store,
            out_shape=shapes,
            in_specs=[vmem_spec] * 5,
            out_specs=(any_spec,) * 5,
            scratch_shapes=[DMA((5,))],
        )(*[pltpu.with_memory_space_constraint(o, pltpu.VMEM) for o in outs])
        return (outs[0],) + tuple(o.reshape(B, SEQ, 2, 64) for o in outs[1:])

    return jax.shard_map(local_step, mesh=mesh, in_specs=(P('dp', None), P('dp'), P(None, 'dp', None), seq_spec, seq_spec, seq_spec, seq_spec, P(), col_spec, col_spec, col_spec, P(None, 'tp', None), P(), P(), ff_spec, ff_spec, P(None, None, 'tp', None)), out_specs=(P('dp', None), head_spec, head_spec, head_spec, head_spec), check_vma=False)
```

```python
import functools

import numpy as np

import jax
import jax.numpy as jnp
from jax import lax
from jax.experimental import pallas as pl
from jax.experimental.pallas import tpu as pltpu
from jax.sharding import PartitionSpec as P

EPS = 1e-5
THETA = 1000000.0
MESH = pl.DeviceIdType.MESH
B = 16
D = 1024
SEQ = 64
BLK = 16
NTP = 4
EXP = 32
FL = 128
PIECES = (((0, 1024),), ((0, 512), (512, 512)))
NP = 2
F32 = jnp.float32
BF16 = jnp.bfloat16


def _norm(h_f, gain_row):
    scale = lax.rsqrt(jnp.mean(h_f * h_f, axis=-1, keepdims=True) + EPS)
    return (h_f * scale * gain_row).astype(BF16)


def _rope(x, cosv, sinv, low):
    rot = jnp.where(low, -pltpu.roll(x, 96, 1), pltpu.roll(x, 32, 1))
    return x * cosv + rot * sinv


def _kernel(hid_h, len_h, cho_h, k1_h, v1_h, k2_h, v2_h, ga_h, wq_h, wk_h, wv_h, wo_h, gm_h, wr_h, wg_h, wu_h, wd_h, inv_h,
            hout, ok1, ov1, ok2, ov2,
            hid, lens, cho, raw, ga, wq, wk, wv, wo, gm, wr, wg, wu, wd, inv,
            spread, snd, kall, xown, xrecv, act, qown, qx, sown, sx, emat,
            sem_s, sem_raw, sem_w, send_c, recv_c, send_x, recv_x, send_q, recv_q, send_s, recv_s):
    me = lax.axis_index("tp")
    chip, core = me // 2, me % 2
    partner = chip * 2 + (1 - core)
    cross_a = (1 - chip) * 2 + core
    cross_b = (1 - chip) * 2 + (1 - core)
    peers = (cross_a, cross_b, partner)

    barrier = pltpu.get_barrier_semaphore()
    for p in peers:
        pl.semaphore_signal(barrier, inc=1, device_id={"tp": p}, device_id_type=MESH)

    raw_src = (k1_h, v1_h, k2_h, v2_h)

    def raw_copy(c):
        return pltpu.make_async_copy(raw_src[c], raw.at[c], sem_raw.at[c])

    smalls = ((hid_h, hid), (len_h, lens), (cho_h, cho), (ga_h, ga), (gm_h, gm), (inv_h, inv),
              (wq_h, wq), (wk_h, wk), (wv_h, wv), (wo_h, wo), (wr_h, wr))

    def small_copy(i):
        return pltpu.make_async_copy(smalls[i][0], smalls[i][1], sem_s.at[i])

    def w_copy(l, k):
        src, dst = ((wg_h, wg), (wu_h, wu), (wd_h, wd))[k]
        return pltpu.make_async_copy(src.at[l], dst.at[l], sem_w.at[l, k])

    FIRST = (0, 1, 3, 5, 6, 7, 8)
    for i in FIRST:
        small_copy(i).start()
    raw_copy(1).start()
    raw_copy(0).start()

    def start_layer(l):
        for k in range(3):
            w_copy(l, k).start()

    def cache_send(c, n):
        pltpu.make_async_remote_copy(
            src_ref=snd.at[c, peers[n]], dst_ref=kall.at[c, me],
            send_sem=send_c.at[0], recv_sem=recv_c.at[c],
            device_id={"tp": peers[n]}, device_id_type=MESH).start()

    def cache_wait(c):
        pltpu.make_async_remote_copy(
            src_ref=snd.at[c, pl.ds(0, 3)], dst_ref=kall.at[c, pl.ds(0, 3)],
            send_sem=send_c.at[0], recv_sem=recv_c.at[c],
            device_id={"tp": partner}, device_id_type=MESH).wait_recv()

    def repack(c):
        spread[...] = raw[c].reshape(B * BLK * 8, 64).astype(F32)
        for p in range(NTP):
            lo = spread[pl.ds(2 * p, B * BLK, stride=8), :]
            hi = spread[pl.ds(2 * p + 1, B * BLK, stride=8), :]
            snd[c, p] = jnp.concatenate([lo, hi], axis=1).astype(BF16).reshape(B, BLK, 128)
        kall[c, me] = snd[c, me]

    for i in FIRST:
        small_copy(i).wait()

    eye = lax.broadcasted_iota(jnp.int32, (B, B), 0) == lax.broadcasted_iota(jnp.int32, (B, B), 1)
    len_row = jnp.broadcast_to(lens[...].astype(F32), (B, B))
    len_col = jnp.sum(jnp.where(eye, len_row, 0.0), axis=1, keepdims=True)
    len_b = jnp.broadcast_to(len_col, (B, 128))
    angle = len_b * inv[...]
    cosv, sinv = jnp.cos(angle), jnp.sin(angle)
    lane = lax.broadcasted_iota(jnp.int32, (B, 128), 1)
    low = (lane % 64) < 32
    left = lane < 64
    col = lax.broadcasted_iota(jnp.int32, (64, 1024), 1)
    row = lax.broadcasted_iota(jnp.int32, (64, 1024), 0)
    len64 = jnp.concatenate([len_col] * 4, axis=0)
    pos = ((col // 256) * BLK + col % BLK).astype(F32)
    valid = (((col // BLK) % B) == (row % B)) & (pos < len64)

    h_f = hid[...].astype(F32)

    def project(l, h_f):
        a = _norm(h_f, ga[pl.ds(l, 1), :].astype(F32))
        qf = jnp.dot(a, wq[l], preferred_element_type=F32)
        kf = jnp.dot(a, wk[l], preferred_element_type=F32)
        vf = jnp.dot(a, wv[l], preferred_element_type=F32)
        q = jnp.concatenate([_rope(qf[:, :128], cosv, sinv, low), _rope(qf[:, 128:], cosv, sinv, low)], axis=1).astype(BF16)
        return q, _rope(kf, cosv, sinv, low).astype(BF16).astype(F32), vf.astype(BF16).astype(F32)

    def head_rows(q):
        q0, q1 = q[:, :128].astype(F32), q[:, 128:].astype(F32)
        zero = jnp.zeros_like(q0)
        return jnp.concatenate([
            jnp.where(left, q0, zero), jnp.where(left, pltpu.roll(q0, 64, 1), zero),
            jnp.where(left, zero, pltpu.roll(q1, 64, 1)), jnp.where(left, zero, q1)], axis=0).astype(BF16)

    def swap(src, dst, send, recv, n):
        pltpu.make_async_remote_copy(src_ref=src, dst_ref=dst, send_sem=send.at[0], recv_sem=recv.at[0],
                                     device_id={"tp": peers[n]}, device_id_type=MESH).start()

    def swapped(ref, send, recv):
        return pltpu.make_async_remote_copy(src_ref=ref.at[pl.ds(0, 3)], dst_ref=ref.at[pl.ds(0, 3)], send_sem=send.at[0],
                                            recv_sem=recv.at[0], device_id={"tp": partner}, device_id_type=MESH)

    q, knew, vnew = project(0, h_f)
    qown[...] = q
    pl.semaphore_wait(barrier, 3)
    for n in range(3):
        swap(qown, qx.at[me], send_q, recv_q, n)
    qx[me] = q
    raw_copy(1).wait()
    repack(1)
    for n in range(3):
        cache_send(1, n)
    raw_copy(0).wait()
    for i in range(len(smalls)):
        if i not in FIRST:
            small_copy(i).start()
    raw_copy(2).start()
    raw_copy(3).start()
    repack(0)
    lane8 = lax.broadcasted_iota(jnp.int32, (8, 128), 1) // BLK
    colk = lax.broadcasted_iota(jnp.int32, (64, 256), 1)
    rowk = lax.broadcasted_iota(jnp.int32, (64, 256), 0)
    own_b = ((colk // BLK) % B) == (rowk % B)
    ecol = lax.broadcasted_iota(jnp.int32, (128, 1024), 1)
    erow = lax.broadcasted_iota(jnp.int32, (128, 1024), 0)
    emat[...] = jnp.where((ecol // 256) * BLK + ecol % BLK == erow, 1.0, 0.0).astype(BF16)
    for i in range(len(smalls)):
        if i not in FIRST:
            small_copy(i).wait()
    raw_copy(2).wait()
    raw_copy(3).wait()
    start_layer(0)
    swapped(qx, send_q, recv_q).wait_recv()
    for p in range(NTP):
        sk = lax.dot_general(head_rows(qx[p]), snd[0, p].reshape(B * BLK, 128), (((1,), (1,)), ((), ())), preferred_element_type=F32) * 0.125
        sk = jnp.where(own_b, sk, 0.0)
        sk = sk[:, :128] + sk[:, 128:]
        for shift in (64, 32, 16):
            sk = sk + pltpu.roll(sk, shift, 1)
        packed = sk[0:8]
        for k in range(1, 8):
            packed = jnp.where(lane8 == k, sk[8 * k:8 * k + 8], packed)
        sown[p] = packed
    for n in range(3):
        swap(sown.at[peers[n]], sx.at[me], send_s, recv_s, n)
    sx[me] = sown[me]
    repack(2)
    cache_send(2, 0)
    cache_send(2, 2)
    repack(3)
    cache_send(3, 2)
    cache_send(0, 2)

    def emit(c, new):
        new3 = jnp.broadcast_to(new[:, None, :], (B, BLK, 128))
        len3 = jnp.broadcast_to(len_b[:, None, :], (B, BLK, 128))
        pos3 = lax.broadcasted_iota(jnp.int32, (B, BLK, 128), 1).astype(F32)
        for s in range(NTP):
            x = jnp.where(pos3 + float(s * BLK) == len3, new3, kall[c, s].astype(F32)).reshape(B * BLK, 128)
            spread[pl.ds(0, B * BLK, stride=2), :] = x[:, :64]
            spread[pl.ds(1, B * BLK, stride=2), :] = x[:, 64:]
            outs[c][:, pl.ds(s * 2 * BLK, 2 * BLK), :] = spread[pl.ds(0, 2 * B * BLK), :].astype(BF16).reshape(B, 2 * BLK, 64)

    def x_send(step, piece, val):
        sl = pl.ds(*PIECES[step % 2][piece])
        xown[step, :, sl] = val
        for n in range(3):
            pltpu.make_async_remote_copy(
                src_ref=xown.at[step, :, sl], dst_ref=xrecv.at[step, me, :, sl],
                send_sem=send_x.at[0], recv_sem=recv_x.at[step],
                device_id={"tp": peers[n]}, device_id_type=MESH).start()
        xrecv[step, me, :, sl] = val

    def x_sum(step):
        pltpu.make_async_remote_copy(
            src_ref=xrecv.at[step, pl.ds(0, 3)], dst_ref=xrecv.at[step, pl.ds(0, 3)],
            send_sem=send_x.at[0], recv_sem=recv_x.at[step],
            device_id={"tp": partner}, device_id_type=MESH).wait_recv()
        tot = xrecv[step, 0].astype(F32)
        for s in range(1, NTP):
            tot = tot + xrecv[step, s].astype(F32)
        return tot

    outs = (ok1, ov1, ok2, ov2)

    for l in range(2):
        if l == 1:
            q, knew, vnew = project(l, h_f)
        qrows = head_rows(q)
        kc, vc = 2 * l, 2 * l + 1
        ns = jnp.sum(qrows.astype(F32) * jnp.concatenate([knew] * 4, axis=0), axis=1, keepdims=True) * 0.125
        if l == 0:
            swapped(sx, send_s, recv_s).wait_recv()
            rows = []
            for k in range(8):
                acc = jnp.zeros((8, 128), F32)
                for sd in range(NTP):
                    shift = (BLK * (sd - k)) % 128
                    part = sx[sd] if shift == 0 else pltpu.roll(sx[sd], shift, 1)
                    acc = jnp.where(lane8 == sd, part, acc)
                rows.append(acc)
            sc = jnp.concatenate(rows, axis=0)
            ok = lax.broadcasted_iota(jnp.int32, (64, 128), 1).astype(F32) < len64
        else:
            cache_wait(kc)
            k2d = kall[kc].reshape(NTP * B * BLK, 128)
            sc = lax.dot_general(qrows, k2d, (((1,), (1,)), ((), ())), preferred_element_type=F32) * 0.125
            ok = valid
        sc = jnp.where(ok, sc, -1e30)
        top = jnp.maximum(jnp.max(sc, axis=1, keepdims=True), ns)
        ex, nex = jnp.exp(sc - top), jnp.exp(ns - top)
        den = jnp.sum(ex, axis=1, keepdims=True) + nex
        prob = (ex / den).astype(BF16)
        nprob = (nex / den).astype(BF16).astype(F32)
        if l == 0:
            wide = jnp.dot(prob, emat[...], preferred_element_type=F32)
            prob = jnp.where(valid, wide, 0.0).astype(BF16)
        cache_wait(vc)
        v2d = kall[vc].reshape(NTP * B * BLK, 128)
        ov = jnp.dot(prob, v2d, preferred_element_type=F32) + nprob * jnp.concatenate([vnew] * 4, axis=0)
        attn = jnp.concatenate([jnp.where(left, ov[0:16], ov[48:64]), jnp.where(left, ov[16:32], ov[32:48])], axis=1).astype(BF16)
        wo_rows = jnp.concatenate([wo[l, pl.ds(0, 64), :], wo[l, pl.ds(192, 64), :], wo[l, pl.ds(64, 128), :]], axis=0)
        x_send(2 * l, 0, jnp.dot(attn, wo_rows, preferred_element_type=F32).astype(BF16))
        if l == 0:
            cache_send(2, 1)
            cache_send(3, 0)
            cache_send(3, 1)
        else:
            cache_send(0, 0)
            cache_send(0, 1)
            emit(kc, knew)
        emit(vc, vnew)
        for k in range(3):
            w_copy(l, k).wait()
        if l == 0:
            start_layer(1)
        h1 = (h_f + x_sum(2 * l)).astype(BF16).astype(F32)
        m = _norm(h1, gm[pl.ds(l, 1), :].astype(F32))

        lg = lax.dot_general(wr[l], m, (((1,), (1,)), ((), ())), preferred_element_type=F32)
        eid = lax.broadcasted_iota(jnp.int32, (EXP, B), 0)
        chosen = eid < 0
        for k in range(8):
            chosen = chosen | (cho[l, pl.ds(k, 1), :] == eid)
        lg = jnp.where(chosen, lg, -jnp.inf)
        ex = jnp.where(chosen, jnp.exp(lg - jnp.max(lg, axis=0, keepdims=True)), 0.0)
        gate_t = ex / jnp.sum(ex, axis=0, keepdims=True)
        gate = gate_t.T
        for e in range(EXP):
            w = jnp.concatenate([wg[l, e], wu[l, e]], axis=1)
            gu = jnp.dot(m, w, preferred_element_type=F32)
            g, u = gu[:, :FL], gu[:, FL:]
            act[:, pl.ds(e * FL, FL)] = (g * jax.nn.sigmoid(g) * u * jnp.broadcast_to(gate[:, e:e + 1], (B, FL))).astype(BF16)
        def down(piece, pairs, acc):
            first, width = PIECES[1][piece]
            for e in pairs:
                rhs = wd[l, pl.ds(e, 2), :, pl.ds(first, width)].reshape(2 * FL, width)
                acc = acc + jnp.dot(act[:, pl.ds(e * FL, 2 * FL)], rhs, preferred_element_type=F32)
            return acc

        acc0 = down(0, range(0, EXP, 2), jnp.zeros((B, PIECES[1][0][1]), F32))
        acc1 = down(1, range(0, 8, 2), jnp.zeros((B, PIECES[1][1][1]), F32))
        x_send(2 * l + 1, 0, acc0.astype(BF16))
        acc1 = down(1, range(8, EXP, 2), acc1)
        x_send(2 * l + 1, 1, acc1.astype(BF16))
        if l == 0:
            kone = knew
        else:
            cache_wait(0)
            emit(0, kone)
        h_f = (h1 + x_sum(2 * l + 1)).astype(BF16).astype(F32)

    hout[...] = h_f.astype(BF16)
    swapped(qx, send_q, recv_q).wait_send()
    swapped(sx, send_s, recv_s).wait_send()
    pltpu.make_async_remote_copy(
        src_ref=snd.at[:, pl.ds(0, 3)], dst_ref=kall.at[:, pl.ds(0, 3)], send_sem=send_c.at[0], recv_sem=recv_c.at[0],
        device_id={"tp": partner}, device_id_type=MESH).wait_send()
    pltpu.make_async_remote_copy(
        src_ref=xrecv.at[:, pl.ds(0, 3)], dst_ref=xrecv.at[:, pl.ds(0, 3)], send_sem=send_x.at[0], recv_sem=recv_x.at[0],
        device_id={"tp": partner}, device_id_type=MESH).wait_send()


def _store(h, k1, v1, k2, v2, ho, ok1, ov1, ok2, ov2, sem):
    copies = [pltpu.make_async_copy(a, b, sem.at[i])
              for i, (a, b) in enumerate(((k1, ok1), (v1, ov1), (k2, ok2), (v2, ov2), (h, ho)))]
    for c in copies:
        c.start()
    for c in copies:
        c.wait()


def solution(mesh):
    seq_spec = P('dp', 'tp', None, None)
    head_spec = P('dp', None, 'tp', None)
    col_spec = P(None, None, 'tp')
    ff_spec = P(None, None, None, 'tp')
    inv_freq = (THETA ** (-2.0 * np.arange(32, dtype=np.float64) / 64)).astype(np.float32)
    inv_row = np.tile(inv_freq, 4)[None, :]

    def local_step(hidden, lengths, choice, keys_one, vals_one, keys_two, vals_two, g_attn, w_q, w_k, w_v, w_o, g_mlp, w_router, w_gate, w_up, w_down):
        shapes = (jax.ShapeDtypeStruct((B, D), BF16),) + (jax.ShapeDtypeStruct((B, 2 * SEQ, 64), BF16),) * 4
        any_spec = pl.BlockSpec(memory_space=pl.ANY)
        vmem_spec = pl.BlockSpec(memory_space=pltpu.VMEM)
        V = pltpu.VMEM
        DMA = pltpu.SemaphoreType.DMA
        outs = pl.pallas_call(
            _kernel,
            out_shape=tuple(V(s.shape, s.dtype) for s in shapes),
            in_specs=[any_spec] * 18,
            out_specs=(vmem_spec,) * 5,
            scratch_shapes=[
                V((B, D), BF16), V((1, B), jnp.int32), V((2, 8, B), jnp.int32), V((4, B, BLK, 8, 64), BF16),
                V((2, D), BF16), V((2, D, 256), BF16), V((2, D, 128), BF16), V((2, D, 128), BF16), V((2, 256, D), BF16),
                V((2, D), BF16), V((2, EXP, D), BF16), V((2, EXP, D, FL), BF16), V((2, EXP, D, FL), BF16), V((2, EXP, FL, D), BF16),
                V((1, 128), F32),
                V((B * BLK * 8, 64), F32), V((4, NTP, B, BLK, 128), BF16), V((4, NTP, B, BLK, 128), BF16),
                V((4, B, D), BF16), V((4, NTP, B, D), BF16), V((B, EXP * FL), BF16), V((B, 256), BF16), V((NTP, B, 256), BF16), V((NTP, 8, 128), F32), V((NTP, 8, 128), F32), V((128, 1024), BF16),
                DMA((11,)), DMA((4,)), DMA((2, 3)), DMA((1,)), DMA((4,)), DMA((1,)), DMA((4,)), DMA((1,)), DMA((1,)), DMA((1,)), DMA((1,)),
            ],
            compiler_params=pltpu.CompilerParams(collective_id=0, has_side_effects=True, vmem_limit_bytes=64_000_000),
        )(hidden, lengths.reshape(1, B), jnp.transpose(choice, (0, 2, 1)), keys_one, vals_one, keys_two, vals_two,
          g_attn, w_q, w_k, w_v, w_o, g_mlp, jnp.transpose(w_router, (0, 2, 1)), w_gate, w_up, w_down, jnp.asarray(inv_row))
        outs = pl.pallas_call(
            _store,
            out_shape=shapes,
            in_specs=[vmem_spec] * 5,
            out_specs=(any_spec,) * 5,
            scratch_shapes=[DMA((5,))],
        )(*[pltpu.with_memory_space_constraint(o, pltpu.VMEM) for o in outs])
        return (outs[0],) + tuple(o.reshape(B, SEQ, 2, 64) for o in outs[1:])

    return jax.shard_map(local_step, mesh=mesh, in_specs=(P('dp', None), P('dp'), P(None, 'dp', None), seq_spec, seq_spec, seq_spec, seq_spec, P(), col_spec, col_spec, col_spec, P(None, 'tp', None), P(), P(), ff_spec, ff_spec, P(None, None, 'tp', None)), out_specs=(P('dp', None), head_spec, head_spec, head_spec, head_spec), check_vma=False)
```

```python
import functools

import numpy as np

import jax
import jax.numpy as jnp
from jax import lax
from jax.experimental import pallas as pl
from jax.experimental.pallas import tpu as pltpu
from jax.sharding import PartitionSpec as P

EPS = 1e-5
THETA = 1000000.0
MESH = pl.DeviceIdType.MESH
B = 16
D = 1024
SEQ = 64
BLK = 16
NTP = 4
EXP = 32
FL = 128
PIECES = (((0, 1024),), ((0, 512), (512, 512)))
NP = 2
F32 = jnp.float32
BF16 = jnp.bfloat16


def _norm(h_f, gain_row):
    scale = lax.rsqrt(jnp.mean(h_f * h_f, axis=-1, keepdims=True) + EPS)
    return (h_f * scale * gain_row).astype(BF16)


def _rope(x, cosv, sinv, low):
    rot = jnp.where(low, -pltpu.roll(x, 96, 1), pltpu.roll(x, 32, 1))
    return x * cosv + rot * sinv


def _kernel(hid_h, len_h, cho_h, k1_h, v1_h, k2_h, v2_h, ga_h, wq_h, wk_h, wv_h, wo_h, gm_h, wr_h, wg_h, wu_h, wd_h, inv_h,
            hout, ok1, ov1, ok2, ov2,
            hid, lens, cho, raw, ga, wq, wk, wv, wo, gm, wr, wg, wu, wd, inv,
            spread, snd, kall, xown, xrecv, act, qown, qx, sown, sx, emat,
            sem_s, sem_raw, sem_w, send_c, recv_c, send_x, recv_x, send_q, recv_q, send_s, recv_s):
    me = lax.axis_index("tp")
    chip, core = me // 2, me % 2
    partner = chip * 2 + (1 - core)
    cross_a = (1 - chip) * 2 + core
    cross_b = (1 - chip) * 2 + (1 - core)
    peers = (cross_a, cross_b, partner)

    barrier = pltpu.get_barrier_semaphore()
    for p in peers:
        pl.semaphore_signal(barrier, inc=1, device_id={"tp": p}, device_id_type=MESH)

    raw_src = (k1_h, v1_h, k2_h, v2_h)

    def raw_copy(c):
        return pltpu.make_async_copy(raw_src[c], raw.at[c], sem_raw.at[c])

    smalls = ((hid_h, hid), (len_h, lens), (cho_h, cho), (ga_h, ga), (gm_h, gm), (inv_h, inv),
              (wq_h.at[0], wq.at[0]), (wk_h.at[0], wk.at[0]), (wv_h.at[0], wv.at[0]), (wo_h, wo), (wr_h, wr),
              (wq_h.at[1], wq.at[1]), (wk_h.at[1], wk.at[1]), (wv_h.at[1], wv.at[1]))

    def small_copy(i):
        return pltpu.make_async_copy(smalls[i][0], smalls[i][1], sem_s.at[i])

    def w_copy(l, k):
        src, dst = ((wg_h, wg), (wu_h, wu), (wd_h, wd))[k]
        return pltpu.make_async_copy(src.at[l], dst.at[l], sem_w.at[l, k])

    FIRST = (0, 1, 3, 5, 6, 7, 8)
    for i in FIRST:
        small_copy(i).start()
    raw_copy(1).start()

    def start_layer(l):
        for k in range(3):
            w_copy(l, k).start()

    def cache_send(c, n):
        pltpu.make_async_remote_copy(
            src_ref=snd.at[c, peers[n]], dst_ref=kall.at[c, me],
            send_sem=send_c.at[0], recv_sem=recv_c.at[c],
            device_id={"tp": peers[n]}, device_id_type=MESH).start()

    def cache_wait(c):
        pltpu.make_async_remote_copy(
            src_ref=snd.at[c, pl.ds(0, 3)], dst_ref=kall.at[c, pl.ds(0, 3)],
            send_sem=send_c.at[0], recv_sem=recv_c.at[c],
            device_id={"tp": partner}, device_id_type=MESH).wait_recv()

    def repack(c):
        spread[...] = raw[c].reshape(B * BLK * 8, 64).astype(F32)
        for p in range(NTP):
            lo = spread[pl.ds(2 * p, B * BLK, stride=8), :]
            hi = spread[pl.ds(2 * p + 1, B * BLK, stride=8), :]
            snd[c, p] = jnp.concatenate([lo, hi], axis=1).astype(BF16).reshape(B, BLK, 128)
        kall[c, me] = snd[c, me]

    for i in FIRST:
        small_copy(i).wait()
    raw_copy(0).start()
    for i in range(len(smalls)):
        if i not in FIRST:
            small_copy(i).start()
    raw_copy(2).start()
    raw_copy(3).start()

    eye = lax.broadcasted_iota(jnp.int32, (B, B), 0) == lax.broadcasted_iota(jnp.int32, (B, B), 1)
    len_row = jnp.broadcast_to(lens[...].astype(F32), (B, B))
    len_col = jnp.sum(jnp.where(eye, len_row, 0.0), axis=1, keepdims=True)
    len_b = jnp.broadcast_to(len_col, (B, 128))
    angle = len_b * inv[...]
    cosv, sinv = jnp.cos(angle), jnp.sin(angle)
    lane = lax.broadcasted_iota(jnp.int32, (B, 128), 1)
    low = (lane % 64) < 32
    left = lane < 64
    col = lax.broadcasted_iota(jnp.int32, (64, 1024), 1)
    row = lax.broadcasted_iota(jnp.int32, (64, 1024), 0)
    len64 = jnp.concatenate([len_col] * 4, axis=0)
    pos = ((col // 256) * BLK + col % BLK).astype(F32)
    valid = (((col // BLK) % B) == (row % B)) & (pos < len64)

    h_f = hid[...].astype(F32)

    def project(l, h_f):
        a = _norm(h_f, ga[pl.ds(l, 1), :].astype(F32))
        qf = jnp.dot(a, wq[l], preferred_element_type=F32)
        kf = jnp.dot(a, wk[l], preferred_element_type=F32)
        vf = jnp.dot(a, wv[l], preferred_element_type=F32)
        q = jnp.concatenate([_rope(qf[:, :128], cosv, sinv, low), _rope(qf[:, 128:], cosv, sinv, low)], axis=1).astype(BF16)
        return q, _rope(kf, cosv, sinv, low).astype(BF16).astype(F32), vf.astype(BF16).astype(F32)

    def head_rows(q):
        q0, q1 = q[:, :128].astype(F32), q[:, 128:].astype(F32)
        zero = jnp.zeros_like(q0)
        return jnp.concatenate([
            jnp.where(left, q0, zero), jnp.where(left, pltpu.roll(q0, 64, 1), zero),
            jnp.where(left, zero, pltpu.roll(q1, 64, 1)), jnp.where(left, zero, q1)], axis=0).astype(BF16)

    def swap(src, dst, send, recv, n):
        pltpu.make_async_remote_copy(src_ref=src, dst_ref=dst, send_sem=send.at[0], recv_sem=recv.at[0],
                                     device_id={"tp": peers[n]}, device_id_type=MESH).start()

    def swapped(ref, send, recv):
        return pltpu.make_async_remote_copy(src_ref=ref.at[pl.ds(0, 3)], dst_ref=ref.at[pl.ds(0, 3)], send_sem=send.at[0],
                                            recv_sem=recv.at[0], device_id={"tp": partner}, device_id_type=MESH)

    q, knew, vnew = project(0, h_f)
    qown[...] = q
    pl.semaphore_wait(barrier, 3)
    for n in range(3):
        swap(qown, qx.at[me], send_q, recv_q, n)
    qx[me] = q
    raw_copy(1).wait()
    repack(1)
    for n in range(3):
        cache_send(1, n)
    raw_copy(0).wait()
    repack(0)
    lane8 = lax.broadcasted_iota(jnp.int32, (8, 128), 1) // BLK
    colk = lax.broadcasted_iota(jnp.int32, (64, 256), 1)
    rowk = lax.broadcasted_iota(jnp.int32, (64, 256), 0)
    own_b = ((colk // BLK) % B) == (rowk % B)
    ecol = lax.broadcasted_iota(jnp.int32, (128, 1024), 1)
    erow = lax.broadcasted_iota(jnp.int32, (128, 1024), 0)
    emat[...] = jnp.where((ecol // 256) * BLK + ecol % BLK == erow, 1.0, 0.0).astype(BF16)
    for i in range(len(smalls)):
        if i not in FIRST:
            small_copy(i).wait()
    raw_copy(2).wait()
    raw_copy(3).wait()
    start_layer(0)
    swapped(qx, send_q, recv_q).wait_recv()
    for p in range(NTP):
        sk = lax.dot_general(head_rows(qx[p]), snd[0, p].reshape(B * BLK, 128), (((1,), (1,)), ((), ())), preferred_element_type=F32) * 0.125
        sk = jnp.where(own_b, sk, 0.0)
        sk = sk[:, :128] + sk[:, 128:]
        for shift in (64, 32, 16):
            sk = sk + pltpu.roll(sk, shift, 1)
        packed = sk[0:8]
        for k in range(1, 8):
            packed = jnp.where(lane8 == k, sk[8 * k:8 * k + 8], packed)
        sown[p] = packed
    for n in range(3):
        swap(sown.at[peers[n]], sx.at[me], send_s, recv_s, n)
    sx[me] = sown[me]
    repack(2)
    cache_send(2, 0)
    cache_send(2, 2)
    repack(3)
    cache_send(3, 2)
    cache_send(0, 2)

    def emit(c, new):
        new3 = jnp.broadcast_to(new[:, None, :], (B, BLK, 128))
        len3 = jnp.broadcast_to(len_b[:, None, :], (B, BLK, 128))
        pos3 = lax.broadcasted_iota(jnp.int32, (B, BLK, 128), 1).astype(F32)
        for s in range(NTP):
            x = jnp.where(pos3 + float(s * BLK) == len3, new3, kall[c, s].astype(F32)).reshape(B * BLK, 128)
            spread[pl.ds(0, B * BLK, stride=2), :] = x[:, :64]
            spread[pl.ds(1, B * BLK, stride=2), :] = x[:, 64:]
            outs[c][:, pl.ds(s * 2 * BLK, 2 * BLK), :] = spread[pl.ds(0, 2 * B * BLK), :].astype(BF16).reshape(B, 2 * BLK, 64)

    def x_send(step, piece, val):
        sl = pl.ds(*PIECES[step % 2][piece])
        xown[step, :, sl] = val
        for n in range(3):
            pltpu.make_async_remote_copy(
                src_ref=xown.at[step, :, sl], dst_ref=xrecv.at[step, me, :, sl],
                send_sem=send_x.at[0], recv_sem=recv_x.at[step],
                device_id={"tp": peers[n]}, device_id_type=MESH).start()
        xrecv[step, me, :, sl] = val

    def x_sum(step):
        pltpu.make_async_remote_copy(
            src_ref=xrecv.at[step, pl.ds(0, 3)], dst_ref=xrecv.at[step, pl.ds(0, 3)],
            send_sem=send_x.at[0], recv_sem=recv_x.at[step],
            device_id={"tp": partner}, device_id_type=MESH).wait_recv()
        tot = xrecv[step, 0].astype(F32)
        for s in range(1, NTP):
            tot = tot + xrecv[step, s].astype(F32)
        return tot

    outs = (ok1, ov1, ok2, ov2)

    for l in range(2):
        if l == 1:
            q, knew, vnew = project(l, h_f)
        qrows = head_rows(q)
        kc, vc = 2 * l, 2 * l + 1
        ns = jnp.sum(qrows.astype(F32) * jnp.concatenate([knew] * 4, axis=0), axis=1, keepdims=True) * 0.125
        if l == 0:
            swapped(sx, send_s, recv_s).wait_recv()
            rows = []
            for k in range(8):
                acc = jnp.zeros((8, 128), F32)
                for sd in range(NTP):
                    shift = (BLK * (sd - k)) % 128
                    part = sx[sd] if shift == 0 else pltpu.roll(sx[sd], shift, 1)
                    acc = jnp.where(lane8 == sd, part, acc)
                rows.append(acc)
            sc = jnp.concatenate(rows, axis=0)
            ok = lax.broadcasted_iota(jnp.int32, (64, 128), 1).astype(F32) < len64
        else:
            cache_wait(kc)
            k2d = kall[kc].reshape(NTP * B * BLK, 128)
            sc = lax.dot_general(qrows, k2d, (((1,), (1,)), ((), ())), preferred_element_type=F32) * 0.125
            ok = valid
        sc = jnp.where(ok, sc, -1e30)
        top = jnp.maximum(jnp.max(sc, axis=1, keepdims=True), ns)
        ex, nex = jnp.exp(sc - top), jnp.exp(ns - top)
        den = jnp.sum(ex, axis=1, keepdims=True) + nex
        prob = (ex / den).astype(BF16)
        nprob = (nex / den).astype(BF16).astype(F32)
        if l == 0:
            wide = jnp.dot(prob, emat[...], preferred_element_type=F32)
            prob = jnp.where(valid, wide, 0.0).astype(BF16)
        cache_wait(vc)
        v2d = kall[vc].reshape(NTP * B * BLK, 128)
        ov = jnp.dot(prob, v2d, preferred_element_type=F32) + nprob * jnp.concatenate([vnew] * 4, axis=0)
        attn = jnp.concatenate([jnp.where(left, ov[0:16], ov[48:64]), jnp.where(left, ov[16:32], ov[32:48])], axis=1).astype(BF16)
        wo_rows = jnp.concatenate([wo[l, pl.ds(0, 64), :], wo[l, pl.ds(192, 64), :], wo[l, pl.ds(64, 128), :]], axis=0)
        x_send(2 * l, 0, jnp.dot(attn, wo_rows, preferred_element_type=F32).astype(BF16))
        if l == 0:
            cache_send(2, 1)
            cache_send(3, 0)
            cache_send(3, 1)
        else:
            cache_send(0, 0)
            cache_send(0, 1)
            emit(kc, knew)
        emit(vc, vnew)
        for k in range(3):
            w_copy(l, k).wait()
        if l == 0:
            start_layer(1)
        h1 = (h_f + x_sum(2 * l)).astype(BF16).astype(F32)
        m = _norm(h1, gm[pl.ds(l, 1), :].astype(F32))

        lg = lax.dot_general(wr[l], m, (((1,), (1,)), ((), ())), preferred_element_type=F32)
        eid = lax.broadcasted_iota(jnp.int32, (EXP, B), 0)
        chosen = eid < 0
        for k in range(8):
            chosen = chosen | (cho[l, pl.ds(k, 1), :] == eid)
        lg = jnp.where(chosen, lg, -jnp.inf)
        ex = jnp.where(chosen, jnp.exp(lg - jnp.max(lg, axis=0, keepdims=True)), 0.0)
        gate_t = ex / jnp.sum(ex, axis=0, keepdims=True)
        gate = gate_t.T
        for e in range(EXP):
            w = jnp.concatenate([wg[l, e], wu[l, e]], axis=1)
            gu = jnp.dot(m, w, preferred_element_type=F32)
            g, u = gu[:, :FL], gu[:, FL:]
            act[:, pl.ds(e * FL, FL)] = (g * jax.nn.sigmoid(g) * u * jnp.broadcast_to(gate[:, e:e + 1], (B, FL))).astype(BF16)
        def down(piece, pairs, acc):
            first, width = PIECES[1][piece]
            for e in pairs:
                rhs = wd[l, pl.ds(e, 2), :, pl.ds(first, width)].reshape(2 * FL, width)
                acc = acc + jnp.dot(act[:, pl.ds(e * FL, 2 * FL)], rhs, preferred_element_type=F32)
            return acc

        acc0 = down(0, range(0, EXP, 2), jnp.zeros((B, PIECES[1][0][1]), F32))
        acc1 = down(1, range(0, 8, 2), jnp.zeros((B, PIECES[1][1][1]), F32))
        x_send(2 * l + 1, 0, acc0.astype(BF16))
        acc1 = down(1, range(8, EXP, 2), acc1)
        x_send(2 * l + 1, 1, acc1.astype(BF16))
        if l == 0:
            kone = knew
        else:
            cache_wait(0)
            emit(0, kone)
        h_f = (h1 + x_sum(2 * l + 1)).astype(BF16).astype(F32)

    hout[...] = h_f.astype(BF16)
    swapped(qx, send_q, recv_q).wait_send()
    swapped(sx, send_s, recv_s).wait_send()
    pltpu.make_async_remote_copy(
        src_ref=snd.at[:, pl.ds(0, 3)], dst_ref=kall.at[:, pl.ds(0, 3)], send_sem=send_c.at[0], recv_sem=recv_c.at[0],
        device_id={"tp": partner}, device_id_type=MESH).wait_send()
    pltpu.make_async_remote_copy(
        src_ref=xrecv.at[:, pl.ds(0, 3)], dst_ref=xrecv.at[:, pl.ds(0, 3)], send_sem=send_x.at[0], recv_sem=recv_x.at[0],
        device_id={"tp": partner}, device_id_type=MESH).wait_send()


def _store(h, k1, v1, k2, v2, ho, ok1, ov1, ok2, ov2, sem):
    copies = [pltpu.make_async_copy(a, b, sem.at[i])
              for i, (a, b) in enumerate(((k1, ok1), (v1, ov1), (k2, ok2), (v2, ov2), (h, ho)))]
    for c in copies:
        c.start()
    for c in copies:
        c.wait()


def solution(mesh):
    seq_spec = P('dp', 'tp', None, None)
    head_spec = P('dp', None, 'tp', None)
    col_spec = P(None, None, 'tp')
    ff_spec = P(None, None, None, 'tp')
    inv_freq = (THETA ** (-2.0 * np.arange(32, dtype=np.float64) / 64)).astype(np.float32)
    inv_row = np.tile(inv_freq, 4)[None, :]

    def local_step(hidden, lengths, choice, keys_one, vals_one, keys_two, vals_two, g_attn, w_q, w_k, w_v, w_o, g_mlp, w_router, w_gate, w_up, w_down):
        shapes = (jax.ShapeDtypeStruct((B, D), BF16),) + (jax.ShapeDtypeStruct((B, 2 * SEQ, 64), BF16),) * 4
        any_spec = pl.BlockSpec(memory_space=pl.ANY)
        vmem_spec = pl.BlockSpec(memory_space=pltpu.VMEM)
        V = pltpu.VMEM
        DMA = pltpu.SemaphoreType.DMA
        outs = pl.pallas_call(
            _kernel,
            out_shape=tuple(V(s.shape, s.dtype) for s in shapes),
            in_specs=[any_spec] * 18,
            out_specs=(vmem_spec,) * 5,
            scratch_shapes=[
                V((B, D), BF16), V((1, B), jnp.int32), V((2, 8, B), jnp.int32), V((4, B, BLK, 8, 64), BF16),
                V((2, D), BF16), V((2, D, 256), BF16), V((2, D, 128), BF16), V((2, D, 128), BF16), V((2, 256, D), BF16),
                V((2, D), BF16), V((2, EXP, D), BF16), V((2, EXP, D, FL), BF16), V((2, EXP, D, FL), BF16), V((2, EXP, FL, D), BF16),
                V((1, 128), F32),
                V((B * BLK * 8, 64), F32), V((4, NTP, B, BLK, 128), BF16), V((4, NTP, B, BLK, 128), BF16),
                V((4, B, D), BF16), V((4, NTP, B, D), BF16), V((B, EXP * FL), BF16), V((B, 256), BF16), V((NTP, B, 256), BF16), V((NTP, 8, 128), F32), V((NTP, 8, 128), F32), V((128, 1024), BF16),
                DMA((14,)), DMA((4,)), DMA((2, 3)), DMA((1,)), DMA((4,)), DMA((1,)), DMA((4,)), DMA((1,)), DMA((1,)), DMA((1,)), DMA((1,)),
            ],
            compiler_params=pltpu.CompilerParams(collective_id=0, has_side_effects=True, vmem_limit_bytes=64_000_000),
        )(hidden, lengths.reshape(1, B), jnp.transpose(choice, (0, 2, 1)), keys_one, vals_one, keys_two, vals_two,
          g_attn, w_q, w_k, w_v, w_o, g_mlp, jnp.transpose(w_router, (0, 2, 1)), w_gate, w_up, w_down, jnp.asarray(inv_row))
        outs = pl.pallas_call(
            _store,
            out_shape=shapes,
            in_specs=[vmem_spec] * 5,
            out_specs=(any_spec,) * 5,
            scratch_shapes=[DMA((5,))],
        )(*[pltpu.with_memory_space_constraint(o, pltpu.VMEM) for o in outs])
        return (outs[0],) + tuple(o.reshape(B, SEQ, 2, 64) for o in outs[1:])

    return jax.shard_map(local_step, mesh=mesh, in_specs=(P('dp', None), P('dp'), P(None, 'dp', None), seq_spec, seq_spec, seq_spec, seq_spec, P(), col_spec, col_spec, col_spec, P(None, 'tp', None), P(), P(), ff_spec, ff_spec, P(None, None, 'tp', None)), out_specs=(P('dp', None), head_spec, head_spec, head_spec, head_spec), check_vma=False)
```

```python
import functools

import numpy as np

import jax
import jax.numpy as jnp
from jax import lax
from jax.experimental import pallas as pl
from jax.experimental.pallas import tpu as pltpu
from jax.sharding import PartitionSpec as P

EPS = 1e-5
THETA = 1000000.0
MESH = pl.DeviceIdType.MESH
B = 16
D = 1024
SEQ = 64
BLK = 16
NTP = 4
EXP = 32
FL = 128
PIECES = (((0, 1024),), ((0, 512), (512, 512)))
NP = 2
F32 = jnp.float32
BF16 = jnp.bfloat16


def _norm(h_f, gain_row):
    scale = lax.rsqrt(jnp.mean(h_f * h_f, axis=-1, keepdims=True) + EPS)
    return (h_f * scale * gain_row).astype(BF16)


def _rope(x, cosv, sinv, low):
    rot = jnp.where(low, -pltpu.roll(x, 96, 1), pltpu.roll(x, 32, 1))
    return x * cosv + rot * sinv


def _kernel(hid_h, len_h, cho_h, k1_h, v1_h, k2_h, v2_h, ga_h, wq_h, wk_h, wv_h, wo_h, gm_h, wr_h, wg_h, wu_h, wd_h, inv_h,
            hout, ok1, ov1, ok2, ov2,
            hid, lens, cho, raw, ga, wq, wk, wv, wo, gm, wr, wg, wu, wd, inv,
            spread, snd, kall, xown, xrecv, act, qown, qx, sown, sx, emat,
            sem_s, sem_raw, sem_w, send_c, recv_c, send_x, recv_x, send_q, recv_q, send_s, recv_s):
    me = lax.axis_index("tp")
    chip, core = me // 2, me % 2
    partner = chip * 2 + (1 - core)
    cross_a = (1 - chip) * 2 + core
    cross_b = (1 - chip) * 2 + (1 - core)
    peers = (cross_a, cross_b, partner)

    barrier = pltpu.get_barrier_semaphore()
    for p in peers:
        pl.semaphore_signal(barrier, inc=1, device_id={"tp": p}, device_id_type=MESH)

    raw_src = (k1_h, v1_h, k2_h, v2_h)

    def raw_copy(c):
        return pltpu.make_async_copy(raw_src[c], raw.at[c], sem_raw.at[c])

    smalls = ((hid_h, hid), (len_h, lens), (cho_h, cho), (ga_h, ga), (gm_h, gm), (inv_h, inv),
              (wq_h.at[0], wq.at[0]), (wk_h.at[0], wk.at[0]), (wv_h.at[0], wv.at[0]), (wo_h, wo), (wr_h, wr),
              (wq_h.at[1], wq.at[1]), (wk_h.at[1], wk.at[1]), (wv_h.at[1], wv.at[1]))

    def small_copy(i):
        return pltpu.make_async_copy(smalls[i][0], smalls[i][1], sem_s.at[i])

    def w_copy(l, k):
        src, dst = ((wg_h, wg), (wu_h, wu), (wd_h, wd))[k]
        return pltpu.make_async_copy(src.at[l], dst.at[l], sem_w.at[l, k])

    FIRST = (0, 1, 3, 5, 6, 7, 8)
    for i in FIRST:
        small_copy(i).start()
    raw_copy(1).start()

    def start_layer(l):
        for k in range(3):
            w_copy(l, k).start()

    def cache_send(c, n):
        pltpu.make_async_remote_copy(
            src_ref=snd.at[c, peers[n]], dst_ref=kall.at[c, me],
            send_sem=send_c.at[0], recv_sem=recv_c.at[c],
            device_id={"tp": peers[n]}, device_id_type=MESH).start()

    def cache_wait(c):
        pltpu.make_async_remote_copy(
            src_ref=snd.at[c, pl.ds(0, 3)], dst_ref=kall.at[c, pl.ds(0, 3)],
            send_sem=send_c.at[0], recv_sem=recv_c.at[c],
            device_id={"tp": partner}, device_id_type=MESH).wait_recv()

    def repack(c):
        spread[...] = raw[c].reshape(B * BLK * 8, 64).astype(F32)
        for p in range(NTP):
            lo = spread[pl.ds(2 * p, B * BLK, stride=8), :]
            hi = spread[pl.ds(2 * p + 1, B * BLK, stride=8), :]
            snd[c, p] = jnp.concatenate([lo, hi], axis=1).astype(BF16).reshape(B, BLK, 128)
        kall[c, me] = snd[c, me]

    for i in FIRST:
        small_copy(i).wait()
    raw_copy(0).start()
    for i in range(len(smalls)):
        if i not in FIRST:
            small_copy(i).start()
    raw_copy(2).start()
    raw_copy(3).start()

    eye = lax.broadcasted_iota(jnp.int32, (B, B), 0) == lax.broadcasted_iota(jnp.int32, (B, B), 1)
    len_row = jnp.broadcast_to(lens[...].astype(F32), (B, B))
    len_col = jnp.sum(jnp.where(eye, len_row, 0.0), axis=1, keepdims=True)
    len_b = jnp.broadcast_to(len_col, (B, 128))
    angle = len_b * inv[...]
    cosv, sinv = jnp.cos(angle), jnp.sin(angle)
    lane = lax.broadcasted_iota(jnp.int32, (B, 128), 1)
    low = (lane % 64) < 32
    left = lane < 64
    col = lax.broadcasted_iota(jnp.int32, (64, 1024), 1)
    row = lax.broadcasted_iota(jnp.int32, (64, 1024), 0)
    len64 = jnp.concatenate([len_col] * 4, axis=0)
    pos = ((col // 256) * BLK + col % BLK).astype(F32)
    valid = (((col // BLK) % B) == (row % B)) & (pos < len64)

    h_f = hid[...].astype(F32)

    def project(l, h_f):
        a = _norm(h_f, ga[pl.ds(l, 1), :].astype(F32))
        qf = jnp.dot(a, wq[l], preferred_element_type=F32)
        kf = jnp.dot(a, wk[l], preferred_element_type=F32)
        vf = jnp.dot(a, wv[l], preferred_element_type=F32)
        q = jnp.concatenate([_rope(qf[:, :128], cosv, sinv, low), _rope(qf[:, 128:], cosv, sinv, low)], axis=1).astype(BF16)
        return q, _rope(kf, cosv, sinv, low).astype(BF16).astype(F32), vf.astype(BF16).astype(F32)

    def head_rows(q):
        q0, q1 = q[:, :128].astype(F32), q[:, 128:].astype(F32)
        zero = jnp.zeros_like(q0)
        return jnp.concatenate([
            jnp.where(left, q0, zero), jnp.where(left, pltpu.roll(q0, 64, 1), zero),
            jnp.where(left, zero, pltpu.roll(q1, 64, 1)), jnp.where(left, zero, q1)], axis=0).astype(BF16)

    def swap(src, dst, send, recv, n):
        pltpu.make_async_remote_copy(src_ref=src, dst_ref=dst, send_sem=send.at[0], recv_sem=recv.at[0],
                                     device_id={"tp": peers[n]}, device_id_type=MESH).start()

    def swapped(ref, send, recv):
        return pltpu.make_async_remote_copy(src_ref=ref.at[pl.ds(0, 3)], dst_ref=ref.at[pl.ds(0, 3)], send_sem=send.at[0],
                                            recv_sem=recv.at[0], device_id={"tp": partner}, device_id_type=MESH)

    q, knew, vnew = project(0, h_f)
    qown[...] = q
    pl.semaphore_wait(barrier, 3)
    for n in range(3):
        swap(qown, qx.at[me], send_q, recv_q, n)
    qx[me] = q
    raw_copy(1).wait()
    repack(1)
    for n in range(3):
        cache_send(1, n)
    raw_copy(0).wait()
    for i in range(len(smalls)):
        if i not in FIRST:
            small_copy(i).wait()
    raw_copy(2).wait()
    raw_copy(3).wait()
    start_layer(0)
    repack(0)
    lane8 = lax.broadcasted_iota(jnp.int32, (8, 128), 1) // BLK
    colk = lax.broadcasted_iota(jnp.int32, (64, 256), 1)
    rowk = lax.broadcasted_iota(jnp.int32, (64, 256), 0)
    own_b = ((colk // BLK) % B) == (rowk % B)
    ecol = lax.broadcasted_iota(jnp.int32, (128, 1024), 1)
    erow = lax.broadcasted_iota(jnp.int32, (128, 1024), 0)
    emat[...] = jnp.where((ecol // 256) * BLK + ecol % BLK == erow, 1.0, 0.0).astype(BF16)
    swapped(qx, send_q, recv_q).wait_recv()
    for p in range(NTP):
        sk = lax.dot_general(head_rows(qx[p]), snd[0, p].reshape(B * BLK, 128), (((1,), (1,)), ((), ())), preferred_element_type=F32) * 0.125
        sk = jnp.where(own_b, sk, 0.0)
        sk = sk[:, :128] + sk[:, 128:]
        for shift in (64, 32, 16):
            sk = sk + pltpu.roll(sk, shift, 1)
        packed = sk[0:8]
        for k in range(1, 8):
            packed = jnp.where(lane8 == k, sk[8 * k:8 * k + 8], packed)
        sown[p] = packed
    for n in range(3):
        swap(sown.at[peers[n]], sx.at[me], send_s, recv_s, n)
    sx[me] = sown[me]
    repack(2)
    cache_send(2, 0)
    cache_send(2, 2)
    repack(3)
    cache_send(3, 2)
    cache_send(0, 2)

    def emit(c, new):
        new3 = jnp.broadcast_to(new[:, None, :], (B, BLK, 128))
        len3 = jnp.broadcast_to(len_b[:, None, :], (B, BLK, 128))
        pos3 = lax.broadcasted_iota(jnp.int32, (B, BLK, 128), 1).astype(F32)
        for s in range(NTP):
            x = jnp.where(pos3 + float(s * BLK) == len3, new3, kall[c, s].astype(F32)).reshape(B * BLK, 128)
            spread[pl.ds(0, B * BLK, stride=2), :] = x[:, :64]
            spread[pl.ds(1, B * BLK, stride=2), :] = x[:, 64:]
            outs[c][:, pl.ds(s * 2 * BLK, 2 * BLK), :] = spread[pl.ds(0, 2 * B * BLK), :].astype(BF16).reshape(B, 2 * BLK, 64)

    def x_send(step, piece, val):
        sl = pl.ds(*PIECES[step % 2][piece])
        xown[step, :, sl] = val
        for n in range(3):
            pltpu.make_async_remote_copy(
                src_ref=xown.at[step, :, sl], dst_ref=xrecv.at[step, me, :, sl],
                send_sem=send_x.at[0], recv_sem=recv_x.at[step],
                device_id={"tp": peers[n]}, device_id_type=MESH).start()
        xrecv[step, me, :, sl] = val

    def x_sum(step):
        pltpu.make_async_remote_copy(
            src_ref=xrecv.at[step, pl.ds(0, 3)], dst_ref=xrecv.at[step, pl.ds(0, 3)],
            send_sem=send_x.at[0], recv_sem=recv_x.at[step],
            device_id={"tp": partner}, device_id_type=MESH).wait_recv()
        tot = xrecv[step, 0].astype(F32)
        for s in range(1, NTP):
            tot = tot + xrecv[step, s].astype(F32)
        return tot

    outs = (ok1, ov1, ok2, ov2)

    for l in range(2):
        if l == 1:
            q, knew, vnew = project(l, h_f)
        qrows = head_rows(q)
        kc, vc = 2 * l, 2 * l + 1
        ns = jnp.sum(qrows.astype(F32) * jnp.concatenate([knew] * 4, axis=0), axis=1, keepdims=True) * 0.125
        if l == 0:
            swapped(sx, send_s, recv_s).wait_recv()
            rows = []
            for k in range(8):
                acc = jnp.zeros((8, 128), F32)
                for sd in range(NTP):
                    shift = (BLK * (sd - k)) % 128
                    part = sx[sd] if shift == 0 else pltpu.roll(sx[sd], shift, 1)
                    acc = jnp.where(lane8 == sd, part, acc)
                rows.append(acc)
            sc = jnp.concatenate(rows, axis=0)
            ok = lax.broadcasted_iota(jnp.int32, (64, 128), 1).astype(F32) < len64
        else:
            cache_wait(kc)
            k2d = kall[kc].reshape(NTP * B * BLK, 128)
            sc = lax.dot_general(qrows, k2d, (((1,), (1,)), ((), ())), preferred_element_type=F32) * 0.125
            ok = valid
        sc = jnp.where(ok, sc, -1e30)
        top = jnp.maximum(jnp.max(sc, axis=1, keepdims=True), ns)
        ex, nex = jnp.exp(sc - top), jnp.exp(ns - top)
        den = jnp.sum(ex, axis=1, keepdims=True) + nex
        prob = (ex / den).astype(BF16)
        nprob = (nex / den).astype(BF16).astype(F32)
        if l == 0:
            wide = jnp.dot(prob, emat[...], preferred_element_type=F32)
            prob = jnp.where(valid, wide, 0.0).astype(BF16)
        cache_wait(vc)
        v2d = kall[vc].reshape(NTP * B * BLK, 128)
        ov = jnp.dot(prob, v2d, preferred_element_type=F32) + nprob * jnp.concatenate([vnew] * 4, axis=0)
        attn = jnp.concatenate([jnp.where(left, ov[0:16], ov[48:64]), jnp.where(left, ov[16:32], ov[32:48])], axis=1).astype(BF16)
        wo_rows = jnp.concatenate([wo[l, pl.ds(0, 64), :], wo[l, pl.ds(192, 64), :], wo[l, pl.ds(64, 128), :]], axis=0)
        x_send(2 * l, 0, jnp.dot(attn, wo_rows, preferred_element_type=F32).astype(BF16))
        if l == 0:
            cache_send(2, 1)
            cache_send(3, 0)
            cache_send(3, 1)
        else:
            cache_send(0, 0)
            cache_send(0, 1)
            emit(kc, knew)
        emit(vc, vnew)
        for k in range(3):
            w_copy(l, k).wait()
        if l == 0:
            start_layer(1)
        h1 = (h_f + x_sum(2 * l)).astype(BF16).astype(F32)
        m = _norm(h1, gm[pl.ds(l, 1), :].astype(F32))

        lg = lax.dot_general(wr[l], m, (((1,), (1,)), ((), ())), preferred_element_type=F32)
        eid = lax.broadcasted_iota(jnp.int32, (EXP, B), 0)
        chosen = eid < 0
        for k in range(8):
            chosen = chosen | (cho[l, pl.ds(k, 1), :] == eid)
        lg = jnp.where(chosen, lg, -jnp.inf)
        ex = jnp.where(chosen, jnp.exp(lg - jnp.max(lg, axis=0, keepdims=True)), 0.0)
        gate_t = ex / jnp.sum(ex, axis=0, keepdims=True)
        gate = gate_t.T
        for e in range(EXP):
            w = jnp.concatenate([wg[l, e], wu[l, e]], axis=1)
            gu = jnp.dot(m, w, preferred_element_type=F32)
            g, u = gu[:, :FL], gu[:, FL:]
            act[:, pl.ds(e * FL, FL)] = (g * jax.nn.sigmoid(g) * u * jnp.broadcast_to(gate[:, e:e + 1], (B, FL))).astype(BF16)
        def down(piece, pairs, acc):
            first, width = PIECES[1][piece]
            for e in pairs:
                rhs = wd[l, pl.ds(e, 2), :, pl.ds(first, width)].reshape(2 * FL, width)
                acc = acc + jnp.dot(act[:, pl.ds(e * FL, 2 * FL)], rhs, preferred_element_type=F32)
            return acc

        acc0 = down(0, range(0, EXP, 2), jnp.zeros((B, PIECES[1][0][1]), F32))
        acc1 = down(1, range(0, 8, 2), jnp.zeros((B, PIECES[1][1][1]), F32))
        x_send(2 * l + 1, 0, acc0.astype(BF16))
        acc1 = down(1, range(8, EXP, 2), acc1)
        x_send(2 * l + 1, 1, acc1.astype(BF16))
        if l == 0:
            kone = knew
        else:
            cache_wait(0)
            emit(0, kone)
        h_f = (h1 + x_sum(2 * l + 1)).astype(BF16).astype(F32)

    hout[...] = h_f.astype(BF16)
    swapped(qx, send_q, recv_q).wait_send()
    swapped(sx, send_s, recv_s).wait_send()
    pltpu.make_async_remote_copy(
        src_ref=snd.at[:, pl.ds(0, 3)], dst_ref=kall.at[:, pl.ds(0, 3)], send_sem=send_c.at[0], recv_sem=recv_c.at[0],
        device_id={"tp": partner}, device_id_type=MESH).wait_send()
    pltpu.make_async_remote_copy(
        src_ref=xrecv.at[:, pl.ds(0, 3)], dst_ref=xrecv.at[:, pl.ds(0, 3)], send_sem=send_x.at[0], recv_sem=recv_x.at[0],
        device_id={"tp": partner}, device_id_type=MESH).wait_send()


def _store(h, k1, v1, k2, v2, ho, ok1, ov1, ok2, ov2, sem):
    copies = [pltpu.make_async_copy(a, b, sem.at[i])
              for i, (a, b) in enumerate(((k1, ok1), (v1, ov1), (k2, ok2), (v2, ov2), (h, ho)))]
    for c in copies:
        c.start()
    for c in copies:
        c.wait()


def solution(mesh):
    seq_spec = P('dp', 'tp', None, None)
    head_spec = P('dp', None, 'tp', None)
    col_spec = P(None, None, 'tp')
    ff_spec = P(None, None, None, 'tp')
    inv_freq = (THETA ** (-2.0 * np.arange(32, dtype=np.float64) / 64)).astype(np.float32)
    inv_row = np.tile(inv_freq, 4)[None, :]

    def local_step(hidden, lengths, choice, keys_one, vals_one, keys_two, vals_two, g_attn, w_q, w_k, w_v, w_o, g_mlp, w_router, w_gate, w_up, w_down):
        shapes = (jax.ShapeDtypeStruct((B, D), BF16),) + (jax.ShapeDtypeStruct((B, 2 * SEQ, 64), BF16),) * 4
        any_spec = pl.BlockSpec(memory_space=pl.ANY)
        vmem_spec = pl.BlockSpec(memory_space=pltpu.VMEM)
        V = pltpu.VMEM
        DMA = pltpu.SemaphoreType.DMA
        outs = pl.pallas_call(
            _kernel,
            out_shape=tuple(V(s.shape, s.dtype) for s in shapes),
            in_specs=[any_spec] * 18,
            out_specs=(vmem_spec,) * 5,
            scratch_shapes=[
                V((B, D), BF16), V((1, B), jnp.int32), V((2, 8, B), jnp.int32), V((4, B, BLK, 8, 64), BF16),
                V((2, D), BF16), V((2, D, 256), BF16), V((2, D, 128), BF16), V((2, D, 128), BF16), V((2, 256, D), BF16),
                V((2, D), BF16), V((2, EXP, D), BF16), V((2, EXP, D, FL), BF16), V((2, EXP, D, FL), BF16), V((2, EXP, FL, D), BF16),
                V((1, 128), F32),
                V((B * BLK * 8, 64), F32), V((4, NTP, B, BLK, 128), BF16), V((4, NTP, B, BLK, 128), BF16),
                V((4, B, D), BF16), V((4, NTP, B, D), BF16), V((B, EXP * FL), BF16), V((B, 256), BF16), V((NTP, B, 256), BF16), V((NTP, 8, 128), F32), V((NTP, 8, 128), F32), V((128, 1024), BF16),
                DMA((14,)), DMA((4,)), DMA((2, 3)), DMA((1,)), DMA((4,)), DMA((1,)), DMA((4,)), DMA((1,)), DMA((1,)), DMA((1,)), DMA((1,)),
            ],
            compiler_params=pltpu.CompilerParams(collective_id=0, has_side_effects=True, vmem_limit_bytes=64_000_000),
        )(hidden, lengths.reshape(1, B), jnp.transpose(choice, (0, 2, 1)), keys_one, vals_one, keys_two, vals_two,
          g_attn, w_q, w_k, w_v, w_o, g_mlp, jnp.transpose(w_router, (0, 2, 1)), w_gate, w_up, w_down, jnp.asarray(inv_row))
        outs = pl.pallas_call(
            _store,
            out_shape=shapes,
            in_specs=[vmem_spec] * 5,
            out_specs=(any_spec,) * 5,
            scratch_shapes=[DMA((5,))],
        )(*[pltpu.with_memory_space_constraint(o, pltpu.VMEM) for o in outs])
        return (outs[0],) + tuple(o.reshape(B, SEQ, 2, 64) for o in outs[1:])

    return jax.shard_map(local_step, mesh=mesh, in_specs=(P('dp', None), P('dp'), P(None, 'dp', None), seq_spec, seq_spec, seq_spec, seq_spec, P(), col_spec, col_spec, col_spec, P(None, 'tp', None), P(), P(), ff_spec, ff_spec, P(None, None, 'tp', None)), out_specs=(P('dp', None), head_spec, head_spec, head_spec, head_spec), check_vma=False)
```

```python
import functools

import numpy as np

import jax
import jax.numpy as jnp
from jax import lax
from jax.experimental import pallas as pl
from jax.experimental.pallas import tpu as pltpu
from jax.sharding import PartitionSpec as P

EPS = 1e-5
THETA = 1000000.0
MESH = pl.DeviceIdType.MESH
B = 16
D = 1024
SEQ = 64
BLK = 16
NTP = 4
EXP = 32
FL = 128
PIECES = (((0, 1024),), ((0, 512), (512, 512)))
NP = 2
F32 = jnp.float32
BF16 = jnp.bfloat16


def _norm(h_f, gain_row):
    scale = lax.rsqrt(jnp.mean(h_f * h_f, axis=-1, keepdims=True) + EPS)
    return (h_f * scale * gain_row).astype(BF16)


def _rope(x, cosv, sinv, low):
    rot = jnp.where(low, -pltpu.roll(x, 96, 1), pltpu.roll(x, 32, 1))
    return x * cosv + rot * sinv


def _kernel(hid_h, len_h, cho_h, k1_h, v1_h, k2_h, v2_h, ga_h, wq_h, wk_h, wv_h, wo_h, gm_h, wr_h, wg_h, wu_h, wd_h, inv_h,
            hout, ok1, ov1, ok2, ov2,
            hid, lens, cho, raw, ga, wq, wk, wv, wo, gm, wr, wg, wu, wd, inv,
            spread, snd, kall, xown, xrecv, act, qown, qx, sown, sx, emat,
            sem_s, sem_raw, sem_w, send_c, recv_c, send_x, recv_x, send_q, recv_q, send_s, recv_s):
    me = lax.axis_index("tp")
    chip, core = me // 2, me % 2
    partner = chip * 2 + (1 - core)
    cross_a = (1 - chip) * 2 + core
    cross_b = (1 - chip) * 2 + (1 - core)
    peers = (cross_a, cross_b, partner)

    barrier = pltpu.get_barrier_semaphore()
    for p in peers:
        pl.semaphore_signal(barrier, inc=1, device_id={"tp": p}, device_id_type=MESH)

    raw_src = (k1_h, v1_h, k2_h, v2_h)

    def raw_copy(c):
        return pltpu.make_async_copy(raw_src[c], raw.at[c], sem_raw.at[c])

    smalls = ((hid_h, hid), (len_h, lens), (cho_h, cho), (ga_h, ga), (gm_h, gm), (inv_h, inv),
              (wq_h.at[0], wq.at[0]), (wk_h.at[0], wk.at[0]), (wv_h.at[0], wv.at[0]), (wo_h, wo), (wr_h, wr),
              (wq_h.at[1], wq.at[1]), (wk_h.at[1], wk.at[1]), (wv_h.at[1], wv.at[1]))

    def small_copy(i):
        return pltpu.make_async_copy(smalls[i][0], smalls[i][1], sem_s.at[i])

    def w_copy(l, k):
        src, dst = ((wg_h, wg), (wu_h, wu), (wd_h, wd))[k]
        return pltpu.make_async_copy(src.at[l], dst.at[l], sem_w.at[l, k])

    FIRST = (0, 1, 3, 5, 6, 7, 8)
    for i in FIRST:
        small_copy(i).start()
    raw_copy(1).start()

    def start_layer(l):
        for k in range(3):
            w_copy(l, k).start()

    def cache_send(c, n):
        pltpu.make_async_remote_copy(
            src_ref=snd.at[c, peers[n]], dst_ref=kall.at[c, me],
            send_sem=send_c.at[0], recv_sem=recv_c.at[c],
            device_id={"tp": peers[n]}, device_id_type=MESH).start()

    def cache_wait(c):
        pltpu.make_async_remote_copy(
            src_ref=snd.at[c, pl.ds(0, 3)], dst_ref=kall.at[c, pl.ds(0, 3)],
            send_sem=send_c.at[0], recv_sem=recv_c.at[c],
            device_id={"tp": partner}, device_id_type=MESH).wait_recv()

    def repack(c):
        spread[...] = raw[c].reshape(B * BLK * 8, 64).astype(F32)
        for p in range(NTP):
            lo = spread[pl.ds(2 * p, B * BLK, stride=8), :]
            hi = spread[pl.ds(2 * p + 1, B * BLK, stride=8), :]
            snd[c, p] = jnp.concatenate([lo, hi], axis=1).astype(BF16).reshape(B, BLK, 128)
        kall[c, me] = snd[c, me]

    for i in FIRST:
        small_copy(i).wait()
    raw_copy(0).start()
    for i in range(len(smalls)):
        if i not in FIRST:
            small_copy(i).start()
    raw_copy(2).start()
    raw_copy(3).start()

    eye = lax.broadcasted_iota(jnp.int32, (B, B), 0) == lax.broadcasted_iota(jnp.int32, (B, B), 1)
    len_row = jnp.broadcast_to(lens[...].astype(F32), (B, B))
    len_col = jnp.sum(jnp.where(eye, len_row, 0.0), axis=1, keepdims=True)
    len_b = jnp.broadcast_to(len_col, (B, 128))
    angle = len_b * inv[...]
    cosv, sinv = jnp.cos(angle), jnp.sin(angle)
    lane = lax.broadcasted_iota(jnp.int32, (B, 128), 1)
    low = (lane % 64) < 32
    left = lane < 64
    col = lax.broadcasted_iota(jnp.int32, (64, 1024), 1)
    row = lax.broadcasted_iota(jnp.int32, (64, 1024), 0)
    len64 = jnp.concatenate([len_col] * 4, axis=0)
    pos = ((col // 256) * BLK + col % BLK).astype(F32)
    valid = (((col // BLK) % B) == (row % B)) & (pos < len64)

    h_f = hid[...].astype(F32)

    def project(l, h_f):
        a = _norm(h_f, ga[pl.ds(l, 1), :].astype(F32))
        qf = jnp.dot(a, wq[l], preferred_element_type=F32)
        kf = jnp.dot(a, wk[l], preferred_element_type=F32)
        vf = jnp.dot(a, wv[l], preferred_element_type=F32)
        q = jnp.concatenate([_rope(qf[:, :128], cosv, sinv, low), _rope(qf[:, 128:], cosv, sinv, low)], axis=1).astype(BF16)
        return q, _rope(kf, cosv, sinv, low).astype(BF16).astype(F32), vf.astype(BF16).astype(F32)

    def head_rows(q):
        q0, q1 = q[:, :128].astype(F32), q[:, 128:].astype(F32)
        zero = jnp.zeros_like(q0)
        return jnp.concatenate([
            jnp.where(left, q0, zero), jnp.where(left, pltpu.roll(q0, 64, 1), zero),
            jnp.where(left, zero, pltpu.roll(q1, 64, 1)), jnp.where(left, zero, q1)], axis=0).astype(BF16)

    def swap(src, dst, send, recv, n):
        pltpu.make_async_remote_copy(src_ref=src, dst_ref=dst, send_sem=send.at[0], recv_sem=recv.at[0],
                                     device_id={"tp": peers[n]}, device_id_type=MESH).start()

    def swapped(ref, send, recv):
        return pltpu.make_async_remote_copy(src_ref=ref.at[pl.ds(0, 3)], dst_ref=ref.at[pl.ds(0, 3)], send_sem=send.at[0],
                                            recv_sem=recv.at[0], device_id={"tp": partner}, device_id_type=MESH)

    q, knew, vnew = project(0, h_f)
    qown[...] = q
    pl.semaphore_wait(barrier, 3)
    for n in range(3):
        swap(qown, qx.at[me], send_q, recv_q, n)
    qx[me] = q
    raw_copy(1).wait()
    repack(1)
    cache_send(1, 0)
    cache_send(1, 2)
    raw_copy(0).wait()
    for i in range(len(smalls)):
        if i not in FIRST:
            small_copy(i).wait()
    raw_copy(2).wait()
    raw_copy(3).wait()
    start_layer(0)
    repack(0)
    lane8 = lax.broadcasted_iota(jnp.int32, (8, 128), 1) // BLK
    colk = lax.broadcasted_iota(jnp.int32, (64, 256), 1)
    rowk = lax.broadcasted_iota(jnp.int32, (64, 256), 0)
    own_b = ((colk // BLK) % B) == (rowk % B)
    ecol = lax.broadcasted_iota(jnp.int32, (128, 1024), 1)
    erow = lax.broadcasted_iota(jnp.int32, (128, 1024), 0)
    emat[...] = jnp.where((ecol // 256) * BLK + ecol % BLK == erow, 1.0, 0.0).astype(BF16)
    swapped(qx, send_q, recv_q).wait_recv()
    for p in range(NTP):
        sk = lax.dot_general(head_rows(qx[p]), snd[0, p].reshape(B * BLK, 128), (((1,), (1,)), ((), ())), preferred_element_type=F32) * 0.125
        sk = jnp.where(own_b, sk, 0.0)
        sk = sk[:, :128] + sk[:, 128:]
        for shift in (64, 32, 16):
            sk = sk + pltpu.roll(sk, shift, 1)
        packed = sk[0:8]
        for k in range(1, 8):
            packed = jnp.where(lane8 == k, sk[8 * k:8 * k + 8], packed)
        sown[p] = packed
    for n in range(3):
        swap(sown.at[peers[n]], sx.at[me], send_s, recv_s, n)
    sx[me] = sown[me]
    cache_send(1, 1)
    repack(2)
    cache_send(2, 0)
    cache_send(2, 2)
    repack(3)
    cache_send(3, 2)
    cache_send(0, 2)

    def emit(c, new):
        new3 = jnp.broadcast_to(new[:, None, :], (B, BLK, 128))
        len3 = jnp.broadcast_to(len_b[:, None, :], (B, BLK, 128))
        pos3 = lax.broadcasted_iota(jnp.int32, (B, BLK, 128), 1).astype(F32)
        for s in range(NTP):
            x = jnp.where(pos3 + float(s * BLK) == len3, new3, kall[c, s].astype(F32)).reshape(B * BLK, 128)
            spread[pl.ds(0, B * BLK, stride=2), :] = x[:, :64]
            spread[pl.ds(1, B * BLK, stride=2), :] = x[:, 64:]
            outs[c][:, pl.ds(s * 2 * BLK, 2 * BLK), :] = spread[pl.ds(0, 2 * B * BLK), :].astype(BF16).reshape(B, 2 * BLK, 64)

    def x_send(step, piece, val):
        sl = pl.ds(*PIECES[step % 2][piece])
        xown[step, :, sl] = val
        for n in range(3):
            pltpu.make_async_remote_copy(
                src_ref=xown.at[step, :, sl], dst_ref=xrecv.at[step, me, :, sl],
                send_sem=send_x.at[0], recv_sem=recv_x.at[step],
                device_id={"tp": peers[n]}, device_id_type=MESH).start()
        xrecv[step, me, :, sl] = val

    def x_sum(step):
        pltpu.make_async_remote_copy(
            src_ref=xrecv.at[step, pl.ds(0, 3)], dst_ref=xrecv.at[step, pl.ds(0, 3)],
            send_sem=send_x.at[0], recv_sem=recv_x.at[step],
            device_id={"tp": partner}, device_id_type=MESH).wait_recv()
        tot = xrecv[step, 0].astype(F32)
        for s in range(1, NTP):
            tot = tot + xrecv[step, s].astype(F32)
        return tot

    outs = (ok1, ov1, ok2, ov2)

    for l in range(2):
        if l == 1:
            q, knew, vnew = project(l, h_f)
        qrows = head_rows(q)
        kc, vc = 2 * l, 2 * l + 1
        ns = jnp.sum(qrows.astype(F32) * jnp.concatenate([knew] * 4, axis=0), axis=1, keepdims=True) * 0.125
        if l == 0:
            swapped(sx, send_s, recv_s).wait_recv()
            rows = []
            for k in range(8):
                acc = jnp.zeros((8, 128), F32)
                for sd in range(NTP):
                    shift = (BLK * (sd - k)) % 128
                    part = sx[sd] if shift == 0 else pltpu.roll(sx[sd], shift, 1)
                    acc = jnp.where(lane8 == sd, part, acc)
                rows.append(acc)
            sc = jnp.concatenate(rows, axis=0)
            ok = lax.broadcasted_iota(jnp.int32, (64, 128), 1).astype(F32) < len64
        else:
            cache_wait(kc)
            k2d = kall[kc].reshape(NTP * B * BLK, 128)
            sc = lax.dot_general(qrows, k2d, (((1,), (1,)), ((), ())), preferred_element_type=F32) * 0.125
            ok = valid
        sc = jnp.where(ok, sc, -1e30)
        top = jnp.maximum(jnp.max(sc, axis=1, keepdims=True), ns)
        ex, nex = jnp.exp(sc - top), jnp.exp(ns - top)
        den = jnp.sum(ex, axis=1, keepdims=True) + nex
        prob = (ex / den).astype(BF16)
        nprob = (nex / den).astype(BF16).astype(F32)
        if l == 0:
            wide = jnp.dot(prob, emat[...], preferred_element_type=F32)
            prob = jnp.where(valid, wide, 0.0).astype(BF16)
        cache_wait(vc)
        v2d = kall[vc].reshape(NTP * B * BLK, 128)
        ov = jnp.dot(prob, v2d, preferred_element_type=F32) + nprob * jnp.concatenate([vnew] * 4, axis=0)
        attn = jnp.concatenate([jnp.where(left, ov[0:16], ov[48:64]), jnp.where(left, ov[16:32], ov[32:48])], axis=1).astype(BF16)
        wo_rows = jnp.concatenate([wo[l, pl.ds(0, 64), :], wo[l, pl.ds(192, 64), :], wo[l, pl.ds(64, 128), :]], axis=0)
        x_send(2 * l, 0, jnp.dot(attn, wo_rows, preferred_element_type=F32).astype(BF16))
        if l == 0:
            cache_send(2, 1)
            cache_send(3, 0)
            cache_send(3, 1)
        else:
            cache_send(0, 0)
            cache_send(0, 1)
            emit(kc, knew)
        emit(vc, vnew)
        for k in range(3):
            w_copy(l, k).wait()
        if l == 0:
            start_layer(1)
        h1 = (h_f + x_sum(2 * l)).astype(BF16).astype(F32)
        m = _norm(h1, gm[pl.ds(l, 1), :].astype(F32))

        lg = lax.dot_general(wr[l], m, (((1,), (1,)), ((), ())), preferred_element_type=F32)
        eid = lax.broadcasted_iota(jnp.int32, (EXP, B), 0)
        chosen = eid < 0
        for k in range(8):
            chosen = chosen | (cho[l, pl.ds(k, 1), :] == eid)
        lg = jnp.where(chosen, lg, -jnp.inf)
        ex = jnp.where(chosen, jnp.exp(lg - jnp.max(lg, axis=0, keepdims=True)), 0.0)
        gate_t = ex / jnp.sum(ex, axis=0, keepdims=True)
        gate = gate_t.T
        for e in range(EXP):
            w = jnp.concatenate([wg[l, e], wu[l, e]], axis=1)
            gu = jnp.dot(m, w, preferred_element_type=F32)
            g, u = gu[:, :FL], gu[:, FL:]
            act[:, pl.ds(e * FL, FL)] = (g * jax.nn.sigmoid(g) * u * jnp.broadcast_to(gate[:, e:e + 1], (B, FL))).astype(BF16)
        def down(piece, pairs, acc):
            first, width = PIECES[1][piece]
            for e in pairs:
                rhs = wd[l, pl.ds(e, 2), :, pl.ds(first, width)].reshape(2 * FL, width)
                acc = acc + jnp.dot(act[:, pl.ds(e * FL, 2 * FL)], rhs, preferred_element_type=F32)
            return acc

        acc0 = down(0, range(0, EXP, 2), jnp.zeros((B, PIECES[1][0][1]), F32))
        acc1 = down(1, range(0, 8, 2), jnp.zeros((B, PIECES[1][1][1]), F32))
        x_send(2 * l + 1, 0, acc0.astype(BF16))
        acc1 = down(1, range(8, EXP, 2), acc1)
        x_send(2 * l + 1, 1, acc1.astype(BF16))
        if l == 0:
            kone = knew
        else:
            cache_wait(0)
            emit(0, kone)
        h_f = (h1 + x_sum(2 * l + 1)).astype(BF16).astype(F32)

    hout[...] = h_f.astype(BF16)
    swapped(qx, send_q, recv_q).wait_send()
    swapped(sx, send_s, recv_s).wait_send()
    pltpu.make_async_remote_copy(
        src_ref=snd.at[:, pl.ds(0, 3)], dst_ref=kall.at[:, pl.ds(0, 3)], send_sem=send_c.at[0], recv_sem=recv_c.at[0],
        device_id={"tp": partner}, device_id_type=MESH).wait_send()
    pltpu.make_async_remote_copy(
        src_ref=xrecv.at[:, pl.ds(0, 3)], dst_ref=xrecv.at[:, pl.ds(0, 3)], send_sem=send_x.at[0], recv_sem=recv_x.at[0],
        device_id={"tp": partner}, device_id_type=MESH).wait_send()


def _store(h, k1, v1, k2, v2, ho, ok1, ov1, ok2, ov2, sem):
    copies = [pltpu.make_async_copy(a, b, sem.at[i])
              for i, (a, b) in enumerate(((k1, ok1), (v1, ov1), (k2, ok2), (v2, ov2), (h, ho)))]
    for c in copies:
        c.start()
    for c in copies:
        c.wait()


def solution(mesh):
    seq_spec = P('dp', 'tp', None, None)
    head_spec = P('dp', None, 'tp', None)
    col_spec = P(None, None, 'tp')
    ff_spec = P(None, None, None, 'tp')
    inv_freq = (THETA ** (-2.0 * np.arange(32, dtype=np.float64) / 64)).astype(np.float32)
    inv_row = np.tile(inv_freq, 4)[None, :]

    def local_step(hidden, lengths, choice, keys_one, vals_one, keys_two, vals_two, g_attn, w_q, w_k, w_v, w_o, g_mlp, w_router, w_gate, w_up, w_down):
        shapes = (jax.ShapeDtypeStruct((B, D), BF16),) + (jax.ShapeDtypeStruct((B, 2 * SEQ, 64), BF16),) * 4
        any_spec = pl.BlockSpec(memory_space=pl.ANY)
        vmem_spec = pl.BlockSpec(memory_space=pltpu.VMEM)
        V = pltpu.VMEM
        DMA = pltpu.SemaphoreType.DMA
        outs = pl.pallas_call(
            _kernel,
            out_shape=tuple(V(s.shape, s.dtype) for s in shapes),
            in_specs=[any_spec] * 18,
            out_specs=(vmem_spec,) * 5,
            scratch_shapes=[
                V((B, D), BF16), V((1, B), jnp.int32), V((2, 8, B), jnp.int32), V((4, B, BLK, 8, 64), BF16),
                V((2, D), BF16), V((2, D, 256), BF16), V((2, D, 128), BF16), V((2, D, 128), BF16), V((2, 256, D), BF16),
                V((2, D), BF16), V((2, EXP, D), BF16), V((2, EXP, D, FL), BF16), V((2, EXP, D, FL), BF16), V((2, EXP, FL, D), BF16),
                V((1, 128), F32),
                V((B * BLK * 8, 64), F32), V((4, NTP, B, BLK, 128), BF16), V((4, NTP, B, BLK, 128), BF16),
                V((4, B, D), BF16), V((4, NTP, B, D), BF16), V((B, EXP * FL), BF16), V((B, 256), BF16), V((NTP, B, 256), BF16), V((NTP, 8, 128), F32), V((NTP, 8, 128), F32), V((128, 1024), BF16),
                DMA((14,)), DMA((4,)), DMA((2, 3)), DMA((1,)), DMA((4,)), DMA((1,)), DMA((4,)), DMA((1,)), DMA((1,)), DMA((1,)), DMA((1,)),
            ],
            compiler_params=pltpu.CompilerParams(collective_id=0, has_side_effects=True, vmem_limit_bytes=64_000_000),
        )(hidden, lengths.reshape(1, B), jnp.transpose(choice, (0, 2, 1)), keys_one, vals_one, keys_two, vals_two,
          g_attn, w_q, w_k, w_v, w_o, g_mlp, jnp.transpose(w_router, (0, 2, 1)), w_gate, w_up, w_down, jnp.asarray(inv_row))
        outs = pl.pallas_call(
            _store,
            out_shape=shapes,
            in_specs=[vmem_spec] * 5,
            out_specs=(any_spec,) * 5,
            scratch_shapes=[DMA((5,))],
        )(*[pltpu.with_memory_space_constraint(o, pltpu.VMEM) for o in outs])
        return (outs[0],) + tuple(o.reshape(B, SEQ, 2, 64) for o in outs[1:])

    return jax.shard_map(local_step, mesh=mesh, in_specs=(P('dp', None), P('dp'), P(None, 'dp', None), seq_spec, seq_spec, seq_spec, seq_spec, P(), col_spec, col_spec, col_spec, P(None, 'tp', None), P(), P(), ff_spec, ff_spec, P(None, None, 'tp', None)), out_specs=(P('dp', None), head_spec, head_spec, head_spec, head_spec), check_vma=False)
```
